32 devices in a mesh: tile: 8 (over z, y), lev: 4 (over x, core).
Axes of the slice: x: 2, y: 2, z: 4, core: 2. Of those that a mesh axis runs over, the one named last changes fastest.
Arguments:
- trajectory: bfloat16 [3, 32, 16384], P(None, 'lev', 'tile'), may hold values from -6 to 6
- increment: bfloat16 [3, 32, 16384], P(None, 'lev', 'tile'), may hold values from -6 to 6
- counts: int32 [8, 8], P('tile'), may hold values from 1 to 512, 2048 in all within a row
- remap_weight: bfloat16 [8, 8, 512, 512], P('tile'), may hold values from -0.25 to 0.25
- kappa: float32 [3], replicated, may hold values from 0.1 to 0.4
- courant: float32 [16384], P('tile'), may hold values from 0.1 to 0.6
- vertical: float32 [16384], P('tile'), may hold values from -0.4 to 0.4
- offset: int32 [16384], P('tile'), may hold values from -2 to 2
Outputs:
- tangent: float32 [3, 32, 16384], P(None, 'lev', 'tile')
- grad_outer: float32 [3, 32, 16384], P(None, 'lev', 'tile')
The draws below stay inside these ranges and needn't reach their ends.
Inputs may be any that keep to these rules, and one draw needn't show every extreme that they name: Each row of counts sums to 2048, and every row has an entry equal to 512.
All inputs are finite; a program needn't handle non-finite values.
Results may differ from the reference program's by a relative error of at most 0.0021.
The reference program's roundings to bfloat16 on the way count: a program that leaves them out, or rounds other values in their place, can miss the bound.
Values may be sent and summed in bfloat16 or wider, within the bound.
No kernel may reach another device: no remote copies, remote signals or barrier semaphores. Data moves between devices by JAX's collectives and lax.ppermute only.
A program may use at most 64 MiB of HBM per device.

```python
import math
import jax
import jax.numpy as jnp
import numpy as np
from jax import lax

TRACERS = 3
LEVELS = 32
REACH = 8
OC_DEV = 2048
HALO = 2
OCOLS = 16384
ICOLS = 16384
CAP = 512
SPAN = 256
WIN = 512
N_TILE = 8


def plant(result, stream_key, smallest, largest):
    spot = [jax.random.randint(jax.random.fold_in(stream_key, axis), (), 0, length) for axis, length in enumerate(result.shape)]
    longest = result.shape.index(max(result.shape))
    neighbour = spot[:longest] + [(spot[longest] + 1) % result.shape[longest]] + spot[longest + 1:]
    return result.at[tuple(spot)].set(smallest).at[tuple(neighbour)].set(largest)


def level_of(stream_key, dims, cuts, low, high):
    def one(dim, parts):
        steps = jax.random.uniform(jax.random.fold_in(jax.random.fold_in(stream_key, 6), dim), (parts,), jnp.float32, low / len(cuts), high / len(cuts))
        return jnp.repeat(jnp.exp(steps), dims[dim] // parts).reshape((-1,) + (1,) * (len(dims) - dim - 1))

    gain = one(*cuts[0])
    for cut in cuts[1:]:
        gain = gain * one(*cut)
    return gain


def split_up(amount, total, limit, skew):
    loads = [(1 << 20) // math.isqrt(rank ** skew) + 1 for rank in range(2, amount + 1)]
    spare, holding = total - limit - (amount - 1), [1] * (amount - 1)
    while spare > 0:
        free = [i for i in range(amount - 1) if holding[i] < limit]
        whole, budget = sum([loads[i] for i in free]), spare
        for i in free:
            addition = min(limit - holding[i], max(1, budget * loads[i] // whole), spare)
            holding[i] = holding[i] + addition
            spare = spare - addition
    return np.array([limit] + holding)


def ragged_sizes(stream_key, amount, total, reach, lean):
    if amount == 2:
        one = jax.random.randint(stream_key, (), max(1, total - reach), min(reach, total - 1) + 1)
        return jnp.stack([one, total - one])
    sizes = jnp.asarray(split_up(amount, total, reach, lean), jnp.int32)
    couples = (amount - 1) // 2
    donor, taker = sizes[1:1 + 2 * couples:2], sizes[2:2 + 2 * couples:2]
    slack = jnp.minimum(donor - 1, reach - taker)
    shifted = jax.random.randint(jax.random.fold_in(stream_key, 1), (couples,), 0, 1 << 20) % (slack + 1)
    sizes = sizes.at[1:1 + 2 * couples:2].set(donor - shifted).at[2:2 + 2 * couples:2].set(taker + shifted)
    return sizes[jax.random.permutation(jax.random.fold_in(stream_key, 2), amount)]


def gaussian(stream_key, shape, spread, bound, shards=(), kind=jnp.bfloat16):
    entries = spread * jax.random.normal(stream_key, shape, jnp.float32)
    if shards:
        entries = entries * level_of(stream_key, shape, shards, -0.22, 0.18)
    return jnp.clip(entries, -bound, bound).astype(kind)


def setup_inputs(seed: int = 0) -> dict:
    seeds = jax.random.split(jax.random.key(seed), 9)
    return {
        "trajectory": gaussian(seeds[0], (TRACERS, LEVELS, OCOLS), 1.0, 6.0, ((1, 4), (2, 8))),
        "increment": gaussian(seeds[1], (TRACERS, LEVELS, OCOLS), 1.0, 6.0, ((1, 4), (2, 8))),
        "counts": jax.vmap(lambda own: ragged_sizes(own, REACH, OC_DEV, CAP, 2))(jax.random.split(seeds[2], N_TILE)).reshape((N_TILE, REACH)).astype(jnp.int32),
        "remap_weight": gaussian(seeds[3], (N_TILE, REACH, WIN, CAP), CAP ** -0.5, 0.25, ((0, 8),)),
        "kappa": jnp.clip(jnp.exp(jax.random.uniform(seeds[4], (TRACERS,), jnp.float32, math.log(0.1), math.log(0.4))), 0.1, 0.4),
        "courant": jnp.clip(0.1 + 0.5 * jax.random.uniform(seeds[5], (ICOLS,), jnp.float32) ** level_of(seeds[5], (ICOLS,), ((0, 8),), -0.2, 0.2), 0.1, 0.6),
        "vertical": jnp.clip(jax.random.uniform(seeds[6], (ICOLS,), jnp.float32, -0.4, 0.4) * level_of(seeds[6], (ICOLS,), ((0, 8),), -0.4, 0.0), -0.4, 0.4),
        "offset": plant(jax.random.randint(seeds[7], (ICOLS,), -HALO, HALO + 1), jax.random.fold_in(seeds[7], 1), -HALO, HALO).astype(jnp.int32),
    }


highest = lax.Precision.HIGHEST


def column_slots(sizes_row, slot_count, column_count):
    sizes_row = sizes_row.astype(jnp.int32)
    group_end = jnp.cumsum(sizes_row).astype(jnp.int32)
    group_start = (group_end - sizes_row).astype(jnp.int32)
    position = jnp.arange(slot_count, dtype=jnp.int32)
    slot_index = jnp.minimum(group_start[:, None] + position[None, :], column_count - 1).astype(jnp.int32)
    slot_live = position[None, :] < sizes_row[:, None]
    columns = jnp.arange(column_count, dtype=jnp.int32)
    owner = jnp.searchsorted(group_end, columns, side="right").astype(jnp.int32)
    back_index = (owner * slot_count + columns - jnp.take(group_start, owner)).astype(jnp.int32)
    return slot_index, slot_live, back_index


def shifted_levels(field, upward):
    zero_level = jnp.zeros_like(field[:, :1])
    if upward:
        return jnp.concatenate([field[:, 1:], zero_level], axis=1)
    return jnp.concatenate([zero_level, field[:, :-1]], axis=1)


def reference(trajectory, increment, counts, remap_weight, kappa, courant, vertical, offset):
    field_rows = TRACERS * LEVELS
    centre = REACH // 2
    fields = jnp.concatenate([trajectory, increment], axis=0).reshape(2 * field_rows, OCOLS)
    senders = jnp.arange(N_TILE, dtype=jnp.int32)
    reach_ids = jnp.arange(REACH, dtype=jnp.int32)

    def forward_sender(sender):
        slot_index, slot_live, back_index = column_slots(counts[sender], CAP, OC_DEV)
        own_cols = lax.dynamic_slice_in_dim(fields, (sender * OC_DEV).astype(jnp.int32), OC_DEV, 1)
        slotted = jnp.take(own_cols, slot_index.reshape(-1), axis=1).reshape(2 * field_rows, REACH, CAP)
        slotted = jnp.where(slot_live[None], slotted, jnp.zeros_like(slotted))
        return jnp.einsum("fdc,dwc->dfw", slotted.astype(jnp.float32), remap_weight[sender].astype(jnp.float32), precision=highest)

    partial_value = lax.map(forward_sender, senders)
    source = ((senders[:, None] - reach_ids[None, :] + centre) % N_TILE).astype(jnp.int32)
    received = partial_value[source, reach_ids[None, :]]
    blocks = received[:, :, :, :SPAN] + jnp.roll(received[:, :, :, SPAN:], 1, axis=1)
    remapped = jnp.transpose(blocks, (2, 0, 1, 3)).reshape(2 * field_rows, ICOLS)
    state = remapped[:field_rows].reshape(TRACERS, LEVELS, ICOLS)
    delta = remapped[field_rows:].reshape(TRACERS, LEVELS, ICOLS)

    rising = jnp.maximum(vertical, 0.0)
    sinking = jnp.maximum(-vertical, 0.0)
    departed = jnp.zeros_like(delta)
    for shift_by in range(-HALO, HALO + 1):
        moved_view = jnp.roll(delta, -shift_by, axis=2)
        departed = departed + jnp.where(offset == shift_by, moved_view, jnp.zeros_like(moved_view))
    below = shifted_levels(delta, False)
    above = shifted_levels(delta, True)
    loss = 2.0 * kappa[:, None, None] * state
    tangent = delta + courant * (departed - delta) + rising * (below - delta) + sinking * (above - delta) - loss * delta

    arrived = jnp.zeros_like(tangent)
    for shift_by in range(-HALO, HALO + 1):
        weight_row = jnp.where(offset == shift_by, courant, jnp.zeros_like(courant))
        arrived = arrived + jnp.roll(weight_row * tangent, shift_by, axis=2)
    diagonal = 1.0 - courant - rising - sinking - loss
    adjoint = diagonal * tangent + arrived + rising * shifted_levels(tangent, True) + sinking * shifted_levels(tangent, False)

    adjoint_blocks = jnp.transpose(adjoint.reshape(field_rows, N_TILE, REACH, SPAN), (1, 2, 0, 3)).astype(jnp.bfloat16)
    windows = jnp.concatenate([adjoint_blocks, jnp.roll(adjoint_blocks, -1, axis=1)], axis=3)
    target = ((senders[:, None] + reach_ids[None, :] - centre) % N_TILE).astype(jnp.int32)
    returned_all = windows[target, reach_ids[None, :]]

    def backward_sender(sender):
        slot_index, slot_live, back_index = column_slots(counts[sender], CAP, OC_DEV)
        slot_grad = jnp.einsum("dfw,dwc->fdc", returned_all[sender].astype(jnp.float32), remap_weight[sender].astype(jnp.float32), precision=highest)
        return jnp.take(slot_grad.reshape(field_rows, REACH * CAP), back_index, axis=1)

    grads = lax.map(backward_sender, senders)
    grad_outer = jnp.transpose(grads, (1, 0, 2)).reshape(TRACERS, LEVELS, OCOLS)
    return tangent, grad_outer
```

```python
import functools

import jax
import jax.numpy as jnp
from jax import lax
from jax.experimental import pallas as pl
from jax.experimental.pallas import tpu as pltpu
from jax.sharding import PartitionSpec as P

HALO = 2
LANE = 128
SUB = 8
VALUE_MAX = 6.0
WEIGHT_MAX = 0.25
F16_MAX = 65504.0


def send_scale(slot_count):
    bound = VALUE_MAX * WEIGHT_MAX * slot_count
    scale = 1.0
    while 2.0 * scale * bound < F16_MAX:
        scale *= 2.0
    while scale * bound >= F16_MAX:
        scale *= 0.5
    return scale


def starts_of(counts_ref, which, reach):
    begin = jnp.int32(0)
    for other in range(reach):
        begin = begin + jnp.where(other < which, counts_ref[0, other], 0)
    return begin


def forward_kernel(scale, counts, gids, traj, inc, ext, coef, w_main, w_low, w_high, out, rows_f32):
    step = pl.program_id(0)
    reach = counts.shape[1]
    tracers, levels, cols = traj.shape
    slots = w_main.shape[-1]
    window = slots + LANE
    main = tracers * levels
    rows = rows_f32.shape[0]

    @pl.when(step == 0)
    def _():
        for m in range(tracers):
            rows_f32[m * levels : (m + 1) * levels, :] = traj[m].astype(jnp.float32)
            rows_f32[main + m * levels : main + (m + 1) * levels, :] = inc[m].astype(jnp.float32)
        rows_f32[2 * main :, :] = ext[...].astype(jnp.float32)

    def slotted(which):
        begin = starts_of(counts, which, reach)
        base = jnp.minimum((begin // LANE) * LANE, cols - window)
        base = pl.multiple_of(base, LANE)
        shift = begin - base
        x = rows_f32[:, pl.ds(base, window)]
        x = pltpu.roll(x, lax.rem(window - shift, window), axis=1)[:, :slots]
        lane = lax.broadcasted_iota(jnp.int32, x.shape, 1)
        return jnp.where(lane < counts[0, which], x, 0.0).astype(jnp.bfloat16)

    contract = (((1,), (1,)), ((), ()))
    group = gids[step]
    y = slotted(group)
    out[0, :rows, :] = scale * lax.dot_general(
        y, w_main[0, 0], contract, preferred_element_type=jnp.float32
    )
    out[0, rows:, : 2 * LANE] = jnp.zeros((SUB, 2 * LANE), jnp.float32)
    out[0, rows:, 2 * LANE : 3 * LANE] = scale * coef[:, cols - LANE :]
    out[0, rows:, 3 * LANE :] = scale * coef[:, :LANE]

    @pl.when((group == 0) | (group == reach - 1))
    def _():
        z = slotted(lax.rem(group + reach - 1, reach))
        out[0, rows:, :rows] = scale * lax.dot_general(
            w_low[0, 0], z, contract, preferred_element_type=jnp.float32
        )

    @pl.when((group == reach - 2) | (group == reach - 1))
    def _():
        z = slotted(lax.rem(group + 1, reach))
        out[0, rows:, LANE : LANE + rows] = scale * lax.dot_general(
            w_high[0, 0], z, contract, preferred_element_type=jnp.float32
        )


def forward(counts, gids, traj, inc, ext, coef, weight, scale):
    tracers, levels, cols = traj.shape
    _, reach, win, slots = weight.shape
    rows = 2 * tracers * levels + ext.shape[0]
    half, last = win // 2 // SUB, win // SUB - 1
    whole = lambda *shape: pl.BlockSpec(shape, lambda i, c, g: (0,) * len(shape))
    return pl.pallas_call(
        functools.partial(forward_kernel, scale),
        grid_spec=pltpu.PrefetchScalarGridSpec(
            num_scalar_prefetch=2,
            grid=(reach,),
            in_specs=[
                whole(tracers, levels, cols),
                whole(tracers, levels, cols),
                whole(*ext.shape),
                whole(*coef.shape),
                pl.BlockSpec((1, 1, win, slots), lambda i, c, g: (0, g[i], 0, 0)),
                pl.BlockSpec(
                    (1, 1, SUB, slots),
                    lambda i, c, g: (
                        0,
                        lax.rem(g[i] + reach - 1, reach),
                        jnp.where(g[i] == 0, half - 1, last),
                        0,
                    ),
                ),
                pl.BlockSpec(
                    (1, 1, SUB, slots),
                    lambda i, c, g: (
                        0,
                        lax.rem(g[i] + 1, reach),
                        jnp.where(g[i] == reach - 2, half, 0),
                        0,
                    ),
                ),
            ],
            out_specs=pl.BlockSpec((1, rows + SUB, win), lambda i, c, g: (i, 0, 0)),
            scratch_shapes=[pltpu.VMEM((rows, cols), jnp.float32)],
        ),
        out_shape=jax.ShapeDtypeStruct((reach, rows + SUB, win), jnp.float32),
        compiler_params=pltpu.CompilerParams(
            dimension_semantics=("arbitrary",), vmem_limit_bytes=16 << 20
        ),
        cost_estimate=pl.CostEstimate(
            flops=2 * reach * rows * win * slots, bytes_accessed=2 * weight.size, transcendentals=0
        ),
        name="remap",
    )(counts, gids, traj, inc, ext, coef, weight, weight, weight)


def stencil_kernel(unscale, gids, edge, kappa, *refs):
    reach = gids.shape[0]
    pieces = refs[:reach]
    coef, tangent_out, windows_out, acc, turn, adj = refs[reach:]
    tracers, levels, cols = tangent_out.shape
    main = tracers * levels
    rows = acc.shape[0]
    span = cols // reach
    wide = cols + LANE

    acc[...] = jnp.zeros_like(acc)
    low = jnp.zeros((SUB, LANE), jnp.float32)
    high = jnp.zeros((SUB, LANE), jnp.float32)
    coef_low = jnp.zeros((SUB, LANE), jnp.float32)
    coef_high = jnp.zeros((SUB, LANE), jnp.float32)
    for k in range(reach):
        group = gids[k]
        first = pl.multiple_of(group * span, LANE)
        second = pl.multiple_of(lax.rem(group + 1, reach) * span, LANE)
        acc[:, pl.ds(first, span)] += unscale * pieces[k][:rows, :span]
        acc[:, pl.ds(second, span)] += unscale * pieces[k][:rows, span:]
        low = low + pieces[k][rows:, :LANE]
        high = high + pieces[k][rows:, LANE : 2 * LANE]
        coef_low = jnp.where(group == reach // 2 + 1, pieces[k][rows:, 2 * LANE : 3 * LANE], coef_low)
        coef_high = jnp.where(group == reach // 2 - 1, pieces[k][rows:, 3 * LANE :], coef_high)
    turn[...] = jnp.zeros_like(turn)
    turn[:SUB, :] = unscale * high
    turn[LANE - SUB :, :] = unscale * low
    acc[:, cols:] = turn[...].T[:rows, :]

    lane = lax.broadcasted_iota(jnp.int32, (SUB, LANE), 1)
    beyond = unscale * jnp.where(lane < LANE // 2, coef_high, coef_low)
    coefs = jnp.concatenate([coef[...], beyond], axis=1)
    spread = lambda row: jnp.broadcast_to(row, (SUB, wide))
    courant = spread(coefs[0:1] + coefs[1:2])
    vertical = spread(coefs[2:3] + coefs[3:4])
    offset = spread(coefs[4:5])
    rising = jnp.maximum(vertical, 0.0)
    sinking = jnp.maximum(-vertical, 0.0)
    shifts = range(-HALO, HALO + 1)
    picked = {s: offset == jnp.float32(s) for s in shifts}
    turned = lambda x, by: x if by % wide == 0 else pltpu.roll(x, by % wide, axis=1)

    def tangent_of(delta, loss, below, above):
        departed = jnp.zeros_like(delta)
        for s in shifts:
            departed = jnp.where(picked[s], turned(delta, -s), departed)
        return (
            delta
            + courant * (departed - delta)
            + rising * (below - delta)
            + sinking * (above - delta)
            - loss * delta
        )

    sub = lax.broadcasted_iota(jnp.int32, (SUB, wide), 0)
    x_state = acc[2 * main : 2 * main + SUB, :]
    x_delta = acc[2 * main + SUB : 2 * main + 2 * SUB, :]
    x_outer = acc[2 * main + 2 * SUB : 2 * main + 3 * SUB, :]
    own = [acc[main + m * levels : main + (m + 1) * levels, :] for m in range(tracers)]
    x_below, x_above = x_outer, x_outer
    x_kappa = jnp.zeros((SUB, wide), jnp.float32)
    for m in range(tracers):
        x_below = jnp.where(sub == tracers + m, spread(own[m][levels - 1 :]), x_below)
        x_above = jnp.where(sub == m, spread(own[m][:1]), x_above)
        x_kappa = jnp.where((sub == m) | (sub == tracers + m), kappa[m], x_kappa)
    x_tangent = tangent_of(x_delta, 2.0 * x_kappa * x_state, x_below, x_above)
    dead = ((sub < tracers) & (edge[0] == 1)) | ((sub >= tracers) & (edge[1] == 1))
    x_tangent = jnp.where(dead, 0.0, x_tangent)

    for m in range(tracers):
        delta = own[m]
        loss = 2.0 * kappa[m] * acc[m * levels : (m + 1) * levels, :]
        below = jnp.where(sub == 0, spread(x_delta[m : m + 1]), pltpu.roll(delta, 1, axis=0))
        above = jnp.where(
            sub == levels - 1,
            spread(x_delta[tracers + m : tracers + m + 1]),
            pltpu.roll(delta, levels - 1, axis=0),
        )
        tangent = tangent_of(delta, loss, below, above)
        tangent_out[m] = tangent[:, :cols]
        flux = courant * tangent
        arrived = jnp.zeros_like(tangent)
        for s in shifts:
            arrived = arrived + turned(jnp.where(picked[s], flux, 0.0), s)
        t_below = jnp.where(sub == 0, spread(x_tangent[m : m + 1]), pltpu.roll(tangent, 1, axis=0))
        t_above = jnp.where(
            sub == levels - 1,
            spread(x_tangent[tracers + m : tracers + m + 1]),
            pltpu.roll(tangent, levels - 1, axis=0),
        )
        adjoint = (
            (1.0 - courant - rising - sinking - loss) * tangent
            + arrived
            + rising * t_above
            + sinking * t_below
        )
        adj[m * levels : (m + 1) * levels, :cols] = adjoint[:, :cols]
        adj[m * levels : (m + 1) * levels, cols:] = adjoint[:, :span]
    for k in range(reach):
        first = pl.multiple_of(gids[k] * span, LANE)
        windows_out[k] = adj[:, pl.ds(first, 2 * span)].astype(jnp.bfloat16)


def stencil(gids, edge, kappa, pieces, coef, tracers, levels, cols, unscale):
    reach = len(pieces)
    rows = pieces[0].shape[0] - SUB
    span = cols // reach
    smem = pl.BlockSpec(memory_space=pltpu.SMEM)
    vmem = pl.BlockSpec(memory_space=pltpu.VMEM)
    return pl.pallas_call(
        functools.partial(stencil_kernel, unscale),
        in_specs=[smem] * 3 + [vmem] * (reach + 1),
        out_specs=[vmem, vmem],
        out_shape=[
            jax.ShapeDtypeStruct((tracers, levels, cols), jnp.float32),
            jax.ShapeDtypeStruct((reach, tracers * levels, 2 * span), jnp.bfloat16),
        ],
        scratch_shapes=[
            pltpu.VMEM((rows, cols + LANE), jnp.float32),
            pltpu.VMEM((LANE, LANE), jnp.float32),
            pltpu.VMEM((tracers * levels, cols + span), jnp.float32),
        ],
        compiler_params=pltpu.CompilerParams(vmem_limit_bytes=24 << 20),
        cost_estimate=pl.CostEstimate(flops=100 * rows * cols, bytes_accessed=8 * rows * cols, transcendentals=0),
        name="stencil",
    )(gids, edge, kappa, *pieces, coef)


def backward_kernel(counts, gids, *refs):
    step = pl.program_id(0)
    reach = counts.shape[1]
    pieces = refs[:reach]
    weight, out, stack = refs[reach:]
    tracers, levels, cols = out.shape
    main = tracers * levels
    slots = weight.shape[-1]
    window = slots + LANE

    @pl.when(step == 0)
    def _():
        out[...] = jnp.zeros_like(out)
        for k in range(reach):
            stack[k] = pieces[k][...].astype(jnp.float32)

    group = gids[step]
    grad = jnp.dot(
        stack[step].astype(jnp.bfloat16), weight[0, 0], preferred_element_type=jnp.float32
    )
    lane = lax.broadcasted_iota(jnp.int32, grad.shape, 1)
    grad = jnp.where(lane < counts[0, group], grad, 0.0)
    grad = jnp.concatenate([grad, jnp.zeros((main, LANE), jnp.float32)], axis=1)
    begin = starts_of(counts, group, reach)
    base = pl.multiple_of(jnp.minimum((begin // LANE) * LANE, cols - window), LANE)
    grad = pltpu.roll(grad, begin - base, axis=1)
    for m in range(tracers):
        out[m, :, pl.ds(base, window)] += grad[m * levels : (m + 1) * levels]


def backward(counts, gids, pieces, weight, tracers, levels, cols):
    _, reach, win, slots = weight.shape
    main = tracers * levels
    return pl.pallas_call(
        backward_kernel,
        grid_spec=pltpu.PrefetchScalarGridSpec(
            num_scalar_prefetch=2,
            grid=(reach,),
            in_specs=[pl.BlockSpec((main, win), lambda i, c, g: (0, 0))] * reach
            + [pl.BlockSpec((1, 1, win, slots), lambda i, c, g: (0, g[i], 0, 0))],
            out_specs=pl.BlockSpec((tracers, levels, cols), lambda i, c, g: (0, 0, 0)),
            scratch_shapes=[pltpu.VMEM((reach, main, win), jnp.float32)],
        ),
        out_shape=jax.ShapeDtypeStruct((tracers, levels, cols), jnp.float32),
        compiler_params=pltpu.CompilerParams(
            dimension_semantics=("arbitrary",), vmem_limit_bytes=16 << 20
        ),
        cost_estimate=pl.CostEstimate(
            flops=2 * reach * main * win * slots, bytes_accessed=2 * weight.size, transcendentals=0
        ),
        name="remap_back",
    )(counts, gids, *pieces, weight)


def plan(tiles, reach):
    centre = reach // 2
    me = lax.axis_index("tile")
    messages = []
    for k in range(reach):
        if tiles == reach and tiles & (tiles - 1) == 0:
            route = [(i, i ^ k) for i in range(tiles)]
            other = me ^ k
            send = lax.rem(other - me + centre + reach, reach)
            take = lax.rem(me - other + centre + reach, reach)
            messages.append((None if k == 0 else route, send, take))
        else:
            route = [(i, (i + k - centre) % tiles) for i in range(tiles)]
            messages.append((None if k == centre else route, jnp.int32(k), jnp.int32(k)))
    return messages


def shards(trajectory, increment, counts, remap_weight, kappa, courant, vertical, offset):
    tracers, levels, cols = trajectory.shape
    reach, _, slots = remap_weight.shape[1:]
    tiles, slabs = lax.axis_size("tile"), lax.axis_size("lev")
    lev = lax.axis_index("lev")
    messages = plan(tiles, reach)
    send_gids = jnp.stack([send for _, send, _ in messages]).astype(jnp.int32)
    take_gids = jnp.stack([take for _, _, take in messages]).astype(jnp.int32)
    edge = jnp.stack([lev == 0, lev == slabs - 1]).astype(jnp.int32)
    scale = send_scale(slots)

    up = [(i, i + 1) for i in range(slabs - 1)]
    down = [(i + 1, i) for i in range(slabs - 1)]
    tail = jnp.stack([trajectory[:, -1], increment[:, -1], increment[:, -2]])
    head = jnp.stack([trajectory[:, 0], increment[:, 0], increment[:, 1]])
    before = lax.ppermute(tail, "lev", up)
    after = lax.ppermute(head, "lev", down)
    blank = jnp.zeros((3, SUB - 2 * tracers, cols), before.dtype)
    ext = jnp.concatenate([before, after, blank], axis=1).reshape(3 * SUB, cols)

    courant_top = lax.reduce_precision(courant, 8, 7)
    vertical_top = lax.reduce_precision(vertical, 8, 7)
    empty = jnp.zeros_like(courant)
    coef = jnp.stack(
        [
            courant_top,
            courant - courant_top,
            vertical_top,
            vertical - vertical_top,
            offset.astype(jnp.float32),
            empty,
            empty,
            empty,
        ]
    )

    partial = forward(counts, send_gids, trajectory, increment, ext, coef, remap_weight, scale)
    packed = partial.astype(jnp.float16)
    pieces = []
    for k, (route, _, _) in enumerate(messages):
        pieces.append(packed[k] if route is None else lax.ppermute(packed[k], "tile", route))
    if tiles != reach:
        rows = packed.shape[1] - SUB
        out_low = [(i, (i + reach // 2) % tiles) for i in range(tiles)]
        out_high = [(i, (i - reach // 2 - 1) % tiles) for i in range(tiles)]
        low = lax.ppermute(packed[0, rows:, :LANE], "tile", out_low)
        high = lax.ppermute(packed[reach - 1, rows:, LANE : 2 * LANE], "tile", out_high)
        pieces[0] = pieces[0].at[rows:, :LANE].set(low)
        pieces[reach - 1] = pieces[reach - 1].at[rows:, LANE : 2 * LANE].set(high)
    pieces = [piece.astype(jnp.float32) for piece in pieces]

    tangent, windows = stencil(
        take_gids, edge, kappa, pieces, coef, tracers, levels, cols, 1.0 / scale
    )
    returned = []
    for k, (route, _, _) in enumerate(messages):
        back = None if route is None else [(j, i) for i, j in route]
        returned.append(windows[k] if back is None else lax.ppermute(windows[k], "tile", back))
    grad_outer = backward(counts, send_gids, returned, remap_weight, tracers, levels, cols)
    return (tangent, grad_outer)


def solution(mesh):
    return jax.shard_map(
        shards,
        mesh=mesh,
        in_specs=(
            P(None, "lev", "tile"),
            P(None, "lev", "tile"),
            P("tile", None),
            P("tile", None, None, None),
            P(),
            P("tile"),
            P("tile"),
            P("tile"),
        ),
        out_specs=(P(None, "lev", "tile"), P(None, "lev", "tile")),
        check_vma=False,
    )
```

```python
import functools

import jax
import jax.numpy as jnp
import numpy as np
from jax import lax
from jax.experimental import pallas as pl
from jax.experimental.pallas import tpu as pltpu
from jax.sharding import PartitionSpec as P

HALO = 2
LANE = 128
SUB = 8
EDGE = 3
COEFS = 5
VALUE_MAX = 6.0
WEIGHT_MAX = 0.25
F16_MAX = 65504.0


VMEM = pl.BlockSpec(memory_space=pltpu.VMEM)
SMEM = pl.BlockSpec(memory_space=pltpu.SMEM)
ANY = pl.BlockSpec(memory_space=pl.ANY)


def send_scale(slot_count):
    bound = VALUE_MAX * WEIGHT_MAX * slot_count
    scale = 1.0
    while 2.0 * scale * bound < F16_MAX:
        scale *= 2.0
    while scale * bound >= F16_MAX:
        scale *= 0.5
    return scale


def cost(flops, moved):
    return pl.CostEstimate(flops=flops, bytes_accessed=moved, transcendentals=0)


def place(counts, which, reach, window, cols):
    begin = jnp.int32(0)
    for other in range(reach):
        begin = begin + jnp.where(other < which, counts[0, other], 0)
    base = jnp.minimum((begin // LANE) * LANE, cols - window)
    return pl.multiple_of(base, LANE), begin - base


IDS = 3


def load_kernel(ids, traj, inc, weight, traj_out, inc_out, w_out, w_low, w_high, sems):
    rounds = w_out.shape[0]
    reach, win = weight.shape[1:3]
    half = win // 2
    copies = [
        pltpu.make_async_copy(traj, traj_out, sems.at[0]),
        pltpu.make_async_copy(inc, inc_out, sems.at[1]),
    ]
    for j in range(rounds):
        group = ids[IDS + j]
        low = lax.rem(group + reach - 1, reach)
        high = lax.rem(group + 1, reach)
        low_at = pl.multiple_of(jnp.where(group == 0, half, win) - SUB, SUB)
        high_at = pl.multiple_of(jnp.where(group == reach - 2, half, 0), SUB)
        copies.append(pltpu.make_async_copy(weight.at[0, group], w_out.at[j], sems.at[2 + 3 * j]))
        copies.append(
            pltpu.make_async_copy(
                weight.at[0, low, pl.ds(low_at, SUB)], w_low.at[j], sems.at[3 + 3 * j]
            )
        )
        copies.append(
            pltpu.make_async_copy(
                weight.at[0, high, pl.ds(high_at, SUB)], w_high.at[j], sems.at[4 + 3 * j]
            )
        )
    for copy in copies:
        copy.start()
    for copy in copies:
        copy.wait()


def load(ids, traj, inc, weight, rounds):
    _, reach, win, slots = weight.shape
    like = lambda *shape: jax.ShapeDtypeStruct(shape, weight.dtype)
    return pl.pallas_call(
        load_kernel,
        in_specs=[SMEM, ANY, ANY, ANY],
        out_specs=[VMEM] * 5,
        out_shape=[
            like(*traj.shape),
            like(*inc.shape),
            like(rounds, win, slots),
            like(rounds, SUB, slots),
            like(rounds, SUB, slots),
        ],
        scratch_shapes=[pltpu.SemaphoreType.DMA((2 + 3 * rounds,))],
        compiler_params=pltpu.CompilerParams(vmem_limit_bytes=8 << 20),
        cost_estimate=cost(0, 2 * rounds * win * slots * 2),
        name="fetch",
    )(ids, traj, inc, weight)


def gather_kernel(ids, traj, inc, traj_too, inc_too, ext, ext_too, rows_out):
    tracers, levels, _ = traj.shape
    main = tracers * levels
    mine = pl.multiple_of(ids[0] * 2 * main, SUB)
    theirs = pl.multiple_of((1 - ids[0]) * 2 * main, SUB)
    for m in range(tracers):
        for at, t, i in ((mine, traj, inc), (theirs, traj_too, inc_too)):
            rows_out[pl.ds(at + m * levels, levels), :] = t[m].astype(jnp.float32)
            rows_out[pl.ds(at + main + m * levels, levels), :] = i[m].astype(jnp.float32)
    beyond = ext[...].astype(jnp.float32) + ext_too[...].astype(jnp.float32)
    rows_out[4 * main :, :] = jnp.zeros_like(rows_out[4 * main :, :])
    rows_out[4 * main : 4 * main + EDGE * tracers, :] = beyond


def gather(ids, traj, inc, traj_too, inc_too, ext, ext_too, rows):
    cols = traj.shape[-1]
    return pl.pallas_call(
        gather_kernel,
        in_specs=[SMEM] + [VMEM] * 6,
        out_specs=VMEM,
        out_shape=jax.ShapeDtypeStruct((rows, cols), jnp.float32),
        compiler_params=pltpu.CompilerParams(vmem_limit_bytes=8 << 20),
        cost_estimate=cost(0, 6 * rows * cols),
        name="gather",
    )(ids, traj, inc, traj_too, inc_too, ext, ext_too)


def forward_kernel(which, scale, tail, ids, counts, rows_in, courant, vertical, offset, w, w_low, w_high, out):
    reach = counts.shape[1]
    rows, cols = rows_in.shape
    slots = w.shape[-1]
    window = slots + LANE
    contract = (((1,), (1,)), ((), ()))

    def slotted(group):
        base, shift = place(counts, group, reach, window, cols)
        x = rows_in[:, pl.ds(base, window)]
        x = pltpu.roll(x, lax.rem(window - shift, window), axis=1)[:, :slots]
        lane = lax.broadcasted_iota(jnp.int32, x.shape, 1)
        return jnp.where(lane < counts[0, group], x, 0.0).astype(jnp.bfloat16)

    group = ids[IDS + which]
    y = slotted(group)
    out[...] = scale * lax.dot_general(y, w[which], contract, preferred_element_type=jnp.float32)
    for part, at in enumerate((cols - LANE, 0)):
        span = slice((2 + part) * LANE, (3 + part) * LANE)
        for row, ref in ((0, courant), (2, vertical)):
            value = ref[:, at : at + LANE]
            top = value.astype(jnp.bfloat16).astype(jnp.float32)
            out[tail + row : tail + row + 1, span] = scale * top
            out[tail + row + 1 : tail + row + 2, span] = scale * (value - top)
        out[tail + 4 : tail + 5, span] = scale * offset[:, at : at + LANE].astype(jnp.float32)

    @pl.when((group == 0) | (group == reach - 1))
    def _():
        z = slotted(lax.rem(group + reach - 1, reach))
        e = scale * lax.dot_general(w_low[which], z, contract, preferred_element_type=jnp.float32)
        out[tail : tail + 2 * HALO, :rows] = e[SUB - 2 * HALO :]

    @pl.when((group == reach - 2) | (group == reach - 1))
    def _():
        z = slotted(lax.rem(group + 1, reach))
        e = scale * lax.dot_general(w_high[which], z, contract, preferred_element_type=jnp.float32)
        out[tail : tail + 2 * HALO, LANE : LANE + rows] = e[: 2 * HALO]


def forward(which, ids, counts, rows_in, courant, vertical, offset, w, w_low, w_high, scale, tail):
    rows = rows_in.shape[0]
    win, slots = w.shape[1:]
    return pl.pallas_call(
        functools.partial(forward_kernel, which, scale, tail),
        in_specs=[SMEM, SMEM] + [VMEM] * 7,
        out_specs=VMEM,
        out_shape=jax.ShapeDtypeStruct((rows, win), jnp.float32),
        compiler_params=pltpu.CompilerParams(vmem_limit_bytes=8 << 20),
        cost_estimate=cost(2 * rows * win * slots, 4 * rows_in.size),
        name=f"remap_{which}",
    )(ids, counts, rows_in, courant, vertical, offset, w, w_low, w_high)


def stencil_kernel(unscale, tail, rounds, reach, ids, kappa, *refs):
    pieces = refs[: 2 * rounds]
    courant_in, vertical_in, offset_in, tangent_out = refs[2 * rounds : 2 * rounds + 4]
    windows_out = refs[2 * rounds + 4 : 3 * rounds + 4]
    acc, turn, adj = refs[3 * rounds + 4 :]
    tracers, levels, cols = tangent_out.shape
    main = tracers * levels
    rows = acc.shape[0]
    span = cols // reach
    wide = cols + LANE

    acc[...] = jnp.zeros_like(acc)
    low = jnp.zeros((2 * HALO, LANE), jnp.float32)
    high = jnp.zeros((2 * HALO, LANE), jnp.float32)
    c_low = jnp.zeros((COEFS, LANE), jnp.float32)
    c_high = jnp.zeros((COEFS, LANE), jnp.float32)
    for k, piece in enumerate(pieces):
        group = ids[IDS + rounds + k]
        first = pl.multiple_of(group * span, LANE)
        second = pl.multiple_of(lax.rem(group + 1, reach) * span, LANE)
        acc[:, pl.ds(first, span)] += unscale * piece[:, :span]
        acc[:, pl.ds(second, span)] += unscale * piece[:, span:]
        is_low = (group == 0) | (group == reach - 1)
        is_high = (group == reach - 2) | (group == reach - 1)
        low = low + jnp.where(is_low, piece[tail : tail + 2 * HALO, :LANE], 0.0)
        high = high + jnp.where(is_high, piece[tail : tail + 2 * HALO, LANE : 2 * LANE], 0.0)
        c_low = jnp.where(group == reach // 2 + 1, piece[tail : tail + COEFS, 2 * LANE : 3 * LANE], c_low)
        c_high = jnp.where(group == reach // 2 - 1, piece[tail : tail + COEFS, 3 * LANE :], c_high)
    turn[...] = jnp.zeros_like(turn)
    turn[: 2 * HALO, :] = unscale * high
    turn[LANE - 2 * HALO :, :] = unscale * low
    acc[:, cols:] = turn[...].T[:rows, :]

    lane = lax.broadcasted_iota(jnp.int32, (COEFS, LANE), 1)
    beyond = unscale * jnp.where(lane < LANE // 2, c_high, c_low)
    spread = lambda row: jnp.broadcast_to(row, (SUB, wide))
    row_of = lambda ref, extra: spread(jnp.concatenate([ref[...].astype(jnp.float32), extra], axis=1))
    courant = row_of(courant_in, beyond[0:1] + beyond[1:2])
    vertical = row_of(vertical_in, beyond[2:3] + beyond[3:4])
    offset = row_of(offset_in, beyond[4:5])
    rising = jnp.maximum(vertical, 0.0)
    sinking = jnp.maximum(-vertical, 0.0)
    shifts = range(-HALO, HALO + 1)
    picked = {s: offset == jnp.float32(s) for s in shifts}
    turned = lambda x, by: x if by % wide == 0 else pltpu.roll(x, by % wide, axis=1)
    keep = 1.0 - courant - rising - sinking

    def tangent_of(delta, loss, below, above):
        departed = jnp.zeros_like(delta)
        for s in shifts:
            departed = jnp.where(picked[s], turned(delta, -s), departed)
        return (keep - loss) * delta + courant * departed + rising * below + sinking * above

    sub = lax.broadcasted_iota(jnp.int32, (SUB, wide), 0)
    has_prev, has_next = ids[1] == 1, ids[2] == 1
    state_of = lambda h, m: acc[2 * h * main + m * levels : 2 * h * main + (m + 1) * levels, :]
    delta_of = lambda h, m: acc[(2 * h + 1) * main + m * levels : (2 * h + 1) * main + (m + 1) * levels, :]
    line = lambda r: acc[4 * main + r : 4 * main + r + 1, :]
    x_state = jnp.zeros((SUB, wide), jnp.float32)
    x_delta, x_below, x_above, x_kappa = x_state, x_state, x_state, x_state
    for m in range(tracers):
        here = sub == m
        outer = line(2 * tracers + m)
        first = delta_of(0, m)[:1]
        final = delta_of(1, m)[levels - 1 :]
        x_state = jnp.where(here, spread(line(m)), x_state)
        x_delta = jnp.where(here, spread(line(tracers + m)), x_delta)
        x_below = jnp.where(here, spread(jnp.where(has_next, final, outer)), x_below)
        x_above = jnp.where(here, spread(jnp.where(has_next, outer, first)), x_above)
        x_kappa = jnp.where(here, kappa[m], x_kappa)
    x_tangent = tangent_of(x_delta, 2.0 * x_kappa * x_state, x_below, x_above)

    def beside(halves, edge):
        lo, hi = halves
        lo_below = jnp.where(has_prev, edge, 0.0)
        hi_above = jnp.where(has_next, edge, 0.0)
        below = (
            jnp.where(sub == 0, spread(lo_below), pltpu.roll(lo, 1, axis=0)),
            jnp.where(sub == 0, spread(lo[levels - 1 :]), pltpu.roll(hi, 1, axis=0)),
        )
        above = (
            jnp.where(sub == levels - 1, spread(hi[:1]), pltpu.roll(lo, levels - 1, axis=0)),
            jnp.where(sub == levels - 1, spread(hi_above), pltpu.roll(hi, levels - 1, axis=0)),
        )
        return below, above

    for m in range(tracers):
        deltas = (delta_of(0, m), delta_of(1, m))
        losses = tuple(2.0 * kappa[m] * state_of(h, m) for h in range(2))
        below, above = beside(deltas, x_delta[m : m + 1])
        tangents = tuple(tangent_of(deltas[h], losses[h], below[h], above[h]) for h in range(2))
        tangent_out[m] = jnp.where(ids[0] == 0, tangents[0][:, :cols], tangents[1][:, :cols])
        t_below, t_above = beside(tangents, x_tangent[m : m + 1])
        for h in range(2):
            tangent = tangents[h]
            flux = courant * tangent
            arrived = jnp.zeros_like(tangent)
            for s in shifts:
                arrived = arrived + turned(jnp.where(picked[s], flux, 0.0), s)
            adjoint = (keep - losses[h]) * tangent + arrived + rising * t_above[h] + sinking * t_below[h]
            at = h * main + m * levels
            adj[at : at + levels, :cols] = adjoint[:, :cols]
            adj[at : at + levels, cols:] = adjoint[:, :span]
    for j in range(rounds):
        first = pl.multiple_of(ids[IDS + rounds + j] * span, LANE)
        windows_out[j][...] = adj[:, pl.ds(first, 2 * span)].astype(jnp.bfloat16)


def stencil(ids, kappa, pieces, courant, vertical, offset, tracers, levels, reach, unscale, tail):
    rows = pieces[0].shape[0]
    rounds = len(pieces) // 2
    cols = courant.shape[1]
    span = cols // reach
    return pl.pallas_call(
        functools.partial(stencil_kernel, unscale, tail, rounds, reach),
        in_specs=[SMEM] * 2 + [VMEM] * (2 * rounds + 3),
        out_specs=[VMEM] * (1 + rounds),
        out_shape=[jax.ShapeDtypeStruct((tracers, levels, cols), jnp.float32)]
        + [jax.ShapeDtypeStruct((2 * tracers * levels, 2 * span), jnp.bfloat16)] * rounds,
        scratch_shapes=[
            pltpu.VMEM((rows, cols + LANE), jnp.float32),
            pltpu.VMEM((LANE, LANE), jnp.float32),
            pltpu.VMEM((2 * tracers * levels, cols + span), jnp.float32),
        ],
        compiler_params=pltpu.CompilerParams(vmem_limit_bytes=24 << 20),
        cost_estimate=cost(100 * rows * cols, 8 * rows * cols),
        name="stencil",
    )(ids, kappa, *pieces, courant, vertical, offset)


def backward_kernel(ids, counts, *refs):
    reach = counts.shape[1]
    pieces = refs[:-3]
    weight, mine, theirs = refs[-3:]
    tracers, levels, cols = mine.shape
    main = tracers * levels
    slots = weight.shape[-1]
    window = slots + LANE
    mine[...] = jnp.zeros_like(mine)
    theirs[...] = jnp.zeros_like(theirs)
    for j, piece in enumerate(pieces):
        group = ids[IDS + j]
        grad = jnp.dot(piece[...], weight[j], preferred_element_type=jnp.float32)
        lane = lax.broadcasted_iota(jnp.int32, grad.shape, 1)
        grad = jnp.where(lane < counts[0, group], grad, 0.0)
        grad = jnp.concatenate([grad, jnp.zeros((2 * main, LANE), jnp.float32)], axis=1)
        base, shift = place(counts, group, reach, window, cols)
        grad = pltpu.roll(grad, shift, axis=1)
        own = jnp.where(ids[0] == 0, grad[:main], grad[main:])
        other = jnp.where(ids[0] == 0, grad[main:], grad[:main])
        for m in range(tracers):
            part = slice(m * levels, (m + 1) * levels)
            mine[m, :, pl.ds(base, window)] += own[part]
            theirs[m, :, pl.ds(base, window)] += other[part]


def backward(ids, counts, pieces, weight, tracers, levels, cols):
    rounds, win, slots = weight.shape
    out = jax.ShapeDtypeStruct((tracers, levels, cols), jnp.float32)
    return pl.pallas_call(
        backward_kernel,
        in_specs=[SMEM, SMEM] + [VMEM] * (rounds + 1),
        out_specs=[VMEM, VMEM],
        out_shape=[out, out],
        compiler_params=pltpu.CompilerParams(vmem_limit_bytes=12 << 20),
        cost_estimate=cost(4 * rounds * tracers * levels * win * slots, 2 * weight.size),
        name="remap_back",
    )(ids, counts, *pieces, weight)


def plan(tiles, slabs, reach):
    rounds = reach // 2
    centre = reach // 2
    cube = tiles == reach and tiles & (tiles - 1) == 0
    routes = []
    if cube:
        flips = np.array([[2 * j + 1 for j in range(rounds)], [2 * j + 2 for j in range(rounds - 1)] + [0]])
        target = lambda t, c, j: t ^ int(flips[c, j])
    else:
        steps = np.array([[-centre + j for j in range(rounds)], [centre - 1 - j for j in range(rounds)]])
        target = lambda t, c, j: (t + int(steps[c, j])) % tiles
    for j in range(rounds):
        routes.append(
            [(t * slabs + v, target(t, v % 2, j) * slabs + v) for t in range(tiles) for v in range(slabs)]
        )
    tile, core = lax.axis_index("tile"), lax.axis_index("lev") % 2
    if cube:
        def groups(core, sign):
            other = tile ^ jnp.where(core == 0, jnp.asarray(flips[0]), jnp.asarray(flips[1]))
            return (sign * (other - tile) + centre + reach) % reach
    else:
        def groups(core, sign):
            return centre + jnp.where(core == 0, jnp.asarray(steps[0]), jnp.asarray(steps[1]))
    pair = lax.axis_index("lev") // 2
    flags = jnp.stack([core, pair > 0, pair < slabs // 2 - 1])
    ids = [flags, groups(core, 1), groups(core, -1), groups(1 - core, -1)]
    return routes, jnp.concatenate([part.astype(jnp.int32) for part in ids])


def shards(trajectory, increment, counts, remap_weight, kappa, courant, vertical, offset):
    tracers, levels, cols = trajectory.shape
    reach, _, slots = remap_weight.shape[1:]
    tiles, slabs = lax.axis_size("tile"), lax.axis_size("lev")
    if slabs not in (2, 4) or reach % 2:
        raise ValueError("unsupported mesh")
    both = ("tile", "lev")
    routes, ids = plan(tiles, slabs, reach)
    rounds = len(routes)
    scale = send_scale(slots)
    tail = 4 * tracers * levels + EDGE * tracers
    rows = -(-(tail + COEFS) // SUB) * SUB

    swap = [(v, v ^ 1) for v in range(slabs)]
    near = [(v, v + 1 if v % 2 else v - 1) for v in range(slabs)]
    far = [(v, v + 2 if v % 2 else v - 2) for v in range(slabs)]
    near, far = ([(a, b) for a, b in way if 0 <= b < slabs] for way in (near, far))
    traj_too = lax.ppermute(trajectory, "lev", swap)
    inc_too = lax.ppermute(increment, "lev", swap)
    last = jnp.concatenate([trajectory[:, -1], increment[:, -1], increment[:, -2]])
    first = jnp.concatenate([trajectory[:, 0], increment[:, 0], increment[:, 1]])
    border = jnp.where(lax.axis_index("lev") % 2 == 1, last, first)
    ext = lax.ppermute(border, "lev", near)
    ext_too = lax.ppermute(border, "lev", far)

    traj_own, inc_own, w, w_low, w_high = load(ids, trajectory, increment, remap_weight, rounds)
    lines = [x.reshape(1, cols) for x in (courant, vertical, offset)]
    rows_in = gather(ids, traj_own, inc_own, traj_too, inc_too, ext, ext_too, rows)
    pieces, message_0 = [], None
    for j, route in enumerate(routes):
        message = forward(j, ids, counts, rows_in, *lines, w, w_low, w_high, scale, tail)
        message = message.astype(jnp.float16)
        message_0 = message_0 if j else message
        pieces.append(lax.ppermute(message, both, route))
    if tiles != reach:
        hops = (reach // 2, -(reach // 2) - 1)
        route = [(t * slabs + v, (t + hops[v % 2]) % tiles * slabs + v) for t in range(tiles) for v in range(slabs)]
        corner = lax.ppermute(message_0[tail:, : 2 * LANE], both, route)
        low_half = lax.broadcasted_iota(jnp.int32, corner.shape, 1) < LANE
        fresh = low_half == (lax.axis_index("lev") % 2 == 0)
        pieces[0] = pieces[0].at[tail:, : 2 * LANE].set(
            jnp.where(fresh, corner, pieces[0][tail:, : 2 * LANE])
        )
    others = [lax.ppermute(piece, "lev", swap) for piece in pieces]
    whole = [piece.astype(jnp.float32) for piece in pieces + others]

    tangent, *windows = stencil(
        ids, kappa, whole, *lines, tracers, levels, reach, 1.0 / scale, tail
    )
    returned = [
        lax.ppermute(window, both, [(b, a) for a, b in route]) for window, route in zip(windows, routes)
    ]
    mine, theirs = backward(ids, counts, returned, w, tracers, levels, cols)
    return (tangent, mine + lax.ppermute(theirs, "lev", swap))


def solution(mesh):
    return jax.shard_map(
        shards,
        mesh=mesh,
        in_specs=(
            P(None, "lev", "tile"),
            P(None, "lev", "tile"),
            P("tile", None),
            P("tile", None, None, None),
            P(),
            P("tile"),
            P("tile"),
            P("tile"),
        ),
        out_specs=(P(None, "lev", "tile"), P(None, "lev", "tile")),
        check_vma=False,
    )
```

```python
import functools

import jax
import jax.numpy as jnp
from jax import lax
from jax.experimental import pallas as pl
from jax.experimental.pallas import tpu as pltpu
from jax.sharding import PartitionSpec as P

HALO = 2
LANE = 128
SUB = 8
EDGE = 3
COEFS = 5
VALUE_MAX = 6.0
WEIGHT_MAX = 0.25
F16_MAX = 65504.0


VMEM = pl.BlockSpec(memory_space=pltpu.VMEM)
SMEM = pl.BlockSpec(memory_space=pltpu.SMEM)
HBM = pl.BlockSpec(memory_space=pltpu.HBM)


def send_scale(slot_count):
    bound = VALUE_MAX * WEIGHT_MAX * slot_count
    scale = 1.0
    while 2.0 * scale * bound < F16_MAX:
        scale *= 2.0
    while scale * bound >= F16_MAX:
        scale *= 0.5
    return scale


def cost(flops, moved):
    return pl.CostEstimate(flops=flops, bytes_accessed=moved, transcendentals=0)


def place(counts, which, reach, window, cols):
    begin = jnp.int32(0)
    for other in range(reach):
        begin = begin + jnp.where(other < which, counts[0, other], 0)
    base = jnp.minimum((begin // LANE) * LANE, cols - window)
    return pl.multiple_of(base, LANE), begin - base


class Plan:
    def __init__(self, tiles, slabs, reach):
        self.tiles, self.slabs, self.reach = tiles, slabs, reach
        self.rounds = reach // 2
        self.cube = tiles == reach and tiles & (tiles - 1) == 0
        if self.cube:
            self.hops = [list(range(reach - 1, 0, -2)), list(range(reach - 2, -1, -2))]
        else:
            self.hops = [list(range(-(reach // 2), 0)), list(range(reach // 2 - 1, -1, -1))]

    def target(self, tile, core, j):
        hop = self.hops[core][j]
        return tile ^ hop if self.cube else (tile + hop) % self.tiles

    def route(self, j):
        cells = [(t, v) for t in range(self.tiles) for v in range(self.slabs)]
        return [(t * self.slabs + v, self.target(t, v % 2, j) * self.slabs + v) for t, v in cells]

    def core(self):
        return lax.rem(lax.axis_index("lev"), 2)

    def has_next(self):
        return lax.axis_index("lev") < self.slabs - 2

    def has_prev(self):
        return lax.axis_index("lev") >= 2

    def group(self, core, j, sign):
        hop = jnp.where(core == 0, jnp.int32(self.hops[0][j]), jnp.int32(self.hops[1][j]))
        centre = self.reach // 2
        if not self.cube:
            return centre + hop
        tile = lax.axis_index("tile")
        return lax.rem(sign * ((tile ^ hop) - tile) + centre + self.reach, self.reach)

    def sent(self, j):
        return self.group(self.core(), j, 1)

    def taken(self, k):
        own = k < self.rounds
        return self.group(self.core() if own else 1 - self.core(), k % self.rounds, -1)


def border_kernel(plan, traj, inc, traj_out, inc_out, border, sems):
    copies = [
        pltpu.make_async_copy(traj, traj_out, sems.at[0]),
        pltpu.make_async_copy(inc, inc_out, sems.at[1]),
    ]
    for copy in copies:
        copy.start()
    for copy in copies:
        copy.wait()
    tracers, levels, _ = traj_out.shape
    lower = plan.core() == 1
    row = 0
    for ref, depth in ((traj_out, 0), (inc_out, 0), (inc_out, 1)):
        for m in range(tracers):
            x = ref[m].astype(jnp.float32)
            low, high = levels - 1 - depth, depth
            line = jnp.where(lower, x[low : low + 1], x[high : high + 1])
            border[row : row + 1, :] = line.astype(border.dtype)
            row += 1


def fetch_border(plan, traj, inc):
    tracers, _, cols = traj.shape
    like = lambda *shape: jax.ShapeDtypeStruct(shape, traj.dtype)
    return pl.pallas_call(
        functools.partial(border_kernel, plan),
        in_specs=[HBM] * 2,
        out_specs=[VMEM] * 3,
        out_shape=[like(*traj.shape), like(*inc.shape), like(EDGE * tracers, cols)],
        scratch_shapes=[pltpu.SemaphoreType.DMA((2,))],
        compiler_params=pltpu.CompilerParams(vmem_limit_bytes=4 << 20),
        cost_estimate=cost(0, 8 * traj.size),
        name="border",
    )(traj, inc)


def load_kernel(plan, weight, w_out, w_low, w_high, sems):
    reach, win = weight.shape[1:3]
    half = win // 2
    copies = []
    for j in range(plan.rounds):
        group = plan.sent(j)
        low = lax.rem(group + reach - 1, reach)
        high = lax.rem(group + 1, reach)
        low_at = pl.multiple_of(jnp.where(group == 0, half, win) - SUB, SUB)
        high_at = pl.multiple_of(jnp.where(group == reach - 2, half, 0), SUB)
        copies.append(pltpu.make_async_copy(weight.at[0, group], w_out.at[j], sems.at[3 * j]))
        copies.append(
            pltpu.make_async_copy(
                weight.at[0, low, pl.ds(low_at, SUB)], w_low.at[j], sems.at[1 + 3 * j]
            )
        )
        copies.append(
            pltpu.make_async_copy(
                weight.at[0, high, pl.ds(high_at, SUB)], w_high.at[j], sems.at[2 + 3 * j]
            )
        )
    for copy in copies:
        copy.start()
    for copy in copies:
        copy.wait()


def load(plan, weight):
    _, _, win, slots = weight.shape
    like = lambda *shape: jax.ShapeDtypeStruct(shape, weight.dtype)
    return pl.pallas_call(
        functools.partial(load_kernel, plan),
        in_specs=[HBM],
        out_specs=[VMEM] * 3,
        out_shape=[
            like(plan.rounds, win, slots),
            like(plan.rounds, SUB, slots),
            like(plan.rounds, SUB, slots),
        ],
        scratch_shapes=[pltpu.SemaphoreType.DMA((3 * plan.rounds,))],
        compiler_params=pltpu.CompilerParams(vmem_limit_bytes=8 << 20),
        cost_estimate=cost(0, 4 * plan.rounds * win * slots),
        name="fetch",
    )(weight)


def gather_kernel(plan, traj, inc, traj_too, inc_too, ext, ext_too, rows_out):
    tracers, levels, _ = traj.shape
    main = tracers * levels
    mine = pl.multiple_of(plan.core() * 2 * main, SUB)
    theirs = pl.multiple_of((1 - plan.core()) * 2 * main, SUB)
    for m in range(tracers):
        for at, t, i in ((mine, traj, inc), (theirs, traj_too, inc_too)):
            rows_out[pl.ds(at + m * levels, levels), :] = t[m].astype(jnp.float32)
            rows_out[pl.ds(at + main + m * levels, levels), :] = i[m].astype(jnp.float32)
    beyond = ext[...].astype(jnp.float32) + ext_too[...].astype(jnp.float32)
    rows_out[4 * main :, :] = jnp.zeros_like(rows_out[4 * main :, :])
    rows_out[4 * main : 4 * main + EDGE * tracers, :] = beyond


def gather(plan, traj, inc, traj_too, inc_too, ext, ext_too, rows):
    cols = traj.shape[-1]
    return pl.pallas_call(
        functools.partial(gather_kernel, plan),
        in_specs=[VMEM] * 6,
        out_specs=VMEM,
        out_shape=jax.ShapeDtypeStruct((rows, cols), jnp.float32),
        compiler_params=pltpu.CompilerParams(vmem_limit_bytes=8 << 20),
        cost_estimate=cost(0, 6 * rows * cols),
        name="gather",
    )(traj, inc, traj_too, inc_too, ext, ext_too)


def forward_kernel(plan, which, scale, tail, counts, rows_in, courant, vertical, offset, w, w_low, w_high, out):
    reach = counts.shape[1]
    rows, cols = rows_in.shape
    slots = w.shape[-1]
    window = slots + LANE
    contract = (((1,), (1,)), ((), ()))

    def slotted(group):
        base, shift = place(counts, group, reach, window, cols)
        x = rows_in[:, pl.ds(base, window)]
        x = pltpu.roll(x, lax.rem(window - shift, window), axis=1)[:, :slots]
        lane = lax.broadcasted_iota(jnp.int32, x.shape, 1)
        return jnp.where(lane < counts[0, group], x, 0.0).astype(jnp.bfloat16)

    group = plan.sent(which)
    y = slotted(group)
    out[...] = scale * lax.dot_general(y, w[which], contract, preferred_element_type=jnp.float32)
    for part, at in enumerate((cols - LANE, 0)):
        span = slice((2 + part) * LANE, (3 + part) * LANE)
        for row, ref in ((0, courant), (2, vertical)):
            value = ref[:, at : at + LANE]
            top = value.astype(jnp.bfloat16).astype(jnp.float32)
            out[tail + row : tail + row + 1, span] = scale * top
            out[tail + row + 1 : tail + row + 2, span] = scale * (value - top)
        out[tail + 4 : tail + 5, span] = scale * offset[:, at : at + LANE].astype(jnp.float32)

    @pl.when((group == 0) | (group == reach - 1))
    def _():
        z = slotted(lax.rem(group + reach - 1, reach))
        e = scale * lax.dot_general(w_low[which], z, contract, preferred_element_type=jnp.float32)
        out[tail : tail + 2 * HALO, :rows] = e[SUB - 2 * HALO :]

    @pl.when((group == reach - 2) | (group == reach - 1))
    def _():
        z = slotted(lax.rem(group + 1, reach))
        e = scale * lax.dot_general(w_high[which], z, contract, preferred_element_type=jnp.float32)
        out[tail : tail + 2 * HALO, LANE : LANE + rows] = e[: 2 * HALO]


def forward(plan, which, counts, rows_in, courant, vertical, offset, w, w_low, w_high, scale, tail):
    rows = rows_in.shape[0]
    win, slots = w.shape[1:]
    return pl.pallas_call(
        functools.partial(forward_kernel, plan, which, scale, tail),
        in_specs=[SMEM] + [VMEM] * 7,
        out_specs=VMEM,
        out_shape=jax.ShapeDtypeStruct((rows, win), jnp.float32),
        compiler_params=pltpu.CompilerParams(vmem_limit_bytes=8 << 20),
        cost_estimate=cost(2 * rows * win * slots, 4 * rows_in.size),
    )(counts, rows_in, courant, vertical, offset, w, w_low, w_high)


def stencil_kernel(plan, unscale, tail, kappa, *refs):
    rounds, reach = plan.rounds, plan.reach
    pieces = refs[: 2 * rounds]
    courant_in, vertical_in, offset_in, tangent_out = refs[2 * rounds : 2 * rounds + 4]
    windows_out = refs[2 * rounds + 4 : 3 * rounds + 4]
    acc, turn, adj = refs[3 * rounds + 4 :]
    tracers, levels, cols = tangent_out.shape
    main = tracers * levels
    rows = acc.shape[0]
    span = cols // reach
    wide = cols + LANE

    acc[...] = jnp.zeros_like(acc)
    low = jnp.zeros((2 * HALO, LANE), jnp.float32)
    high = jnp.zeros((2 * HALO, LANE), jnp.float32)
    c_low = jnp.zeros((COEFS, LANE), jnp.float32)
    c_high = jnp.zeros((COEFS, LANE), jnp.float32)
    for k, piece in enumerate(pieces):
        group = plan.taken(k)
        first = pl.multiple_of(group * span, LANE)
        second = pl.multiple_of(lax.rem(group + 1, reach) * span, LANE)
        acc[:, pl.ds(first, span)] += unscale * piece[:, :span]
        acc[:, pl.ds(second, span)] += unscale * piece[:, span:]
        is_low = (group == 0) | (group == reach - 1)
        is_high = (group == reach - 2) | (group == reach - 1)
        low = low + jnp.where(is_low, piece[tail : tail + 2 * HALO, :LANE], 0.0)
        high = high + jnp.where(is_high, piece[tail : tail + 2 * HALO, LANE : 2 * LANE], 0.0)
        c_low = jnp.where(group == reach // 2 + 1, piece[tail : tail + COEFS, 2 * LANE : 3 * LANE], c_low)
        c_high = jnp.where(group == reach // 2 - 1, piece[tail : tail + COEFS, 3 * LANE :], c_high)
    turn[...] = jnp.zeros_like(turn)
    turn[: 2 * HALO, :] = unscale * high
    turn[LANE - 2 * HALO :, :] = unscale * low
    acc[:, cols:] = turn[...].T[:rows, :]

    lane = lax.broadcasted_iota(jnp.int32, (COEFS, LANE), 1)
    beyond = unscale * jnp.where(lane < LANE // 2, c_high, c_low)
    spread = lambda row: jnp.broadcast_to(row, (SUB, wide))
    row_of = lambda ref, extra: spread(jnp.concatenate([ref[...].astype(jnp.float32), extra], axis=1))
    courant = row_of(courant_in, beyond[0:1] + beyond[1:2])
    vertical = row_of(vertical_in, beyond[2:3] + beyond[3:4])
    offset = row_of(offset_in, beyond[4:5])
    rising = jnp.maximum(vertical, 0.0)
    sinking = jnp.maximum(-vertical, 0.0)
    shifts = range(-HALO, HALO + 1)
    picked = {s: offset == jnp.float32(s) for s in shifts}
    turned = lambda x, by: x if by % wide == 0 else pltpu.roll(x, by % wide, axis=1)
    keep = 1.0 - courant - rising - sinking

    def tangent_of(delta, loss, below, above):
        departed = jnp.zeros_like(delta)
        for s in shifts:
            departed = jnp.where(picked[s], turned(delta, -s), departed)
        return (keep - loss) * delta + courant * departed + rising * below + sinking * above

    sub = lax.broadcasted_iota(jnp.int32, (SUB, wide), 0)
    has_prev, has_next = plan.has_prev(), plan.has_next()
    state_of = lambda h, m: acc[2 * h * main + m * levels : 2 * h * main + (m + 1) * levels, :]
    delta_of = lambda h, m: acc[(2 * h + 1) * main + m * levels : (2 * h + 1) * main + (m + 1) * levels, :]
    line = lambda r: acc[4 * main + r : 4 * main + r + 1, :]
    x_state = jnp.zeros((SUB, wide), jnp.float32)
    x_delta, x_below, x_above, x_kappa = x_state, x_state, x_state, x_state
    for m in range(tracers):
        here = sub == m
        outer = line(2 * tracers + m)
        first = delta_of(0, m)[:1]
        final = delta_of(1, m)[levels - 1 :]
        x_state = jnp.where(here, spread(line(m)), x_state)
        x_delta = jnp.where(here, spread(line(tracers + m)), x_delta)
        x_below = jnp.where(here, spread(jnp.where(has_next, final, outer)), x_below)
        x_above = jnp.where(here, spread(jnp.where(has_next, outer, first)), x_above)
        x_kappa = jnp.where(here, kappa[m], x_kappa)
    x_tangent = tangent_of(x_delta, 2.0 * x_kappa * x_state, x_below, x_above)

    def beside(halves, edge):
        lo, hi = halves
        lo_below = jnp.where(has_prev, edge, 0.0)
        hi_above = jnp.where(has_next, edge, 0.0)
        below = (
            jnp.where(sub == 0, spread(lo_below), pltpu.roll(lo, 1, axis=0)),
            jnp.where(sub == 0, spread(lo[levels - 1 :]), pltpu.roll(hi, 1, axis=0)),
        )
        above = (
            jnp.where(sub == levels - 1, spread(hi[:1]), pltpu.roll(lo, levels - 1, axis=0)),
            jnp.where(sub == levels - 1, spread(hi_above), pltpu.roll(hi, levels - 1, axis=0)),
        )
        return below, above

    for m in range(tracers):
        deltas = (delta_of(0, m), delta_of(1, m))
        losses = tuple(2.0 * kappa[m] * state_of(h, m) for h in range(2))
        below, above = beside(deltas, x_delta[m : m + 1])
        tangents = tuple(tangent_of(deltas[h], losses[h], below[h], above[h]) for h in range(2))
        tangent_out[m] = jnp.where(plan.core() == 0, tangents[0][:, :cols], tangents[1][:, :cols])
        t_below, t_above = beside(tangents, x_tangent[m : m + 1])
        for h in range(2):
            tangent = tangents[h]
            flux = courant * tangent
            arrived = jnp.zeros_like(tangent)
            for s in shifts:
                arrived = arrived + turned(jnp.where(picked[s], flux, 0.0), s)
            adjoint = (keep - losses[h]) * tangent + arrived + rising * t_above[h] + sinking * t_below[h]
            at = h * main + m * levels
            adj[at : at + levels, :cols] = adjoint[:, :cols]
            adj[at : at + levels, cols:] = adjoint[:, :span]
    for j in range(rounds):
        first = pl.multiple_of(plan.taken(j) * span, LANE)
        windows_out[j][...] = adj[:, pl.ds(first, 2 * span)].astype(jnp.bfloat16)


def stencil(plan, kappa, pieces, courant, vertical, offset, tracers, levels, unscale, tail):
    rows = pieces[0].shape[0]
    rounds = plan.rounds
    cols = courant.shape[1]
    span = cols // plan.reach
    return pl.pallas_call(
        functools.partial(stencil_kernel, plan, unscale, tail),
        in_specs=[SMEM] + [VMEM] * (2 * rounds + 3),
        out_specs=[VMEM] * (1 + rounds),
        out_shape=[jax.ShapeDtypeStruct((tracers, levels, cols), jnp.float32)]
        + [jax.ShapeDtypeStruct((2 * tracers * levels, 2 * span), jnp.bfloat16)] * rounds,
        scratch_shapes=[
            pltpu.VMEM((rows, cols + LANE), jnp.float32),
            pltpu.VMEM((LANE, LANE), jnp.float32),
            pltpu.VMEM((2 * tracers * levels, cols + span), jnp.float32),
        ],
        compiler_params=pltpu.CompilerParams(vmem_limit_bytes=24 << 20),
        cost_estimate=cost(100 * rows * cols, 8 * rows * cols),
        name="stencil",
    )(kappa, *pieces, courant, vertical, offset)


def backward_kernel(plan, counts, *refs):
    reach = counts.shape[1]
    pieces = refs[:-3]
    weight, mine, theirs = refs[-3:]
    tracers, levels, cols = mine.shape
    main = tracers * levels
    slots = weight.shape[-1]
    window = slots + LANE
    mine[...] = jnp.zeros_like(mine)
    theirs[...] = jnp.zeros_like(theirs)
    for j, piece in enumerate(pieces):
        group = plan.sent(j)
        grad = jnp.dot(piece[...], weight[j], preferred_element_type=jnp.float32)
        lane = lax.broadcasted_iota(jnp.int32, grad.shape, 1)
        grad = jnp.where(lane < counts[0, group], grad, 0.0)
        grad = jnp.concatenate([grad, jnp.zeros((2 * main, LANE), jnp.float32)], axis=1)
        base, shift = place(counts, group, reach, window, cols)
        grad = pltpu.roll(grad, shift, axis=1)
        own = jnp.where(plan.core() == 0, grad[:main], grad[main:])
        other = jnp.where(plan.core() == 0, grad[main:], grad[:main])
        for m in range(tracers):
            part = slice(m * levels, (m + 1) * levels)
            mine[m, :, pl.ds(base, window)] += own[part]
            theirs[m, :, pl.ds(base, window)] += other[part]


def backward(plan, counts, pieces, weight, tracers, levels, cols):
    rounds, win, slots = weight.shape
    out = jax.ShapeDtypeStruct((tracers, levels, cols), jnp.float32)
    return pl.pallas_call(
        functools.partial(backward_kernel, plan),
        in_specs=[SMEM] + [VMEM] * (rounds + 1),
        out_specs=[VMEM, VMEM],
        out_shape=[out, out],
        compiler_params=pltpu.CompilerParams(vmem_limit_bytes=12 << 20),
        cost_estimate=cost(4 * rounds * tracers * levels * win * slots, 2 * weight.size),
        name="remap_back",
    )(counts, *pieces, weight)


def step(trajectory, increment, counts, remap_weight, kappa, courant, vertical, offset):
    tracers, levels, cols = trajectory.shape
    reach, _, slots = remap_weight.shape[1:]
    tiles, slabs = lax.axis_size("tile"), lax.axis_size("lev")
    if slabs not in (2, 4) or reach % 2:
        raise ValueError("unsupported mesh")
    both = ("tile", "lev")
    plan = Plan(tiles, slabs, reach)
    routes = [plan.route(j) for j in range(plan.rounds)]
    scale = send_scale(slots)
    tail = 4 * tracers * levels + EDGE * tracers
    rows = -(-(tail + COEFS) // SUB) * SUB

    swap = [(v, v ^ 1) for v in range(slabs)]
    near = [(v, v + 1 if v % 2 else v - 1) for v in range(slabs)]
    far = [(v, v + 2 if v % 2 else v - 2) for v in range(slabs)]
    near, far = ([(a, b) for a, b in way if 0 <= b < slabs] for way in (near, far))
    traj_too = lax.ppermute(trajectory, "lev", swap)
    inc_too = lax.ppermute(increment, "lev", swap)
    traj_own, inc_own, border = fetch_border(plan, trajectory, increment)
    ext = lax.ppermute(border, "lev", near)
    ext_too = lax.ppermute(border, "lev", far)

    w, w_low, w_high = load(plan, remap_weight)
    lines = [x.reshape(1, cols) for x in (courant, vertical, offset)]
    rows_in = gather(plan, traj_own, inc_own, traj_too, inc_too, ext, ext_too, rows)
    pieces, message_0 = [], None
    for j, route in enumerate(routes):
        message = forward(plan, j, counts, rows_in, *lines, w, w_low, w_high, scale, tail)
        message = message.astype(jnp.float16)
        message_0 = message_0 if j else message
        pieces.append(lax.ppermute(message, both, route))
    if tiles != reach:
        hops = (reach // 2, -(reach // 2) - 1)
        route = [(t * slabs + v, (t + hops[v % 2]) % tiles * slabs + v) for t in range(tiles) for v in range(slabs)]
        corner = lax.ppermute(message_0[tail:, : 2 * LANE], both, route)
        low_half = lax.broadcasted_iota(jnp.int32, corner.shape, 1) < LANE
        fresh = low_half == (lax.axis_index("lev") % 2 == 0)
        pieces[0] = pieces[0].at[tail:, : 2 * LANE].set(
            jnp.where(fresh, corner, pieces[0][tail:, : 2 * LANE])
        )
    others = []
    for piece in pieces:
        others.append(lax.ppermute(piece, "lev", swap))
    whole = [piece.astype(jnp.float32) for piece in pieces + others]

    tangent, *windows = stencil(plan, kappa, whole, *lines, tracers, levels, 1.0 / scale, tail)
    returned = []
    for window, route in zip(windows, routes):
        returned.append(lax.ppermute(window, both, [(b, a) for a, b in route]))
    mine, theirs = backward(plan, counts, returned, w, tracers, levels, cols)
    return (tangent, mine + lax.ppermute(theirs, "lev", swap))


def solution(mesh):
    return jax.shard_map(
        step,
        mesh=mesh,
        in_specs=(
            P(None, "lev", "tile"),
            P(None, "lev", "tile"),
            P("tile", None),
            P("tile", None, None, None),
            P(),
            P("tile"),
            P("tile"),
            P("tile"),
        ),
        out_specs=(P(None, "lev", "tile"), P(None, "lev", "tile")),
        check_vma=False,
    )
```

```python
import functools

import jax
import jax.numpy as jnp
from jax import lax
from jax.experimental import pallas as pl
from jax.experimental.pallas import tpu as pltpu
from jax.sharding import PartitionSpec as P

HALO = 2
LANE = 128
SUB = 8
EDGE = 3
COEFS = 5
VALUE_MAX = 6.0
WEIGHT_MAX = 0.25
F16_MAX = 65504.0


VMEM = pl.BlockSpec(memory_space=pltpu.VMEM)
SMEM = pl.BlockSpec(memory_space=pltpu.SMEM)
HBM = pl.BlockSpec(memory_space=pltpu.HBM)


def send_scale(slot_count):
    bound = VALUE_MAX * WEIGHT_MAX * slot_count
    scale = 1.0
    while 2.0 * scale * bound < F16_MAX:
        scale *= 2.0
    while scale * bound >= F16_MAX:
        scale *= 0.5
    return scale


def cost(flops, moved):
    return pl.CostEstimate(flops=flops, bytes_accessed=moved, transcendentals=0)


def place(counts, which):
    sizes = counts[...].astype(jnp.float32)
    lane = lax.broadcasted_iota(jnp.int32, sizes.shape, 1)
    begin = jnp.sum(jnp.where(lane < which, sizes, 0.0)).astype(jnp.int32)
    size = jnp.sum(jnp.where(lane == which, sizes, 0.0)).astype(jnp.int32)
    base = pl.multiple_of((begin // LANE) * LANE, LANE)
    return base, begin - base, size


def columns(x):
    return [x[:, at : at + LANE] for at in range(0, x.shape[1], LANE)]


class Plan:
    def __init__(self, tiles, slabs, reach):
        self.tiles, self.slabs, self.reach = tiles, slabs, reach
        self.rounds = reach // 2
        self.cube = tiles == reach and tiles & (tiles - 1) == 0
        if self.cube:
            self.hops = [list(range(reach - 1, 0, -2)), list(range(reach - 2, -1, -2))]
        else:
            self.hops = [list(range(-(reach // 2), 0)), list(range(reach // 2 - 1, -1, -1))]

    def target(self, tile, core, j):
        hop = self.hops[core][j]
        return tile ^ hop if self.cube else (tile + hop) % self.tiles

    def route(self, j):
        cells = [(t, v) for t in range(self.tiles) for v in range(self.slabs)]
        return [(t * self.slabs + v, self.target(t, v % 2, j) * self.slabs + v) for t, v in cells]

    def core(self):
        return lax.rem(lax.axis_index("lev"), 2)

    def has_next(self):
        return lax.axis_index("lev") < self.slabs - 2

    def has_prev(self):
        return lax.axis_index("lev") >= 2

    def group(self, core, j, sign):
        hop = jnp.where(core == 0, jnp.int32(self.hops[0][j]), jnp.int32(self.hops[1][j]))
        centre = self.reach // 2
        if not self.cube:
            return centre + hop
        tile = lax.axis_index("tile")
        return lax.rem(sign * ((tile ^ hop) - tile) + centre + self.reach, self.reach)

    def sent(self, j):
        return self.group(self.core(), j, 1)

    def taken(self, k):
        return self.group(self.owner(k), k % self.rounds, -1)

    def returned(self, k):
        return self.group(self.owner(k), k % self.rounds, 1)

    def owner(self, k):
        return self.core() if k < self.rounds else 1 - self.core()


def border_kernel(plan, traj, inc, traj_out, inc_out, border, sems):
    copies = [
        pltpu.make_async_copy(traj, traj_out, sems.at[0]),
        pltpu.make_async_copy(inc, inc_out, sems.at[1]),
    ]
    for copy in copies:
        copy.start()
    for copy in copies:
        copy.wait()
    tracers, levels, _ = traj_out.shape
    lower = plan.core() == 1
    row = 0
    for ref, depth in ((traj_out, 0), (inc_out, 0), (inc_out, 1)):
        for m in range(tracers):
            x = ref[m].astype(jnp.float32)
            low, high = levels - 1 - depth, depth
            line = jnp.where(lower, x[low : low + 1], x[high : high + 1])
            border[row : row + 1, :] = line.astype(border.dtype)
            row += 1


def fetch_border(plan, traj, inc):
    tracers, _, cols = traj.shape
    like = lambda *shape: jax.ShapeDtypeStruct(shape, traj.dtype)
    return pl.pallas_call(
        functools.partial(border_kernel, plan),
        in_specs=[HBM] * 2,
        out_specs=[VMEM] * 3,
        out_shape=[like(*traj.shape), like(*inc.shape), like(EDGE * tracers, cols)],
        scratch_shapes=[pltpu.SemaphoreType.DMA((2,))],
        compiler_params=pltpu.CompilerParams(vmem_limit_bytes=4 << 20),
        cost_estimate=cost(0, 8 * traj.size),
        name="border",
    )(traj, inc)


def load_kernel(plan, weight, w_out, w_low, w_high, sems):
    reach, win = weight.shape[1:3]
    half = win // 2
    copies = []
    for j in range(plan.rounds):
        group = plan.sent(j)
        low = lax.rem(group + reach - 1, reach)
        high = lax.rem(group + 1, reach)
        low_at = pl.multiple_of(jnp.where(group == 0, half, win) - SUB, SUB)
        high_at = pl.multiple_of(jnp.where(group == reach - 2, half, 0), SUB)
        copies.append(pltpu.make_async_copy(weight.at[0, group], w_out.at[j], sems.at[3 * j]))
        copies.append(
            pltpu.make_async_copy(
                weight.at[0, low, pl.ds(low_at, SUB)], w_low.at[j], sems.at[1 + 3 * j]
            )
        )
        copies.append(
            pltpu.make_async_copy(
                weight.at[0, high, pl.ds(high_at, SUB)], w_high.at[j], sems.at[2 + 3 * j]
            )
        )
    for copy in copies:
        copy.start()
    for copy in copies:
        copy.wait()


def load(plan, weight):
    _, _, win, slots = weight.shape
    like = lambda *shape: jax.ShapeDtypeStruct(shape, weight.dtype)
    return pl.pallas_call(
        functools.partial(load_kernel, plan),
        in_specs=[HBM],
        out_specs=[VMEM] * 3,
        out_shape=[
            like(plan.rounds, win, slots),
            like(plan.rounds, SUB, slots),
            like(plan.rounds, SUB, slots),
        ],
        scratch_shapes=[pltpu.SemaphoreType.DMA((3 * plan.rounds,))],
        compiler_params=pltpu.CompilerParams(vmem_limit_bytes=8 << 20),
        cost_estimate=cost(0, 4 * plan.rounds * win * slots),
        name="fetch",
    )(weight)


def gather_kernel(plan, traj, inc, traj_too, inc_too, ext, ext_too, rows_out):
    tracers, levels, cols = traj.shape
    main = tracers * levels
    mine = pl.multiple_of(plan.core() * 2 * main, SUB)
    theirs = pl.multiple_of((1 - plan.core()) * 2 * main, SUB)
    for m in range(tracers):
        for at, t, i in ((mine, traj, inc), (theirs, traj_too, inc_too)):
            rows_out[pl.ds(at + m * levels, levels), :cols] = t[m].astype(jnp.float32)
            rows_out[pl.ds(at + main + m * levels, levels), :cols] = i[m].astype(jnp.float32)
    rows_out[:, cols:] = jnp.zeros_like(rows_out[:, cols:])
    rows_out[4 * main :, :cols] = jnp.zeros_like(rows_out[4 * main :, :cols])
    beyond = ext[...].astype(jnp.float32) + ext_too[...].astype(jnp.float32)
    rows_out[4 * main : 4 * main + EDGE * tracers, :cols] = beyond


def gather(plan, traj, inc, traj_too, inc_too, ext, ext_too, rows, cols):
    return pl.pallas_call(
        functools.partial(gather_kernel, plan),
        in_specs=[VMEM] * 6,
        out_specs=VMEM,
        out_shape=jax.ShapeDtypeStruct((rows, cols), jnp.float32),
        compiler_params=pltpu.CompilerParams(vmem_limit_bytes=8 << 20),
        cost_estimate=cost(0, 6 * rows * cols),
        name="gather",
    )(traj, inc, traj_too, inc_too, ext, ext_too)


def forward_kernel(plan, which, scale, tail, counts, rows_in, courant, vertical, offset, w, w_low, w_high, out):
    reach, rows, cols = plan.reach, rows_in.shape[0], courant.shape[1]
    slots = w.shape[-1]
    contract = (((1,), (1,)), ((), ()))
    lane = lax.broadcasted_iota(jnp.int32, (rows, LANE), 1)

    def slotted(group):
        base, shift, size = place(counts, group)
        turned = [
            pltpu.roll(x, lax.rem(LANE - shift, LANE), axis=1)
            for x in columns(rows_in[:, pl.ds(base, slots + LANE)])
        ]
        parts = []
        for at, (x, following) in enumerate(zip(turned[:-1], turned[1:])):
            x = jnp.where(lane < LANE - shift, x, following)
            parts.append(jnp.where(lane < size - at * LANE, x, 0.0))
        return jnp.concatenate(parts, axis=1).astype(jnp.bfloat16)

    group = plan.sent(which)
    y = slotted(group)
    out[...] = scale * lax.dot_general(y, w[which], contract, preferred_element_type=jnp.float32)
    for part, at in enumerate((cols - LANE, 0)):
        span = slice((2 + part) * LANE, (3 + part) * LANE)
        for row, ref in ((0, courant), (2, vertical)):
            value = ref[:, at : at + LANE]
            top = value.astype(jnp.bfloat16).astype(jnp.float32)
            out[tail + row : tail + row + 1, span] = scale * top
            out[tail + row + 1 : tail + row + 2, span] = scale * (value - top)
        out[tail + 4 : tail + 5, span] = scale * offset[:, at : at + LANE].astype(jnp.float32)

    @pl.when((group == 0) | (group == reach - 1))
    def _():
        z = slotted(lax.rem(group + reach - 1, reach))
        e = scale * lax.dot_general(w_low[which], z, contract, preferred_element_type=jnp.float32)
        out[tail : tail + 2 * HALO, :rows] = e[SUB - 2 * HALO :]

    @pl.when((group == reach - 2) | (group == reach - 1))
    def _():
        z = slotted(lax.rem(group + 1, reach))
        e = scale * lax.dot_general(w_high[which], z, contract, preferred_element_type=jnp.float32)
        out[tail : tail + 2 * HALO, LANE : LANE + rows] = e[: 2 * HALO]


def forward(plan, which, counts, rows_in, courant, vertical, offset, w, w_low, w_high, scale, tail):
    rows = rows_in.shape[0]
    win, slots = w.shape[1:]
    return pl.pallas_call(
        functools.partial(forward_kernel, plan, which, scale, tail),
        in_specs=[VMEM] * 8,
        out_specs=VMEM,
        out_shape=jax.ShapeDtypeStruct((rows, win), jnp.float32),
        compiler_params=pltpu.CompilerParams(vmem_limit_bytes=8 << 20),
        cost_estimate=cost(2 * rows * win * slots, 4 * rows_in.size),
    )(counts, rows_in, courant, vertical, offset, w, w_low, w_high)


def collect(plan, unscale, tail, numbers, pieces, acc, low, high, c_low, c_high):
    reach = plan.reach
    span = pieces[0].shape[1] // 2
    for k, piece in zip(numbers, pieces):
        group = plan.taken(k)
        first = pl.multiple_of(group * span, LANE)
        second = pl.multiple_of(lax.rem(group + 1, reach) * span, LANE)
        acc[:, pl.ds(first, span)] += unscale * piece[:, :span]
        acc[:, pl.ds(second, span)] += unscale * piece[:, span:]
        is_low = (group == 0) | (group == reach - 1)
        is_high = (group == reach - 2) | (group == reach - 1)
        low = low + jnp.where(is_low, piece[tail : tail + 2 * HALO, :LANE], 0.0)
        high = high + jnp.where(is_high, piece[tail : tail + 2 * HALO, LANE : 2 * LANE], 0.0)
        c_low = jnp.where(group == reach // 2 + 1, piece[tail : tail + COEFS, 2 * LANE : 3 * LANE], c_low)
        c_high = jnp.where(group == reach // 2 - 1, piece[tail : tail + COEFS, 3 * LANE :], c_high)
    return low, high, c_low, c_high


HALO_SLOTS = ((0, 2 * HALO), (SUB, 2 * HALO), (2 * SUB, COEFS), (3 * SUB, COEFS))


def assemble_kernel(plan, unscale, tail, numbers, *refs):
    pieces, (acc, side) = refs[:-2], refs[-2:]
    acc[...] = jnp.zeros_like(acc)
    side[...] = jnp.zeros_like(side)
    blank = [jnp.zeros((size, LANE), jnp.float32) for _, size in HALO_SLOTS]
    halo = collect(plan, unscale, tail, numbers, pieces, acc, *blank)
    for (at, size), part in zip(HALO_SLOTS, halo):
        side[at : at + size, :] = part


def assemble(plan, numbers, pieces, unscale, tail, cols):
    rows = pieces[0].shape[0]
    return pl.pallas_call(
        functools.partial(assemble_kernel, plan, unscale, tail, numbers),
        in_specs=[VMEM] * len(pieces),
        out_specs=[VMEM] * 2,
        out_shape=[
            jax.ShapeDtypeStruct((rows, cols + LANE), jnp.float32),
            jax.ShapeDtypeStruct((4 * SUB, LANE), jnp.float32),
        ],
        compiler_params=pltpu.CompilerParams(vmem_limit_bytes=8 << 20),
        cost_estimate=cost(4 * rows * cols, 8 * rows * cols),
        name="assemble",
    )(*pieces)


def stencil_kernel(plan, unscale, tail, numbers, kappa_in, acc_in, side, *refs):
    rounds, reach = plan.rounds, plan.reach
    pieces = refs[: len(numbers)]
    courant_in, vertical_in, offset_in, tangent_out = refs[len(numbers) : len(numbers) + 4]
    windows_out = refs[len(numbers) + 4 : len(numbers) + 4 + rounds]
    acc, turn, adj = refs[len(numbers) + 4 + rounds :]
    tracers = kappa_in.shape[1]
    levels = tangent_out.shape[0] // (2 * tracers)
    cols = courant_in.shape[1]
    main = tracers * levels
    rows = acc.shape[0]
    span = cols // reach
    wide = cols + LANE

    acc[...] = acc_in[...]
    halo = [side[at : at + size, :] for at, size in HALO_SLOTS]
    low, high, c_low, c_high = collect(plan, unscale, tail, numbers, pieces, acc, *halo)
    turn[...] = jnp.zeros_like(turn)
    turn[: 2 * HALO, :] = unscale * high
    turn[LANE - 2 * HALO :, :] = unscale * low
    acc[:, cols:] = turn[...].T[:rows, :]

    lane = lax.broadcasted_iota(jnp.int32, (COEFS, LANE), 1)
    beyond = unscale * jnp.where(lane < LANE // 2, c_high, c_low)
    spread = lambda row: jnp.broadcast_to(row, (SUB, wide))
    kappa = [jnp.broadcast_to(kappa_in[:, m : m + 1], (SUB, wide)) for m in range(tracers)]
    row_of = lambda ref, extra: spread(jnp.concatenate([ref[...].astype(jnp.float32), extra], axis=1))
    courant = row_of(courant_in, beyond[0:1] + beyond[1:2])
    vertical = row_of(vertical_in, beyond[2:3] + beyond[3:4])
    offset = row_of(offset_in, beyond[4:5])
    rising = jnp.maximum(vertical, 0.0)
    sinking = jnp.maximum(-vertical, 0.0)
    shifts = range(-HALO, HALO + 1)
    picked = {s: offset == jnp.float32(s) for s in shifts}
    turned = lambda x, by: x if by % wide == 0 else pltpu.roll(x, by % wide, axis=1)
    keep = 1.0 - courant - rising - sinking

    def tangent_of(delta, loss, below, above):
        departed = jnp.zeros_like(delta)
        for s in shifts:
            departed = jnp.where(picked[s], turned(delta, -s), departed)
        return (keep - loss) * delta + courant * departed + rising * below + sinking * above

    sub = lax.broadcasted_iota(jnp.int32, (SUB, wide), 0)
    has_prev, has_next = plan.has_prev(), plan.has_next()
    state_of = lambda h, m: acc[2 * h * main + m * levels : 2 * h * main + (m + 1) * levels, :]
    delta_of = lambda h, m: acc[(2 * h + 1) * main + m * levels : (2 * h + 1) * main + (m + 1) * levels, :]
    line = lambda r: acc[4 * main + r : 4 * main + r + 1, :]
    x_state = jnp.zeros((SUB, wide), jnp.float32)
    x_delta, x_below, x_above, x_kappa = x_state, x_state, x_state, x_state
    for m in range(tracers):
        here = sub == m
        outer = line(2 * tracers + m)
        first = delta_of(0, m)[:1]
        final = delta_of(1, m)[levels - 1 :]
        x_state = jnp.where(here, spread(line(m)), x_state)
        x_delta = jnp.where(here, spread(line(tracers + m)), x_delta)
        x_below = jnp.where(here, spread(jnp.where(has_next, final, outer)), x_below)
        x_above = jnp.where(here, spread(jnp.where(has_next, outer, first)), x_above)
        x_kappa = jnp.where(here, kappa[m], x_kappa)
    x_tangent = tangent_of(x_delta, 2.0 * x_kappa * x_state, x_below, x_above)

    def beside(halves, edge):
        lo, hi = halves
        lo_below = jnp.where(has_prev, edge, 0.0)
        hi_above = jnp.where(has_next, edge, 0.0)
        below = (
            jnp.where(sub == 0, spread(lo_below), pltpu.roll(lo, 1, axis=0)),
            jnp.where(sub == 0, spread(lo[levels - 1 :]), pltpu.roll(hi, 1, axis=0)),
        )
        above = (
            jnp.where(sub == levels - 1, spread(hi[:1]), pltpu.roll(lo, levels - 1, axis=0)),
            jnp.where(sub == levels - 1, spread(hi_above), pltpu.roll(hi, levels - 1, axis=0)),
        )
        return below, above

    for m in range(tracers):
        deltas = (delta_of(0, m), delta_of(1, m))
        losses = tuple(2.0 * kappa[m] * state_of(h, m) for h in range(2))
        below, above = beside(deltas, x_delta[m : m + 1])
        tangents = tuple(tangent_of(deltas[h], losses[h], below[h], above[h]) for h in range(2))
        for h in range(2):
            at = h * main + m * levels
            tangent_out[at : at + levels, :] = tangents[h][:, :cols]
        t_below, t_above = beside(tangents, x_tangent[m : m + 1])
        for h in range(2):
            tangent = tangents[h]
            flux = courant * tangent
            arrived = jnp.zeros_like(tangent)
            for s in shifts:
                arrived = arrived + turned(jnp.where(picked[s], flux, 0.0), s)
            adjoint = (keep - losses[h]) * tangent + arrived + rising * t_above[h] + sinking * t_below[h]
            at = h * main + m * levels
            adj[at : at + levels, :cols] = adjoint[:, :cols]
            adj[at : at + levels, cols:] = adjoint[:, :span]
    for j in range(rounds):
        first = pl.multiple_of(plan.taken(j) * span, LANE)
        windows_out[j][...] = adj[:, pl.ds(first, 2 * span)].astype(jnp.bfloat16)


def stencil(plan, kappa, acc, side, numbers, pieces, courant, vertical, offset, levels, unscale, tail):
    rows = pieces[0].shape[0]
    cols = courant.shape[1]
    span = cols // plan.reach
    main = 2 * kappa.shape[1] * levels
    return pl.pallas_call(
        functools.partial(stencil_kernel, plan, unscale, tail, numbers),
        in_specs=[VMEM] * (6 + len(pieces)),
        out_specs=[VMEM] * (1 + plan.rounds),
        out_shape=[jax.ShapeDtypeStruct((main, cols), jnp.float32)]
        + [jax.ShapeDtypeStruct((main, 2 * span), jnp.bfloat16)] * plan.rounds,
        scratch_shapes=[
            pltpu.VMEM((rows, cols + LANE), jnp.float32),
            pltpu.VMEM((LANE, LANE), jnp.float32),
            pltpu.VMEM((main, cols + span), jnp.float32),
        ],
        compiler_params=pltpu.CompilerParams(vmem_limit_bytes=24 << 20),
        cost_estimate=cost(100 * rows * cols, 8 * rows * cols),
        name="stencil",
    )(kappa, acc, side, *pieces, courant, vertical, offset)


def emit_kernel(plan, both, out):
    tracers, levels, _ = out.shape
    at = pl.multiple_of(plan.core() * tracers * levels, SUB)
    for m in range(tracers):
        out[m] = both[pl.ds(at + m * levels, levels), :]


def emit(plan, both, tracers):
    main, cols = both.shape
    return pl.pallas_call(
        functools.partial(emit_kernel, plan),
        in_specs=[VMEM],
        out_specs=VMEM,
        out_shape=jax.ShapeDtypeStruct((tracers, main // 2 // tracers, cols), jnp.float32),
        compiler_params=pltpu.CompilerParams(vmem_limit_bytes=4 << 20),
        cost_estimate=cost(0, 4 * both.size),
        name="emit",
    )(both)


def backward_kernel(plan, last, numbers, counts, weight, *refs):
    pieces = refs[: len(numbers)]
    start = refs[len(numbers)] if last else None
    out = refs[len(numbers) + last]
    acc = refs[-1] if last else out
    slots = weight.shape[-1]
    main = acc.shape[0]
    acc[...] = start[...] if last else jnp.zeros_like(acc)
    lane = lax.broadcasted_iota(jnp.int32, (main, LANE), 1)
    blank = jnp.zeros((main, LANE), jnp.float32)
    for k, piece in zip(numbers, pieces):
        group = plan.returned(k)
        both = piece[...].astype(jnp.float32)
        own = jnp.where(plan.core() == 0, both[:main], both[main:]).astype(jnp.bfloat16)
        grad = jnp.dot(own, weight[0, group], preferred_element_type=jnp.float32)
        base, shift, size = place(counts, group)
        turned = [
            pltpu.roll(jnp.where(lane < size - at * LANE, x, 0.0), shift, axis=1)
            for at, x in enumerate(columns(grad))
        ]
        placed = [
            jnp.where(lane < shift, before, x) for before, x in zip([blank] + turned, turned + [blank])
        ]
        acc[:, pl.ds(base, slots + LANE)] += jnp.concatenate(placed, axis=1)
    if last:
        tracers, levels, cols = out.shape
        for m in range(tracers):
            out[m] = acc[m * levels : (m + 1) * levels, :cols]


def backward(plan, counts, weight, numbers, pieces, start, shape):
    tracers, levels, cols = shape
    slots = weight.shape[-1]
    main = tracers * levels
    last = start is not None
    padded = (main, cols + slots)
    return pl.pallas_call(
        functools.partial(backward_kernel, plan, int(last), numbers),
        in_specs=[VMEM] * (2 + len(pieces) + last),
        out_specs=VMEM,
        out_shape=jax.ShapeDtypeStruct(shape if last else padded, jnp.float32),
        scratch_shapes=[pltpu.VMEM(padded, jnp.float32)] if last else [],
        compiler_params=pltpu.CompilerParams(vmem_limit_bytes=12 << 20),
        cost_estimate=cost(2 * len(pieces) * main * 512 * slots, weight.size),
        name="back_last" if last else "back",
    )(counts, weight, *pieces, *([start] if last else []))


def step(trajectory, increment, counts, remap_weight, kappa, courant, vertical, offset):
    tracers, levels, cols = trajectory.shape
    reach, _, slots = remap_weight.shape[1:]
    tiles, slabs = lax.axis_size("tile"), lax.axis_size("lev")
    if slabs not in (2, 4) or reach % 2:
        raise ValueError("unsupported mesh")
    both = ("tile", "lev")
    plan = Plan(tiles, slabs, reach)
    routes = [plan.route(j) for j in range(plan.rounds)]
    scale = send_scale(slots)
    tail = 4 * tracers * levels + EDGE * tracers
    rows = -(-(tail + COEFS) // SUB) * SUB

    swap = [(v, v ^ 1) for v in range(slabs)]
    near = [(v, v + 1 if v % 2 else v - 1) for v in range(slabs)]
    far = [(v, v + 2 if v % 2 else v - 2) for v in range(slabs)]
    near, far = ([(a, b) for a, b in way if 0 <= b < slabs] for way in (near, far))
    traj_own, inc_own, border = fetch_border(plan, trajectory, increment)
    ext = lax.ppermute(border, "lev", near)
    ext_too = lax.ppermute(border, "lev", far)

    traj_too = lax.ppermute(trajectory, "lev", swap)
    inc_too = lax.ppermute(increment, "lev", swap)

    w, w_low, w_high = load(plan, remap_weight)
    lines = [x.reshape(1, cols) for x in (courant, vertical, offset)]
    rows_in = gather(plan, traj_own, inc_own, traj_too, inc_too, ext, ext_too, rows, cols + slots)
    pieces, message_0 = [], None
    for j, route in enumerate(routes):
        message = forward(plan, j, counts, rows_in, *lines, w, w_low, w_high, scale, tail)
        message = message.astype(jnp.float16)
        message_0 = message_0 if j else message
        pieces.append(lax.ppermute(message, both, route))
    if tiles != reach:
        hops = (reach // 2, -(reach // 2) - 1)
        route = [(t * slabs + v, (t + hops[v % 2]) % tiles * slabs + v) for t in range(tiles) for v in range(slabs)]
        corner = lax.ppermute(message_0[tail:, : 2 * LANE], both, route)
        low_half = lax.broadcasted_iota(jnp.int32, corner.shape, 1) < LANE
        fresh = low_half == (lax.axis_index("lev") % 2 == 0)
        pieces[0] = pieces[0].at[tail:, : 2 * LANE].set(
            jnp.where(fresh, corner, pieces[0][tail:, : 2 * LANE])
        )
    others = []
    for piece in pieces:
        others.append(lax.ppermute(piece, "lev", swap))
    whole = [piece.astype(jnp.float32) for piece in pieces + others]
    final = plan.rounds - 1
    early = [k for k in range(2 * plan.rounds) if k % plan.rounds != final]
    late = [final, plan.rounds + final]
    pick = lambda values, numbers: [values[k] for k in numbers]

    acc, side = assemble(plan, early, pick(whole, early), 1.0 / scale, tail, cols)
    tangents, *windows = stencil(
        plan, kappa.reshape(1, -1), acc, side, late, pick(whole, late), *lines, levels, 1.0 / scale, tail
    )
    returned, regained = [], []
    for window, route in zip(windows, routes):
        returned.append(lax.ppermute(window, both, [(b, a) for a, b in route]))
    for window in returned:
        regained.append(lax.ppermute(window, "lev", swap))
    tangent = emit(plan, tangents, tracers)
    parts = returned + regained
    grad = backward(plan, counts, remap_weight, early, pick(parts, early), None, trajectory.shape)
    grad = backward(plan, counts, remap_weight, late, pick(parts, late), grad, trajectory.shape)
    return (tangent, grad)


def solution(mesh):
    return jax.shard_map(
        step,
        mesh=mesh,
        in_specs=(
            P(None, "lev", "tile"),
            P(None, "lev", "tile"),
            P("tile", None),
            P("tile", None, None, None),
            P(),
            P("tile"),
            P("tile"),
            P("tile"),
        ),
        out_specs=(P(None, "lev", "tile"), P(None, "lev", "tile")),
        check_vma=False,
    )
```

```python
import functools

import jax
import jax.numpy as jnp
from jax import lax
from jax.experimental import pallas as pl
from jax.experimental.pallas import tpu as pltpu
from jax.sharding import PartitionSpec as P

HALO = 2
LANE = 128
SUB = 8
EDGE = 3
COEFS = 5
VALUE_MAX = 6.0
WEIGHT_MAX = 0.25
F16_MAX = 65504.0


VMEM = pl.BlockSpec(memory_space=pltpu.VMEM)
SMEM = pl.BlockSpec(memory_space=pltpu.SMEM)
HBM = pl.BlockSpec(memory_space=pltpu.HBM)


def send_scale(slot_count):
    bound = VALUE_MAX * WEIGHT_MAX * slot_count
    scale = 1.0
    while 2.0 * scale * bound < F16_MAX:
        scale *= 2.0
    while scale * bound >= F16_MAX:
        scale *= 0.5
    return scale


def cost(flops, moved):
    return pl.CostEstimate(flops=flops, bytes_accessed=moved, transcendentals=0)


def place(counts, which):
    sizes = counts[...].astype(jnp.float32)
    lane = lax.broadcasted_iota(jnp.int32, sizes.shape, 1)
    begin = jnp.sum(jnp.where(lane < which, sizes, 0.0)).astype(jnp.int32)
    size = jnp.sum(jnp.where(lane == which, sizes, 0.0)).astype(jnp.int32)
    base = pl.multiple_of((begin // LANE) * LANE, LANE)
    return base, begin - base, size


def columns(x):
    return [x[:, at : at + LANE] for at in range(0, x.shape[1], LANE)]


class Plan:
    def __init__(self, tiles, slabs, reach):
        self.tiles, self.slabs, self.reach = tiles, slabs, reach
        self.rounds = reach // 2
        self.cube = tiles == reach and tiles & (tiles - 1) == 0
        if self.cube:
            self.hops = self.balanced(reach)
        else:
            self.hops = [list(range(-(reach // 2), 0)), list(range(reach // 2 - 1, -1, -1))]

    def balanced(self, reach):
        hops, load = [[], []], [0, 0]
        for flip in range(reach - 1, -1, -1):
            core = 0 if (load[0], len(hops[0])) < (load[1], len(hops[1])) else 1
            core = 1 if flip == 0 or len(hops[0]) == self.rounds else core
            core = 0 if len(hops[1]) == self.rounds - (flip > 0) else core
            hops[core].append(flip)
            load[core] += (flip >> 1) + (flip & 1)
        return hops

    def target(self, tile, core, j):
        hop = self.hops[core][j]
        return tile ^ hop if self.cube else (tile + hop) % self.tiles

    def route(self, j):
        cells = [(t, v) for t in range(self.tiles) for v in range(self.slabs)]
        return [(t * self.slabs + v, self.target(t, v % 2, j) * self.slabs + v) for t, v in cells]

    def core(self):
        return lax.rem(lax.axis_index("lev"), 2)

    def has_next(self):
        return lax.axis_index("lev") < self.slabs - 2

    def has_prev(self):
        return lax.axis_index("lev") >= 2

    def group(self, core, j, sign):
        hop = jnp.where(core == 0, jnp.int32(self.hops[0][j]), jnp.int32(self.hops[1][j]))
        centre = self.reach // 2
        if not self.cube:
            return centre + hop
        tile = lax.axis_index("tile")
        return lax.rem(sign * ((tile ^ hop) - tile) + centre + self.reach, self.reach)

    def sent(self, j):
        return self.group(self.core(), j, 1)

    def taken(self, k):
        return self.group(self.owner(k), k % self.rounds, -1)

    def returned(self, k):
        return self.group(self.owner(k), k % self.rounds, 1)

    def owner(self, k):
        return self.core() if k < self.rounds else 1 - self.core()


def border_kernel(plan, traj, inc, traj_out, inc_out, border, lines, sems):
    copies = [
        pltpu.make_async_copy(traj, traj_out, sems.at[0]),
        pltpu.make_async_copy(inc, inc_out, sems.at[1]),
    ]
    for copy in copies:
        copy.start()
    for copy in copies:
        copy.wait()
    tracers, levels, cols = traj_out.shape
    lower = plan.core() == 1
    row = 0
    for ref, depth in ((traj_out, 0), (inc_out, 0), (inc_out, 1)):
        for m in range(tracers):
            x = ref[m].astype(jnp.float32)
            low, high = levels - 1 - depth, depth
            line = jnp.where(lower, x[low : low + 1], x[high : high + 1])
            if row < SUB:
                lines[row : row + 1, :cols] = line
            else:
                part = cols // SUB
                at = cols + (row - SUB) * part
                for piece in range(SUB):
                    lines[piece : piece + 1, at : at + part] = line[:, piece * part : (piece + 1) * part]
            row += 1
    border[...] = lines[...].astype(border.dtype)


def unpacked(border, count, cols):
    part = cols // SUB
    rows = [border[:, :cols]]
    for row in range(SUB, count):
        at = cols + (row - SUB) * part
        pieces = [border[piece : piece + 1, at : at + part] for piece in range(SUB)]
        rows.append(jnp.concatenate(pieces, axis=1))
    return jnp.concatenate(rows, axis=0)[:count]


def fetch_border(plan, traj, inc):
    tracers, _, cols = traj.shape
    like = lambda *shape: jax.ShapeDtypeStruct(shape, traj.dtype)
    wide = cols + max(0, EDGE * tracers - SUB) * (cols // SUB)
    return pl.pallas_call(
        functools.partial(border_kernel, plan),
        in_specs=[HBM] * 2,
        out_specs=[VMEM] * 3,
        out_shape=[like(*traj.shape), like(*inc.shape), like(SUB, wide)],
        scratch_shapes=[pltpu.VMEM((SUB, wide), jnp.float32), pltpu.SemaphoreType.DMA((2,))],
        compiler_params=pltpu.CompilerParams(vmem_limit_bytes=4 << 20),
        cost_estimate=cost(0, 8 * traj.size),
        name="border",
    )(traj, inc)


def load_kernel(plan, weight, w_out, w_low, w_high, sems):
    reach, win = weight.shape[1:3]
    half = win // 2
    copies = []
    for j in range(plan.rounds):
        group = plan.sent(j)
        low = lax.rem(group + reach - 1, reach)
        high = lax.rem(group + 1, reach)
        low_at = pl.multiple_of(jnp.where(group == 0, half, win) - SUB, SUB)
        high_at = pl.multiple_of(jnp.where(group == reach - 2, half, 0), SUB)
        copies.append(pltpu.make_async_copy(weight.at[0, group], w_out.at[j], sems.at[3 * j]))
        copies.append(
            pltpu.make_async_copy(
                weight.at[0, low, pl.ds(low_at, SUB)], w_low.at[j], sems.at[1 + 3 * j]
            )
        )
        copies.append(
            pltpu.make_async_copy(
                weight.at[0, high, pl.ds(high_at, SUB)], w_high.at[j], sems.at[2 + 3 * j]
            )
        )
    for copy in copies:
        copy.start()
    for copy in copies:
        copy.wait()


def load(plan, weight):
    _, _, win, slots = weight.shape
    like = lambda *shape: jax.ShapeDtypeStruct(shape, weight.dtype)
    return pl.pallas_call(
        functools.partial(load_kernel, plan),
        in_specs=[HBM],
        out_specs=[VMEM] * 3,
        out_shape=[
            like(plan.rounds, win, slots),
            like(plan.rounds, SUB, slots),
            like(plan.rounds, SUB, slots),
        ],
        scratch_shapes=[pltpu.SemaphoreType.DMA((3 * plan.rounds,))],
        compiler_params=pltpu.CompilerParams(vmem_limit_bytes=8 << 20),
        cost_estimate=cost(0, 4 * plan.rounds * win * slots),
        name="fetch",
    )(weight)


def gather_kernel(plan, traj, inc, traj_too, inc_too, ext, ext_too, rows_out):
    tracers, levels, cols = traj.shape
    main = tracers * levels
    mine = pl.multiple_of(plan.core() * 2 * main, SUB)
    theirs = pl.multiple_of((1 - plan.core()) * 2 * main, SUB)
    for m in range(tracers):
        for at, t, i in ((mine, traj, inc), (theirs, traj_too, inc_too)):
            rows_out[pl.ds(at + m * levels, levels), :cols] = t[m].astype(jnp.float32)
            rows_out[pl.ds(at + main + m * levels, levels), :cols] = i[m].astype(jnp.float32)
    rows_out[:, cols:] = jnp.zeros_like(rows_out[:, cols:])
    rows_out[4 * main :, :cols] = jnp.zeros_like(rows_out[4 * main :, :cols])
    beyond = ext[...].astype(jnp.float32) + ext_too[...].astype(jnp.float32)
    rows_out[4 * main : 4 * main + EDGE * tracers, :cols] = unpacked(beyond, EDGE * tracers, cols)


def gather(plan, traj, inc, traj_too, inc_too, ext, ext_too, rows, cols):
    return pl.pallas_call(
        functools.partial(gather_kernel, plan),
        in_specs=[VMEM] * 6,
        out_specs=VMEM,
        out_shape=jax.ShapeDtypeStruct((rows, cols), jnp.float32),
        compiler_params=pltpu.CompilerParams(vmem_limit_bytes=8 << 20),
        cost_estimate=cost(0, 6 * rows * cols),
        name="gather",
    )(traj, inc, traj_too, inc_too, ext, ext_too)


def forward_kernel(plan, which, scale, tail, counts, rows_in, courant, vertical, offset, w, w_low, w_high, out):
    reach, rows, cols = plan.reach, rows_in.shape[0], courant.shape[1]
    slots = w.shape[-1]
    contract = (((1,), (1,)), ((), ()))
    lane = lax.broadcasted_iota(jnp.int32, (rows, LANE), 1)

    def slotted(group):
        base, shift, size = place(counts, group)
        turned = [
            pltpu.roll(x, lax.rem(LANE - shift, LANE), axis=1)
            for x in columns(rows_in[:, pl.ds(base, slots + LANE)])
        ]
        parts = []
        for at, (x, following) in enumerate(zip(turned[:-1], turned[1:])):
            x = jnp.where(lane < LANE - shift, x, following)
            parts.append(jnp.where(lane < size - at * LANE, x, 0.0))
        return jnp.concatenate(parts, axis=1).astype(jnp.bfloat16)

    group = plan.sent(which)
    y = slotted(group)
    out[...] = scale * lax.dot_general(y, w[which], contract, preferred_element_type=jnp.float32)
    for part, at in enumerate((cols - LANE, 0)):
        span = slice((2 + part) * LANE, (3 + part) * LANE)
        for row, ref in ((0, courant), (2, vertical)):
            value = ref[:, at : at + LANE]
            top = value.astype(jnp.bfloat16).astype(jnp.float32)
            out[tail + row : tail + row + 1, span] = scale * top
            out[tail + row + 1 : tail + row + 2, span] = scale * (value - top)
        out[tail + 4 : tail + 5, span] = scale * offset[:, at : at + LANE].astype(jnp.float32)

    @pl.when((group == 0) | (group == reach - 1))
    def _():
        z = slotted(lax.rem(group + reach - 1, reach))
        e = scale * lax.dot_general(w_low[which], z, contract, preferred_element_type=jnp.float32)
        out[tail : tail + 2 * HALO, :rows] = e[SUB - 2 * HALO :]

    @pl.when((group == reach - 2) | (group == reach - 1))
    def _():
        z = slotted(lax.rem(group + 1, reach))
        e = scale * lax.dot_general(w_high[which], z, contract, preferred_element_type=jnp.float32)
        out[tail : tail + 2 * HALO, LANE : LANE + rows] = e[: 2 * HALO]


def forward(plan, which, counts, rows_in, courant, vertical, offset, w, w_low, w_high, scale, tail):
    rows = rows_in.shape[0]
    win, slots = w.shape[1:]
    return pl.pallas_call(
        functools.partial(forward_kernel, plan, which, scale, tail),
        in_specs=[VMEM] * 8,
        out_specs=VMEM,
        out_shape=jax.ShapeDtypeStruct((rows, win), jnp.float32),
        compiler_params=pltpu.CompilerParams(vmem_limit_bytes=8 << 20),
        cost_estimate=cost(2 * rows * win * slots, 4 * rows_in.size),
    )(counts, rows_in, courant, vertical, offset, w, w_low, w_high)


def collect(plan, unscale, tail, numbers, pieces, acc, low, high, c_low, c_high):
    reach = plan.reach
    span = pieces[0].shape[1] // 2
    for k, piece in zip(numbers, pieces):
        group = plan.taken(k)
        first = pl.multiple_of(group * span, LANE)
        second = pl.multiple_of(lax.rem(group + 1, reach) * span, LANE)
        acc[:, pl.ds(first, span)] += unscale * piece[:, :span]
        acc[:, pl.ds(second, span)] += unscale * piece[:, span:]
        is_low = (group == 0) | (group == reach - 1)
        is_high = (group == reach - 2) | (group == reach - 1)
        low = low + jnp.where(is_low, piece[tail : tail + 2 * HALO, :LANE], 0.0)
        high = high + jnp.where(is_high, piece[tail : tail + 2 * HALO, LANE : 2 * LANE], 0.0)
        c_low = jnp.where(group == reach // 2 + 1, piece[tail : tail + COEFS, 2 * LANE : 3 * LANE], c_low)
        c_high = jnp.where(group == reach // 2 - 1, piece[tail : tail + COEFS, 3 * LANE :], c_high)
    return low, high, c_low, c_high


HALO_SLOTS = ((0, 2 * HALO), (SUB, 2 * HALO), (2 * SUB, COEFS), (3 * SUB, COEFS))


def assemble_kernel(plan, unscale, tail, numbers, *refs):
    pieces, (acc, side) = refs[:-2], refs[-2:]
    acc[...] = jnp.zeros_like(acc)
    side[...] = jnp.zeros_like(side)
    blank = [jnp.zeros((size, LANE), jnp.float32) for _, size in HALO_SLOTS]
    halo = collect(plan, unscale, tail, numbers, pieces, acc, *blank)
    for (at, size), part in zip(HALO_SLOTS, halo):
        side[at : at + size, :] = part


def assemble(plan, numbers, pieces, unscale, tail, cols):
    rows = pieces[0].shape[0]
    return pl.pallas_call(
        functools.partial(assemble_kernel, plan, unscale, tail, numbers),
        in_specs=[VMEM] * len(pieces),
        out_specs=[VMEM] * 2,
        out_shape=[
            jax.ShapeDtypeStruct((rows, cols + LANE), jnp.float32),
            jax.ShapeDtypeStruct((4 * SUB, LANE), jnp.float32),
        ],
        compiler_params=pltpu.CompilerParams(vmem_limit_bytes=8 << 20),
        cost_estimate=cost(4 * rows * cols, 8 * rows * cols),
        name="assemble",
    )(*pieces)


def stencil_kernel(plan, unscale, tail, numbers, kappa_in, acc_in, side, *refs):
    rounds, reach = plan.rounds, plan.reach
    pieces = refs[: len(numbers)]
    courant_in, vertical_in, offset_in, tangent_out = refs[len(numbers) : len(numbers) + 4]
    windows_out = refs[len(numbers) + 4 : len(numbers) + 4 + rounds]
    acc, turn, adj = refs[len(numbers) + 4 + rounds :]
    tracers = kappa_in.shape[1]
    levels = tangent_out.shape[0] // (2 * tracers)
    cols = courant_in.shape[1]
    main = tracers * levels
    rows = acc.shape[0]
    span = cols // reach
    wide = cols + LANE

    acc[...] = acc_in[...]
    halo = [side[at : at + size, :] for at, size in HALO_SLOTS]
    low, high, c_low, c_high = collect(plan, unscale, tail, numbers, pieces, acc, *halo)
    turn[...] = jnp.zeros_like(turn)
    turn[: 2 * HALO, :] = unscale * high
    turn[LANE - 2 * HALO :, :] = unscale * low
    acc[:, cols:] = turn[...].T[:rows, :]

    lane = lax.broadcasted_iota(jnp.int32, (COEFS, LANE), 1)
    beyond = unscale * jnp.where(lane < LANE // 2, c_high, c_low)
    spread = lambda row: jnp.broadcast_to(row, (SUB, wide))
    kappa = [jnp.broadcast_to(kappa_in[:, m : m + 1], (SUB, wide)) for m in range(tracers)]
    row_of = lambda ref, extra: spread(jnp.concatenate([ref[...].astype(jnp.float32), extra], axis=1))
    courant = row_of(courant_in, beyond[0:1] + beyond[1:2])
    vertical = row_of(vertical_in, beyond[2:3] + beyond[3:4])
    offset = row_of(offset_in, beyond[4:5])
    rising = jnp.maximum(vertical, 0.0)
    sinking = jnp.maximum(-vertical, 0.0)
    shifts = range(-HALO, HALO + 1)
    picked = {s: offset == jnp.float32(s) for s in shifts}
    turned = lambda x, by: x if by % wide == 0 else pltpu.roll(x, by % wide, axis=1)
    keep = 1.0 - courant - rising - sinking

    def tangent_of(delta, loss, below, above):
        departed = jnp.zeros_like(delta)
        for s in shifts:
            departed = jnp.where(picked[s], turned(delta, -s), departed)
        return (keep - loss) * delta + courant * departed + rising * below + sinking * above

    sub = lax.broadcasted_iota(jnp.int32, (SUB, wide), 0)
    has_prev, has_next = plan.has_prev(), plan.has_next()
    state_of = lambda h, m: acc[2 * h * main + m * levels : 2 * h * main + (m + 1) * levels, :]
    delta_of = lambda h, m: acc[(2 * h + 1) * main + m * levels : (2 * h + 1) * main + (m + 1) * levels, :]
    line = lambda r: acc[4 * main + r : 4 * main + r + 1, :]
    x_state = jnp.zeros((SUB, wide), jnp.float32)
    x_delta, x_below, x_above, x_kappa = x_state, x_state, x_state, x_state
    for m in range(tracers):
        here = sub == m
        outer = line(2 * tracers + m)
        first = delta_of(0, m)[:1]
        final = delta_of(1, m)[levels - 1 :]
        x_state = jnp.where(here, spread(line(m)), x_state)
        x_delta = jnp.where(here, spread(line(tracers + m)), x_delta)
        x_below = jnp.where(here, spread(jnp.where(has_next, final, outer)), x_below)
        x_above = jnp.where(here, spread(jnp.where(has_next, outer, first)), x_above)
        x_kappa = jnp.where(here, kappa[m], x_kappa)
    x_tangent = tangent_of(x_delta, 2.0 * x_kappa * x_state, x_below, x_above)

    def beside(halves, edge):
        lo, hi = halves
        lo_below = jnp.where(has_prev, edge, 0.0)
        hi_above = jnp.where(has_next, edge, 0.0)
        below = (
            jnp.where(sub == 0, spread(lo_below), pltpu.roll(lo, 1, axis=0)),
            jnp.where(sub == 0, spread(lo[levels - 1 :]), pltpu.roll(hi, 1, axis=0)),
        )
        above = (
            jnp.where(sub == levels - 1, spread(hi[:1]), pltpu.roll(lo, levels - 1, axis=0)),
            jnp.where(sub == levels - 1, spread(hi_above), pltpu.roll(hi, levels - 1, axis=0)),
        )
        return below, above

    for m in range(tracers):
        deltas = (delta_of(0, m), delta_of(1, m))
        losses = tuple(2.0 * kappa[m] * state_of(h, m) for h in range(2))
        below, above = beside(deltas, x_delta[m : m + 1])
        tangents = tuple(tangent_of(deltas[h], losses[h], below[h], above[h]) for h in range(2))
        for h in range(2):
            at = h * main + m * levels
            tangent_out[at : at + levels, :] = tangents[h][:, :cols]
        t_below, t_above = beside(tangents, x_tangent[m : m + 1])
        for h in range(2):
            tangent = tangents[h]
            flux = courant * tangent
            arrived = jnp.zeros_like(tangent)
            for s in shifts:
                arrived = arrived + turned(jnp.where(picked[s], flux, 0.0), s)
            adjoint = (keep - losses[h]) * tangent + arrived + rising * t_above[h] + sinking * t_below[h]
            at = h * main + m * levels
            adj[at : at + levels, :cols] = adjoint[:, :cols]
            adj[at : at + levels, cols:] = adjoint[:, :span]
    for j in range(rounds):
        first = pl.multiple_of(plan.taken(j) * span, LANE)
        windows_out[j][...] = adj[:, pl.ds(first, 2 * span)].astype(jnp.bfloat16)


def stencil(plan, kappa, acc, side, numbers, pieces, courant, vertical, offset, levels, unscale, tail):
    rows = pieces[0].shape[0]
    cols = courant.shape[1]
    span = cols // plan.reach
    main = 2 * kappa.shape[1] * levels
    return pl.pallas_call(
        functools.partial(stencil_kernel, plan, unscale, tail, numbers),
        in_specs=[VMEM] * (6 + len(pieces)),
        out_specs=[VMEM] * (1 + plan.rounds),
        out_shape=[jax.ShapeDtypeStruct((main, cols), jnp.float32)]
        + [jax.ShapeDtypeStruct((main, 2 * span), jnp.bfloat16)] * plan.rounds,
        scratch_shapes=[
            pltpu.VMEM((rows, cols + LANE), jnp.float32),
            pltpu.VMEM((LANE, LANE), jnp.float32),
            pltpu.VMEM((main, cols + span), jnp.float32),
        ],
        compiler_params=pltpu.CompilerParams(vmem_limit_bytes=24 << 20),
        cost_estimate=cost(100 * rows * cols, 8 * rows * cols),
        name="stencil",
    )(kappa, acc, side, *pieces, courant, vertical, offset)


def emit_kernel(plan, both, out):
    tracers, levels, _ = out.shape
    at = pl.multiple_of(plan.core() * tracers * levels, SUB)
    for m in range(tracers):
        out[m] = both[pl.ds(at + m * levels, levels), :]


def emit(plan, both, tracers):
    main, cols = both.shape
    return pl.pallas_call(
        functools.partial(emit_kernel, plan),
        in_specs=[VMEM],
        out_specs=VMEM,
        out_shape=jax.ShapeDtypeStruct((tracers, main // 2 // tracers, cols), jnp.float32),
        compiler_params=pltpu.CompilerParams(vmem_limit_bytes=4 << 20),
        cost_estimate=cost(0, 4 * both.size),
        name="emit",
    )(both)


def backward_kernel(plan, last, numbers, counts, weight, *refs):
    pieces = refs[: len(numbers)]
    start = refs[len(numbers)] if last else None
    out = refs[len(numbers) + last]
    acc = refs[-1] if last else out
    slots = weight.shape[-1]
    main = acc.shape[0]
    acc[...] = start[...] if last else jnp.zeros_like(acc)
    lane = lax.broadcasted_iota(jnp.int32, (main, LANE), 1)
    blank = jnp.zeros((main, LANE), jnp.float32)
    for k, piece in zip(numbers, pieces):
        group = plan.returned(k)
        both = piece[...].astype(jnp.float32)
        own = jnp.where(plan.core() == 0, both[:main], both[main:]).astype(jnp.bfloat16)
        grad = jnp.dot(own, weight[0, group], preferred_element_type=jnp.float32)
        base, shift, size = place(counts, group)
        turned = [
            pltpu.roll(jnp.where(lane < size - at * LANE, x, 0.0), shift, axis=1)
            for at, x in enumerate(columns(grad))
        ]
        placed = [
            jnp.where(lane < shift, before, x) for before, x in zip([blank] + turned, turned + [blank])
        ]
        acc[:, pl.ds(base, slots + LANE)] += jnp.concatenate(placed, axis=1)
    if last:
        tracers, levels, cols = out.shape
        for m in range(tracers):
            out[m] = acc[m * levels : (m + 1) * levels, :cols]


def backward(plan, counts, weight, numbers, pieces, start, shape):
    tracers, levels, cols = shape
    slots = weight.shape[-1]
    main = tracers * levels
    last = start is not None
    padded = (main, cols + slots)
    return pl.pallas_call(
        functools.partial(backward_kernel, plan, int(last), numbers),
        in_specs=[VMEM] * (2 + len(pieces) + last),
        out_specs=VMEM,
        out_shape=jax.ShapeDtypeStruct(shape if last else padded, jnp.float32),
        scratch_shapes=[pltpu.VMEM(padded, jnp.float32)] if last else [],
        compiler_params=pltpu.CompilerParams(vmem_limit_bytes=12 << 20),
        cost_estimate=cost(2 * len(pieces) * main * 512 * slots, weight.size),
        name="back_last" if last else "back",
    )(counts, weight, *pieces, *([start] if last else []))


def step(trajectory, increment, counts, remap_weight, kappa, courant, vertical, offset):
    tracers, levels, cols = trajectory.shape
    reach, _, slots = remap_weight.shape[1:]
    tiles, slabs = lax.axis_size("tile"), lax.axis_size("lev")
    if slabs not in (2, 4) or reach % 2:
        raise ValueError("unsupported mesh")
    both = ("tile", "lev")
    plan = Plan(tiles, slabs, reach)
    routes = [plan.route(j) for j in range(plan.rounds)]
    scale = send_scale(slots)
    tail = 4 * tracers * levels + EDGE * tracers
    rows = -(-(tail + COEFS) // SUB) * SUB

    swap = [(v, v ^ 1) for v in range(slabs)]
    near = [(v, v + 1 if v % 2 else v - 1) for v in range(slabs)]
    far = [(v, v + 2 if v % 2 else v - 2) for v in range(slabs)]
    near, far = ([(a, b) for a, b in way if 0 <= b < slabs] for way in (near, far))
    traj_own, inc_own, border = fetch_border(plan, trajectory, increment)
    ext = lax.ppermute(border, "lev", near)
    ext_too = lax.ppermute(border, "lev", far)

    traj_too = lax.ppermute(trajectory, "lev", swap)
    inc_too = lax.ppermute(increment, "lev", swap)

    w, w_low, w_high = load(plan, remap_weight)
    lines = [x.reshape(1, cols) for x in (courant, vertical, offset)]
    rows_in = gather(plan, traj_own, inc_own, traj_too, inc_too, ext, ext_too, rows, cols + slots)
    pieces, message_0 = [], None
    for j, route in enumerate(routes):
        message = forward(plan, j, counts, rows_in, *lines, w, w_low, w_high, scale, tail)
        message = message.astype(jnp.float16)
        message_0 = message_0 if j else message
        pieces.append(lax.ppermute(message, both, route))
    if tiles != reach:
        hops = (reach // 2, -(reach // 2) - 1)
        route = [(t * slabs + v, (t + hops[v % 2]) % tiles * slabs + v) for t in range(tiles) for v in range(slabs)]
        corner = lax.ppermute(message_0[tail:, : 2 * LANE], both, route)
        low_half = lax.broadcasted_iota(jnp.int32, corner.shape, 1) < LANE
        fresh = low_half == (lax.axis_index("lev") % 2 == 0)
        pieces[0] = pieces[0].at[tail:, : 2 * LANE].set(
            jnp.where(fresh, corner, pieces[0][tail:, : 2 * LANE])
        )
    others = []
    for piece in pieces:
        others.append(lax.ppermute(piece, "lev", swap))
    whole = [piece.astype(jnp.float32) for piece in pieces + others]
    final = plan.rounds - 1
    early = [k for k in range(2 * plan.rounds) if k % plan.rounds != final]
    late = [final, plan.rounds + final]
    pick = lambda values, numbers: [values[k] for k in numbers]

    acc, side = assemble(plan, early, pick(whole, early), 1.0 / scale, tail, cols)
    tangents, *windows = stencil(
        plan, kappa.reshape(1, -1), acc, side, late, pick(whole, late), *lines, levels, 1.0 / scale, tail
    )
    returned, regained = [], []
    for window, route in zip(windows, routes):
        returned.append(lax.ppermute(window, both, [(b, a) for a, b in route]))
    for window in returned:
        regained.append(lax.ppermute(window, "lev", swap))
    tangent = emit(plan, tangents, tracers)
    parts = returned + regained
    grad = backward(plan, counts, remap_weight, early, pick(parts, early), None, trajectory.shape)
    grad = backward(plan, counts, remap_weight, late, pick(parts, late), grad, trajectory.shape)
    return (tangent, grad)


def solution(mesh):
    return jax.shard_map(
        step,
        mesh=mesh,
        in_specs=(
            P(None, "lev", "tile"),
            P(None, "lev", "tile"),
            P("tile", None),
            P("tile", None, None, None),
            P(),
            P("tile"),
            P("tile"),
            P("tile"),
        ),
        out_specs=(P(None, "lev", "tile"), P(None, "lev", "tile")),
        check_vma=False,
    )
```

```python
import functools

import jax
import jax.numpy as jnp
from jax import lax
from jax.experimental import pallas as pl
from jax.experimental.pallas import tpu as pltpu
from jax.sharding import PartitionSpec as P

HALO = 2
LANE = 128
SUB = 8
EDGE = 3
COEFS = 5
VALUE_MAX = 6.0
WEIGHT_MAX = 0.25
F16_MAX = 65504.0


VMEM = pl.BlockSpec(memory_space=pltpu.VMEM)
SMEM = pl.BlockSpec(memory_space=pltpu.SMEM)
HBM = pl.BlockSpec(memory_space=pltpu.HBM)


def send_scale(slot_count):
    bound = VALUE_MAX * WEIGHT_MAX * slot_count
    scale = 1.0
    while 2.0 * scale * bound < F16_MAX:
        scale *= 2.0
    while scale * bound >= F16_MAX:
        scale *= 0.5
    return scale


def cost(flops, moved):
    return pl.CostEstimate(flops=flops, bytes_accessed=moved, transcendentals=0)


def place(counts, which):
    sizes = counts[...].astype(jnp.float32)
    lane = lax.broadcasted_iota(jnp.int32, sizes.shape, 1)
    begin = jnp.sum(jnp.where(lane < which, sizes, 0.0)).astype(jnp.int32)
    size = jnp.sum(jnp.where(lane == which, sizes, 0.0)).astype(jnp.int32)
    base = pl.multiple_of((begin // LANE) * LANE, LANE)
    return base, begin - base, size


def columns(x):
    return [x[:, at : at + LANE] for at in range(0, x.shape[1], LANE)]


def shifted(x, lane, shift, size):
    turned = [
        pltpu.roll(jnp.where(lane < size - at * LANE, part, 0.0), shift, axis=1)
        for at, part in enumerate(columns(x))
    ]
    blank = jnp.zeros_like(turned[0])
    parts = [jnp.where(lane < shift, low, high) for low, high in zip([blank] + turned, turned + [blank])]
    return jnp.concatenate(parts, axis=1)


class Plan:
    def __init__(self, tiles, slabs, reach):
        self.tiles, self.slabs, self.reach = tiles, slabs, reach
        self.rounds = reach // 2
        self.cube = tiles == reach and tiles & (tiles - 1) == 0
        if self.cube:
            self.hops = self.balanced(reach)
        else:
            self.hops = [list(range(-(reach // 2), 0)), list(range(reach // 2 - 1, -1, -1))]

    def balanced(self, reach):
        hops, load = [[], []], [0, 0]
        for flip in range(reach - 1, -1, -1):
            core = 0 if (load[0], len(hops[0])) < (load[1], len(hops[1])) else 1
            core = 1 if flip == 0 or len(hops[0]) == self.rounds else core
            core = 0 if len(hops[1]) == self.rounds - (flip > 0) else core
            hops[core].append(flip)
            load[core] += (flip >> 1) + (flip & 1)
        return hops

    def target(self, tile, core, j):
        hop = self.hops[core][j]
        return tile ^ hop if self.cube else (tile + hop) % self.tiles

    def route(self, j):
        cells = [(t, v) for t in range(self.tiles) for v in range(self.slabs)]
        return [(t * self.slabs + v, self.target(t, v % 2, j) * self.slabs + v) for t, v in cells]

    def core(self):
        return lax.rem(lax.axis_index("lev"), 2)

    def has_next(self):
        return lax.axis_index("lev") < self.slabs - 2

    def has_prev(self):
        return lax.axis_index("lev") >= 2

    def group(self, core, j, sign):
        hop = jnp.where(core == 0, jnp.int32(self.hops[0][j]), jnp.int32(self.hops[1][j]))
        centre = self.reach // 2
        if not self.cube:
            return centre + hop
        tile = lax.axis_index("tile")
        return lax.rem(sign * ((tile ^ hop) - tile) + centre + self.reach, self.reach)

    def sent(self, j):
        return self.group(self.core(), j, 1)

    def taken(self, k):
        return self.group(self.owner(k), k % self.rounds, -1)

    def returned(self, k):
        return self.group(self.owner(k), k % self.rounds, 1)

    def owner(self, k):
        return self.core() if k < self.rounds else 1 - self.core()


def border_kernel(plan, traj, inc, traj_out, inc_out, border, lines, sems):
    copies = [
        pltpu.make_async_copy(traj, traj_out, sems.at[0]),
        pltpu.make_async_copy(inc, inc_out, sems.at[1]),
    ]
    for copy in copies:
        copy.start()
    for copy in copies:
        copy.wait()
    tracers, levels, cols = traj_out.shape
    lower = plan.core() == 1
    row = 0
    for ref, depth in ((traj_out, 0), (inc_out, 0), (inc_out, 1)):
        for m in range(tracers):
            x = ref[m].astype(jnp.float32)
            low, high = levels - 1 - depth, depth
            line = jnp.where(lower, x[low : low + 1], x[high : high + 1])
            if row < SUB:
                lines[row : row + 1, :cols] = line
            else:
                part = cols // SUB
                at = cols + (row - SUB) * part
                for piece in range(SUB):
                    lines[piece : piece + 1, at : at + part] = line[:, piece * part : (piece + 1) * part]
            row += 1
    border[...] = lines[...].astype(border.dtype)


def unpacked(border, count, cols):
    part = cols // SUB
    rows = [border[:, :cols]]
    for row in range(SUB, count):
        at = cols + (row - SUB) * part
        pieces = [border[piece : piece + 1, at : at + part] for piece in range(SUB)]
        rows.append(jnp.concatenate(pieces, axis=1))
    return jnp.concatenate(rows, axis=0)[:count]


def fetch_border(plan, traj, inc):
    tracers, _, cols = traj.shape
    like = lambda *shape: jax.ShapeDtypeStruct(shape, traj.dtype)
    wide = cols + max(0, EDGE * tracers - SUB) * (cols // SUB)
    return pl.pallas_call(
        functools.partial(border_kernel, plan),
        in_specs=[HBM] * 2,
        out_specs=[VMEM] * 3,
        out_shape=[like(*traj.shape), like(*inc.shape), like(SUB, wide)],
        scratch_shapes=[pltpu.VMEM((SUB, wide), jnp.float32), pltpu.SemaphoreType.DMA((2,))],
        compiler_params=pltpu.CompilerParams(vmem_limit_bytes=4 << 20),
        cost_estimate=cost(0, 8 * traj.size),
        name="border",
    )(traj, inc)


def load_kernel(plan, weight, w_out, w_low, w_high, sems):
    reach, win = weight.shape[1:3]
    half = win // 2
    copies = []
    for j in range(plan.rounds):
        group = plan.sent(j)
        low = lax.rem(group + reach - 1, reach)
        high = lax.rem(group + 1, reach)
        low_at = pl.multiple_of(jnp.where(group == 0, half, win) - SUB, SUB)
        high_at = pl.multiple_of(jnp.where(group == reach - 2, half, 0), SUB)
        copies.append(pltpu.make_async_copy(weight.at[0, group], w_out.at[j], sems.at[3 * j]))
        copies.append(
            pltpu.make_async_copy(
                weight.at[0, low, pl.ds(low_at, SUB)], w_low.at[j], sems.at[1 + 3 * j]
            )
        )
        copies.append(
            pltpu.make_async_copy(
                weight.at[0, high, pl.ds(high_at, SUB)], w_high.at[j], sems.at[2 + 3 * j]
            )
        )
    for copy in copies:
        copy.start()
    for copy in copies:
        copy.wait()


def load(plan, weight):
    _, _, win, slots = weight.shape
    like = lambda *shape: jax.ShapeDtypeStruct(shape, weight.dtype)
    return pl.pallas_call(
        functools.partial(load_kernel, plan),
        in_specs=[HBM],
        out_specs=[VMEM] * 3,
        out_shape=[
            like(plan.rounds, win, slots),
            like(plan.rounds, SUB, slots),
            like(plan.rounds, SUB, slots),
        ],
        scratch_shapes=[pltpu.SemaphoreType.DMA((3 * plan.rounds,))],
        compiler_params=pltpu.CompilerParams(vmem_limit_bytes=8 << 20),
        cost_estimate=cost(0, 4 * plan.rounds * win * slots),
        name="fetch",
    )(weight)


def gather_kernel(plan, traj, inc, traj_too, inc_too, ext, ext_too, rows_out):
    tracers, levels, cols = traj.shape
    main = tracers * levels
    mine = pl.multiple_of(plan.core() * 2 * main, SUB)
    theirs = pl.multiple_of((1 - plan.core()) * 2 * main, SUB)
    for m in range(tracers):
        for at, t, i in ((mine, traj, inc), (theirs, traj_too, inc_too)):
            rows_out[pl.ds(at + m * levels, levels), :cols] = t[m].astype(jnp.float32)
            rows_out[pl.ds(at + main + m * levels, levels), :cols] = i[m].astype(jnp.float32)
    rows_out[:, cols:] = jnp.zeros_like(rows_out[:, cols:])
    rows_out[4 * main :, :cols] = jnp.zeros_like(rows_out[4 * main :, :cols])
    beyond = ext[...].astype(jnp.float32) + ext_too[...].astype(jnp.float32)
    rows_out[4 * main : 4 * main + EDGE * tracers, :cols] = unpacked(beyond, EDGE * tracers, cols)


def gather(plan, traj, inc, traj_too, inc_too, ext, ext_too, rows, cols):
    return pl.pallas_call(
        functools.partial(gather_kernel, plan),
        in_specs=[VMEM] * 6,
        out_specs=VMEM,
        out_shape=jax.ShapeDtypeStruct((rows, cols), jnp.float32),
        compiler_params=pltpu.CompilerParams(vmem_limit_bytes=8 << 20),
        cost_estimate=cost(0, 6 * rows * cols),
        name="gather",
    )(traj, inc, traj_too, inc_too, ext, ext_too)


def forward_kernel(plan, which, scale, tail, counts, rows_in, courant, vertical, offset, w, w_low, w_high, out):
    reach, rows, cols = plan.reach, rows_in.shape[0], courant.shape[1]
    slots = w.shape[-1]
    contract = (((1,), (1,)), ((), ()))
    lane = lax.broadcasted_iota(jnp.int32, (rows, LANE), 1)

    def slotted(group):
        base, shift, size = place(counts, group)
        turned = [
            pltpu.roll(x, lax.rem(LANE - shift, LANE), axis=1)
            for x in columns(rows_in[:, pl.ds(base, slots + LANE)])
        ]
        parts = []
        for at, (x, following) in enumerate(zip(turned[:-1], turned[1:])):
            x = jnp.where(lane < LANE - shift, x, following)
            parts.append(jnp.where(lane < size - at * LANE, x, 0.0))
        return jnp.concatenate(parts, axis=1).astype(jnp.bfloat16)

    group = plan.sent(which)
    y = slotted(group)
    out[...] = scale * lax.dot_general(y, w[which], contract, preferred_element_type=jnp.float32)
    for part, at in enumerate((cols - LANE, 0)):
        span = slice((2 + part) * LANE, (3 + part) * LANE)
        for row, ref in ((0, courant), (2, vertical)):
            value = ref[:, at : at + LANE]
            top = value.astype(jnp.bfloat16).astype(jnp.float32)
            out[tail + row : tail + row + 1, span] = scale * top
            out[tail + row + 1 : tail + row + 2, span] = scale * (value - top)
        out[tail + 4 : tail + 5, span] = scale * offset[:, at : at + LANE].astype(jnp.float32)

    def edge(weights, group):
        base, shift, size = place(counts, group)
        lane = lax.broadcasted_iota(jnp.int32, (SUB, LANE), 1)
        weights = shifted(weights.astype(jnp.float32), lane, shift, size).astype(jnp.bfloat16)
        x = rows_in[:, pl.ds(base, slots + LANE)].astype(jnp.bfloat16)
        return scale * lax.dot_general(weights, x, contract, preferred_element_type=jnp.float32)

    @pl.when((group == 0) | (group == reach - 1))
    def _():
        e = edge(w_low[which], lax.rem(group + reach - 1, reach))
        out[tail : tail + 2 * HALO, :rows] = e[SUB - 2 * HALO :]

    @pl.when((group == reach - 2) | (group == reach - 1))
    def _():
        e = edge(w_high[which], lax.rem(group + 1, reach))
        out[tail : tail + 2 * HALO, LANE : LANE + rows] = e[: 2 * HALO]


def forward(plan, which, counts, rows_in, courant, vertical, offset, w, w_low, w_high, scale, tail):
    rows = rows_in.shape[0]
    win, slots = w.shape[1:]
    return pl.pallas_call(
        functools.partial(forward_kernel, plan, which, scale, tail),
        in_specs=[VMEM] * 8,
        out_specs=VMEM,
        out_shape=jax.ShapeDtypeStruct((rows, win), jnp.float32),
        compiler_params=pltpu.CompilerParams(vmem_limit_bytes=8 << 20),
        cost_estimate=cost(2 * rows * win * slots, 4 * rows_in.size),
    )(counts, rows_in, courant, vertical, offset, w, w_low, w_high)


def collect(plan, unscale, tail, numbers, pieces, acc, low, high, c_low, c_high):
    reach = plan.reach
    span = pieces[0].shape[1] // 2
    for k, piece in zip(numbers, pieces):
        group = plan.taken(k)
        first = pl.multiple_of(group * span, LANE)
        second = pl.multiple_of(lax.rem(group + 1, reach) * span, LANE)
        acc[:, pl.ds(first, span)] += unscale * piece[:, :span]
        acc[:, pl.ds(second, span)] += unscale * piece[:, span:]
        is_low = (group == 0) | (group == reach - 1)
        is_high = (group == reach - 2) | (group == reach - 1)
        low = low + jnp.where(is_low, piece[tail : tail + 2 * HALO, :LANE], 0.0)
        high = high + jnp.where(is_high, piece[tail : tail + 2 * HALO, LANE : 2 * LANE], 0.0)
        c_low = jnp.where(group == reach // 2 + 1, piece[tail : tail + COEFS, 2 * LANE : 3 * LANE], c_low)
        c_high = jnp.where(group == reach // 2 - 1, piece[tail : tail + COEFS, 3 * LANE :], c_high)
    return low, high, c_low, c_high


HALO_SLOTS = ((0, 2 * HALO), (SUB, 2 * HALO), (2 * SUB, COEFS), (3 * SUB, COEFS))


def assemble_kernel(plan, unscale, tail, numbers, *refs):
    pieces, (acc, side) = refs[:-2], refs[-2:]
    acc[...] = jnp.zeros_like(acc)
    side[...] = jnp.zeros_like(side)
    blank = [jnp.zeros((size, LANE), jnp.float32) for _, size in HALO_SLOTS]
    halo = collect(plan, unscale, tail, numbers, pieces, acc, *blank)
    for (at, size), part in zip(HALO_SLOTS, halo):
        side[at : at + size, :] = part


def assemble(plan, numbers, pieces, unscale, tail, cols):
    rows = pieces[0].shape[0]
    return pl.pallas_call(
        functools.partial(assemble_kernel, plan, unscale, tail, numbers),
        in_specs=[VMEM] * len(pieces),
        out_specs=[VMEM] * 2,
        out_shape=[
            jax.ShapeDtypeStruct((rows, cols + LANE), jnp.float32),
            jax.ShapeDtypeStruct((4 * SUB, LANE), jnp.float32),
        ],
        compiler_params=pltpu.CompilerParams(vmem_limit_bytes=8 << 20),
        cost_estimate=cost(4 * rows * cols, 8 * rows * cols),
        name="assemble",
    )(*pieces)


def stencil_kernel(plan, unscale, tail, numbers, kappa_in, acc_in, side, *refs):
    rounds, reach = plan.rounds, plan.reach
    pieces = refs[: len(numbers)]
    courant_in, vertical_in, offset_in, tangent_out = refs[len(numbers) : len(numbers) + 4]
    windows_out = refs[len(numbers) + 4 : len(numbers) + 4 + rounds]
    acc, turn, adj = refs[len(numbers) + 4 + rounds :]
    tracers = kappa_in.shape[1]
    levels = tangent_out.shape[0] // (2 * tracers)
    cols = courant_in.shape[1]
    main = tracers * levels
    rows = acc.shape[0]
    span = cols // reach
    wide = cols + LANE

    acc[...] = acc_in[...]
    halo = [side[at : at + size, :] for at, size in HALO_SLOTS]
    low, high, c_low, c_high = collect(plan, unscale, tail, numbers, pieces, acc, *halo)
    turn[...] = jnp.zeros_like(turn)
    turn[: 2 * HALO, :] = unscale * high
    turn[LANE - 2 * HALO :, :] = unscale * low
    acc[:, cols:] = turn[...].T[:rows, :]

    lane = lax.broadcasted_iota(jnp.int32, (COEFS, LANE), 1)
    beyond = unscale * jnp.where(lane < LANE // 2, c_high, c_low)
    spread = lambda row: jnp.broadcast_to(row, (SUB, wide))
    kappa = [jnp.broadcast_to(kappa_in[:, m : m + 1], (SUB, wide)) for m in range(tracers)]
    row_of = lambda ref, extra: spread(jnp.concatenate([ref[...].astype(jnp.float32), extra], axis=1))
    courant = row_of(courant_in, beyond[0:1] + beyond[1:2])
    vertical = row_of(vertical_in, beyond[2:3] + beyond[3:4])
    offset = row_of(offset_in, beyond[4:5])
    rising = jnp.maximum(vertical, 0.0)
    sinking = jnp.maximum(-vertical, 0.0)
    shifts = range(-HALO, HALO + 1)
    picked = {s: offset == jnp.float32(s) for s in shifts}
    turned = lambda x, by: x if by % wide == 0 else pltpu.roll(x, by % wide, axis=1)
    keep = 1.0 - courant - rising - sinking

    def tangent_of(delta, loss, below, above):
        departed = jnp.zeros_like(delta)
        for s in shifts:
            departed = jnp.where(picked[s], turned(delta, -s), departed)
        return (keep - loss) * delta + courant * departed + rising * below + sinking * above

    sub = lax.broadcasted_iota(jnp.int32, (SUB, wide), 0)
    has_prev, has_next = plan.has_prev(), plan.has_next()
    state_of = lambda h, m: acc[2 * h * main + m * levels : 2 * h * main + (m + 1) * levels, :]
    delta_of = lambda h, m: acc[(2 * h + 1) * main + m * levels : (2 * h + 1) * main + (m + 1) * levels, :]
    line = lambda r: acc[4 * main + r : 4 * main + r + 1, :]
    x_state = jnp.zeros((SUB, wide), jnp.float32)
    x_delta, x_below, x_above, x_kappa = x_state, x_state, x_state, x_state
    for m in range(tracers):
        here = sub == m
        outer = line(2 * tracers + m)
        first = delta_of(0, m)[:1]
        final = delta_of(1, m)[levels - 1 :]
        x_state = jnp.where(here, spread(line(m)), x_state)
        x_delta = jnp.where(here, spread(line(tracers + m)), x_delta)
        x_below = jnp.where(here, spread(jnp.where(has_next, final, outer)), x_below)
        x_above = jnp.where(here, spread(jnp.where(has_next, outer, first)), x_above)
        x_kappa = jnp.where(here, kappa[m], x_kappa)
    x_tangent = tangent_of(x_delta, 2.0 * x_kappa * x_state, x_below, x_above)

    def beside(halves, edge):
        lo, hi = halves
        lo_below = jnp.where(has_prev, edge, 0.0)
        hi_above = jnp.where(has_next, edge, 0.0)
        below = (
            jnp.where(sub == 0, spread(lo_below), pltpu.roll(lo, 1, axis=0)),
            jnp.where(sub == 0, spread(lo[levels - 1 :]), pltpu.roll(hi, 1, axis=0)),
        )
        above = (
            jnp.where(sub == levels - 1, spread(hi[:1]), pltpu.roll(lo, levels - 1, axis=0)),
            jnp.where(sub == levels - 1, spread(hi_above), pltpu.roll(hi, levels - 1, axis=0)),
        )
        return below, above

    for m in range(tracers):
        deltas = (delta_of(0, m), delta_of(1, m))
        losses = tuple(2.0 * kappa[m] * state_of(h, m) for h in range(2))
        below, above = beside(deltas, x_delta[m : m + 1])
        tangents = tuple(tangent_of(deltas[h], losses[h], below[h], above[h]) for h in range(2))
        for h in range(2):
            at = h * main + m * levels
            tangent_out[at : at + levels, :] = tangents[h][:, :cols]
        t_below, t_above = beside(tangents, x_tangent[m : m + 1])
        for h in range(2):
            tangent = tangents[h]
            flux = courant * tangent
            arrived = jnp.zeros_like(tangent)
            for s in shifts:
                arrived = arrived + turned(jnp.where(picked[s], flux, 0.0), s)
            adjoint = (keep - losses[h]) * tangent + arrived + rising * t_above[h] + sinking * t_below[h]
            at = h * main + m * levels
            adj[at : at + levels, :cols] = adjoint[:, :cols]
            adj[at : at + levels, cols:] = adjoint[:, :span]
    for j in range(rounds):
        first = pl.multiple_of(plan.taken(j) * span, LANE)
        windows_out[j][...] = adj[:, pl.ds(first, 2 * span)].astype(jnp.bfloat16)


def stencil(plan, kappa, acc, side, numbers, pieces, courant, vertical, offset, levels, unscale, tail):
    rows = pieces[0].shape[0]
    cols = courant.shape[1]
    span = cols // plan.reach
    main = 2 * kappa.shape[1] * levels
    return pl.pallas_call(
        functools.partial(stencil_kernel, plan, unscale, tail, numbers),
        in_specs=[VMEM] * (6 + len(pieces)),
        out_specs=[VMEM] * (1 + plan.rounds),
        out_shape=[jax.ShapeDtypeStruct((main, cols), jnp.float32)]
        + [jax.ShapeDtypeStruct((main, 2 * span), jnp.bfloat16)] * plan.rounds,
        scratch_shapes=[
            pltpu.VMEM((rows, cols + LANE), jnp.float32),
            pltpu.VMEM((LANE, LANE), jnp.float32),
            pltpu.VMEM((main, cols + span), jnp.float32),
        ],
        compiler_params=pltpu.CompilerParams(vmem_limit_bytes=24 << 20),
        cost_estimate=cost(100 * rows * cols, 8 * rows * cols),
        name="stencil",
    )(kappa, acc, side, *pieces, courant, vertical, offset)


def emit_kernel(plan, both, out):
    tracers, levels, _ = out.shape
    at = pl.multiple_of(plan.core() * tracers * levels, SUB)
    for m in range(tracers):
        out[m] = both[pl.ds(at + m * levels, levels), :]


def emit(plan, both, tracers):
    main, cols = both.shape
    return pl.pallas_call(
        functools.partial(emit_kernel, plan),
        in_specs=[VMEM],
        out_specs=VMEM,
        out_shape=jax.ShapeDtypeStruct((tracers, main // 2 // tracers, cols), jnp.float32),
        compiler_params=pltpu.CompilerParams(vmem_limit_bytes=4 << 20),
        cost_estimate=cost(0, 4 * both.size),
        name="emit",
    )(both)


def backward_kernel(plan, last, numbers, counts, weight, *refs):
    pieces = refs[: len(numbers)]
    start = refs[len(numbers)] if last else None
    out = refs[len(numbers) + last]
    acc = refs[-1] if last else out
    slots = weight.shape[-1]
    main = acc.shape[0]
    acc[...] = start[...] if last else jnp.zeros_like(acc)
    lane = lax.broadcasted_iota(jnp.int32, (main, LANE), 1)
    for k, piece in zip(numbers, pieces):
        group = plan.returned(k)
        both = piece[...].astype(jnp.float32)
        own = jnp.where(plan.core() == 0, both[:main], both[main:]).astype(jnp.bfloat16)
        grad = jnp.dot(own, weight[0, group], preferred_element_type=jnp.float32)
        base, shift, size = place(counts, group)
        acc[:, pl.ds(base, slots + LANE)] += shifted(grad, lane, shift, size)
    if last:
        tracers, levels, cols = out.shape
        for m in range(tracers):
            out[m] = acc[m * levels : (m + 1) * levels, :cols]


def backward(plan, counts, weight, numbers, pieces, start, shape):
    tracers, levels, cols = shape
    slots = weight.shape[-1]
    main = tracers * levels
    last = start is not None
    padded = (main, cols + slots)
    return pl.pallas_call(
        functools.partial(backward_kernel, plan, int(last), numbers),
        in_specs=[VMEM] * (2 + len(pieces) + last),
        out_specs=VMEM,
        out_shape=jax.ShapeDtypeStruct(shape if last else padded, jnp.float32),
        scratch_shapes=[pltpu.VMEM(padded, jnp.float32)] if last else [],
        compiler_params=pltpu.CompilerParams(vmem_limit_bytes=12 << 20),
        cost_estimate=cost(2 * len(pieces) * main * 512 * slots, weight.size),
        name="back_last" if last else "back",
    )(counts, weight, *pieces, *([start] if last else []))


def step(trajectory, increment, counts, remap_weight, kappa, courant, vertical, offset):
    tracers, levels, cols = trajectory.shape
    reach, _, slots = remap_weight.shape[1:]
    tiles, slabs = lax.axis_size("tile"), lax.axis_size("lev")
    if slabs not in (2, 4) or reach % 2:
        raise ValueError("unsupported mesh")
    both = ("tile", "lev")
    plan = Plan(tiles, slabs, reach)
    routes = [plan.route(j) for j in range(plan.rounds)]
    scale = send_scale(slots)
    tail = 4 * tracers * levels + EDGE * tracers
    rows = -(-(tail + COEFS) // SUB) * SUB

    swap = [(v, v ^ 1) for v in range(slabs)]
    near = [(v, v + 1 if v % 2 else v - 1) for v in range(slabs)]
    far = [(v, v + 2 if v % 2 else v - 2) for v in range(slabs)]
    near, far = ([(a, b) for a, b in way if 0 <= b < slabs] for way in (near, far))
    traj_own, inc_own, border = fetch_border(plan, *(pltpu.with_memory_space_constraint(x, pltpu.HBM) for x in (trajectory, increment)))
    ext = lax.ppermute(border, "lev", near)
    ext_too = lax.ppermute(border, "lev", far)

    traj_too = lax.ppermute(trajectory, "lev", swap)
    inc_too = lax.ppermute(increment, "lev", swap)

    w, w_low, w_high = load(plan, pltpu.with_memory_space_constraint(remap_weight, pltpu.HBM))
    lines = [x.reshape(1, cols) for x in (courant, vertical, offset)]
    rows_in = gather(plan, traj_own, inc_own, traj_too, inc_too, ext, ext_too, rows, cols + slots)
    pieces, message_0 = [], None
    for j, route in enumerate(routes):
        message = forward(plan, j, counts, rows_in, *lines, w, w_low, w_high, scale, tail)
        message = message.astype(jnp.float16)
        message_0 = message_0 if j else message
        pieces.append(lax.ppermute(message, both, route))
    if tiles != reach:
        hops = (reach // 2, -(reach // 2) - 1)
        route = [(t * slabs + v, (t + hops[v % 2]) % tiles * slabs + v) for t in range(tiles) for v in range(slabs)]
        corner = lax.ppermute(message_0[tail:, : 2 * LANE], both, route)
        low_half = lax.broadcasted_iota(jnp.int32, corner.shape, 1) < LANE
        fresh = low_half == (lax.axis_index("lev") % 2 == 0)
        pieces[0] = pieces[0].at[tail:, : 2 * LANE].set(
            jnp.where(fresh, corner, pieces[0][tail:, : 2 * LANE])
        )
    others = []
    for piece in pieces:
        others.append(lax.ppermute(piece, "lev", swap))
    whole = [piece.astype(jnp.float32) for piece in pieces + others]
    final = plan.rounds - 1
    early = [k for k in range(2 * plan.rounds) if k % plan.rounds != final]
    late = [final, plan.rounds + final]
    pick = lambda values, numbers: [values[k] for k in numbers]

    acc, side = assemble(plan, early, pick(whole, early), 1.0 / scale, tail, cols)
    tangents, *windows = stencil(
        plan, kappa.reshape(1, -1), acc, side, late, pick(whole, late), *lines, levels, 1.0 / scale, tail
    )
    returned, regained = [], []
    for window, route in zip(windows, routes):
        returned.append(lax.ppermute(window, both, [(b, a) for a, b in route]))
    for window in returned:
        regained.append(lax.ppermute(window, "lev", swap))
    tangent = emit(plan, tangents, tracers)
    parts = returned + regained
    grad = backward(plan, counts, remap_weight, early, pick(parts, early), None, trajectory.shape)
    grad = backward(plan, counts, remap_weight, late, pick(parts, late), grad, trajectory.shape)
    return (tangent, grad)


def solution(mesh):
    return jax.shard_map(
        step,
        mesh=mesh,
        in_specs=(
            P(None, "lev", "tile"),
            P(None, "lev", "tile"),
            P("tile", None),
            P("tile", None, None, None),
            P(),
            P("tile"),
            P("tile"),
            P("tile"),
        ),
        out_specs=(P(None, "lev", "tile"), P(None, "lev", "tile")),
        check_vma=False,
    )
```

```python
import functools

import jax
import jax.numpy as jnp
from jax import lax
from jax.experimental import pallas as pl
from jax.experimental.pallas import tpu as pltpu
from jax.sharding import PartitionSpec as P

HALO = 2
LANE = 128
SUB = 8
EDGE = 3
COEFS = 5
PACK = 1024
TUNED = {8: ((5, 2, 6, 1), (4, 3, 7, 0))}
VALUE_MAX = 6.0
WEIGHT_MAX = 0.25
F16_MAX = 65504.0


VMEM = pl.BlockSpec(memory_space=pltpu.VMEM)
SMEM = pl.BlockSpec(memory_space=pltpu.SMEM)
HBM = pl.BlockSpec(memory_space=pltpu.HBM)


def send_scale(slot_count):
    bound = VALUE_MAX * WEIGHT_MAX * slot_count
    scale = 1.0
    while 2.0 * scale * bound < F16_MAX:
        scale *= 2.0
    while scale * bound >= F16_MAX:
        scale *= 0.5
    return scale


def cost(flops, moved):
    return pl.CostEstimate(flops=flops, bytes_accessed=moved, transcendentals=0)


def place(counts, which):
    sizes = counts[...].astype(jnp.float32)
    lane = lax.broadcasted_iota(jnp.int32, sizes.shape, 1)
    packed = jnp.sum(jnp.where(lane < which, PACK * sizes, jnp.where(lane == which, sizes, 0.0)))
    packed = packed.astype(jnp.int32)
    begin = packed // PACK
    size = packed - begin * PACK
    base = pl.multiple_of((begin // LANE) * LANE, LANE)
    return base, begin - base, size


def columns(x):
    return [x[:, at : at + LANE] for at in range(0, x.shape[1], LANE)]


def shifted(x, lane, shift, size):
    turned = [
        pltpu.roll(jnp.where(lane < size - at * LANE, part, 0.0), shift, axis=1)
        for at, part in enumerate(columns(x))
    ]
    blank = jnp.zeros_like(turned[0])
    parts = [jnp.where(lane < shift, low, high) for low, high in zip([blank] + turned, turned + [blank])]
    return jnp.concatenate(parts, axis=1)


class Plan:
    def __init__(self, tiles, slabs, reach):
        self.tiles, self.slabs, self.reach = tiles, slabs, reach
        self.rounds = reach // 2
        self.cube = tiles == reach and tiles & (tiles - 1) == 0
        if self.cube:
            self.hops = TUNED.get(reach) or self.balanced(reach)
        else:
            self.hops = [list(range(-(reach // 2), 0)), list(range(reach // 2 - 1, -1, -1))]

    def balanced(self, reach):
        hops, load = [[], []], [0, 0]
        for flip in range(reach - 1, -1, -1):
            core = 0 if (load[0], len(hops[0])) < (load[1], len(hops[1])) else 1
            core = 1 if flip == 0 or len(hops[0]) == self.rounds else core
            core = 0 if len(hops[1]) == self.rounds - (flip > 0) else core
            hops[core].append(flip)
            load[core] += (flip >> 1) + (flip & 1)
        return hops

    def target(self, tile, core, j):
        hop = self.hops[core][j]
        return tile ^ hop if self.cube else (tile + hop) % self.tiles

    def route(self, j):
        cells = [(t, v) for t in range(self.tiles) for v in range(self.slabs)]
        return [(t * self.slabs + v, self.target(t, v % 2, j) * self.slabs + v) for t, v in cells]

    def core(self):
        return lax.rem(lax.axis_index("lev"), 2)

    def has_next(self):
        return lax.axis_index("lev") < self.slabs - 2

    def has_prev(self):
        return lax.axis_index("lev") >= 2

    def group(self, core, j, sign):
        hop = jnp.where(core == 0, jnp.int32(self.hops[0][j]), jnp.int32(self.hops[1][j]))
        centre = self.reach // 2
        if not self.cube:
            return centre + hop
        tile = lax.axis_index("tile")
        return lax.rem(sign * ((tile ^ hop) - tile) + centre + self.reach, self.reach)

    def sent(self, j):
        return self.group(self.core(), j, 1)

    def taken(self, k):
        return self.group(self.owner(k), k % self.rounds, -1)

    def returned(self, k):
        return self.group(self.owner(k), k % self.rounds, 1)

    def owner(self, k):
        return self.core() if k < self.rounds else 1 - self.core()


def border_kernel(plan, traj, inc, traj_out, inc_out, border, lines, sems):
    copies = [
        pltpu.make_async_copy(traj, traj_out, sems.at[0]),
        pltpu.make_async_copy(inc, inc_out, sems.at[1]),
    ]
    for copy in copies:
        copy.start()
    for copy in copies:
        copy.wait()
    tracers, levels, cols = traj_out.shape
    lower = plan.core() == 1
    row = 0
    for ref, depth in ((traj_out, 0), (inc_out, 0), (inc_out, 1)):
        for m in range(tracers):
            x = ref[m].astype(jnp.float32)
            low, high = levels - 1 - depth, depth
            line = jnp.where(lower, x[low : low + 1], x[high : high + 1])
            if row < SUB:
                lines[row : row + 1, :cols] = line
            else:
                part = cols // SUB
                at = cols + (row - SUB) * part
                for piece in range(SUB):
                    lines[piece : piece + 1, at : at + part] = line[:, piece * part : (piece + 1) * part]
            row += 1
    border[...] = lines[...].astype(border.dtype)


def unpacked(border, count, cols):
    part = cols // SUB
    rows = [border[:, :cols]]
    for row in range(SUB, count):
        at = cols + (row - SUB) * part
        pieces = [border[piece : piece + 1, at : at + part] for piece in range(SUB)]
        rows.append(jnp.concatenate(pieces, axis=1))
    return jnp.concatenate(rows, axis=0)[:count]


def fetch_border(plan, traj, inc):
    tracers, _, cols = traj.shape
    like = lambda *shape: jax.ShapeDtypeStruct(shape, traj.dtype)
    wide = cols + max(0, EDGE * tracers - SUB) * (cols // SUB)
    return pl.pallas_call(
        functools.partial(border_kernel, plan),
        in_specs=[HBM] * 2,
        out_specs=[VMEM] * 3,
        out_shape=[like(*traj.shape), like(*inc.shape), like(SUB, wide)],
        scratch_shapes=[pltpu.VMEM((SUB, wide), jnp.float32), pltpu.SemaphoreType.DMA((2,))],
        compiler_params=pltpu.CompilerParams(vmem_limit_bytes=4 << 20),
        cost_estimate=cost(0, 8 * traj.size),
        name="border",
    )(traj, inc)


def load_kernel(plan, weight, w_out, w_low, w_high, sems):
    reach, win = weight.shape[1:3]
    half = win // 2
    copies = []
    for j in range(plan.rounds):
        group = plan.sent(j)
        low = lax.rem(group + reach - 1, reach)
        high = lax.rem(group + 1, reach)
        low_at = pl.multiple_of(jnp.where(group == 0, half, win) - SUB, SUB)
        high_at = pl.multiple_of(jnp.where(group == reach - 2, half, 0), SUB)
        copies.append(pltpu.make_async_copy(weight.at[0, group], w_out.at[j], sems.at[3 * j]))
        copies.append(
            pltpu.make_async_copy(
                weight.at[0, low, pl.ds(low_at, SUB)], w_low.at[j], sems.at[1 + 3 * j]
            )
        )
        copies.append(
            pltpu.make_async_copy(
                weight.at[0, high, pl.ds(high_at, SUB)], w_high.at[j], sems.at[2 + 3 * j]
            )
        )
    for copy in copies:
        copy.start()
    for copy in copies:
        copy.wait()


def load(plan, weight):
    _, _, win, slots = weight.shape
    like = lambda *shape: jax.ShapeDtypeStruct(shape, weight.dtype)
    return pl.pallas_call(
        functools.partial(load_kernel, plan),
        in_specs=[HBM],
        out_specs=[VMEM] * 3,
        out_shape=[
            like(plan.rounds, win, slots),
            like(plan.rounds, SUB, slots),
            like(plan.rounds, SUB, slots),
        ],
        scratch_shapes=[pltpu.SemaphoreType.DMA((3 * plan.rounds,))],
        compiler_params=pltpu.CompilerParams(vmem_limit_bytes=8 << 20),
        cost_estimate=cost(0, 4 * plan.rounds * win * slots),
        name="fetch",
    )(weight)


def gather_kernel(plan, traj, inc, traj_too, inc_too, ext, ext_too, rows_out):
    tracers, levels, cols = traj.shape
    main = tracers * levels
    mine = pl.multiple_of(plan.core() * 2 * main, SUB)
    theirs = pl.multiple_of((1 - plan.core()) * 2 * main, SUB)
    for m in range(tracers):
        for at, t, i in ((mine, traj, inc), (theirs, traj_too, inc_too)):
            rows_out[pl.ds(at + m * levels, levels), :cols] = t[m].astype(jnp.float32)
            rows_out[pl.ds(at + main + m * levels, levels), :cols] = i[m].astype(jnp.float32)
    rows_out[:, cols:] = jnp.zeros_like(rows_out[:, cols:])
    rows_out[4 * main :, :cols] = jnp.zeros_like(rows_out[4 * main :, :cols])
    beyond = ext[...].astype(jnp.float32) + ext_too[...].astype(jnp.float32)
    rows_out[4 * main : 4 * main + EDGE * tracers, :cols] = unpacked(beyond, EDGE * tracers, cols)


def gather(plan, traj, inc, traj_too, inc_too, ext, ext_too, rows, cols):
    return pl.pallas_call(
        functools.partial(gather_kernel, plan),
        in_specs=[VMEM] * 6,
        out_specs=VMEM,
        out_shape=jax.ShapeDtypeStruct((rows, cols), jnp.float32),
        compiler_params=pltpu.CompilerParams(vmem_limit_bytes=8 << 20),
        cost_estimate=cost(0, 6 * rows * cols),
        name="gather",
    )(traj, inc, traj_too, inc_too, ext, ext_too)


def forward_kernel(plan, which, scale, tail, counts, rows_in, courant, vertical, offset, w, w_low, w_high, out):
    reach, rows, cols = plan.reach, rows_in.shape[0], courant.shape[1]
    slots = w.shape[-1]
    contract = (((1,), (1,)), ((), ()))
    lane = lax.broadcasted_iota(jnp.int32, (rows, LANE), 1)

    def slotted(group):
        base, shift, size = place(counts, group)
        turned = [
            pltpu.roll(x, lax.rem(LANE - shift, LANE), axis=1)
            for x in columns(rows_in[:, pl.ds(base, slots + LANE)])
        ]
        parts = []
        for at, (x, following) in enumerate(zip(turned[:-1], turned[1:])):
            x = jnp.where(lane < LANE - shift, x, following)
            parts.append(jnp.where(lane < size - at * LANE, x, 0.0))
        return jnp.concatenate(parts, axis=1).astype(jnp.bfloat16)

    group = plan.sent(which)
    y = slotted(group)
    out[...] = scale * lax.dot_general(y, w[which], contract, preferred_element_type=jnp.float32)
    for part, at in enumerate((cols - LANE, 0)):
        span = slice((2 + part) * LANE, (3 + part) * LANE)
        for row, ref in ((0, courant), (2, vertical)):
            value = ref[:, at : at + LANE]
            top = value.astype(jnp.bfloat16).astype(jnp.float32)
            out[tail + row : tail + row + 1, span] = scale * top
            out[tail + row + 1 : tail + row + 2, span] = scale * (value - top)
        out[tail + 4 : tail + 5, span] = scale * offset[:, at : at + LANE].astype(jnp.float32)

    def edge(weights, group):
        base, shift, size = place(counts, group)
        lane = lax.broadcasted_iota(jnp.int32, (SUB, LANE), 1)
        weights = shifted(weights.astype(jnp.float32), lane, shift, size).astype(jnp.bfloat16)
        x = rows_in[:, pl.ds(base, slots + LANE)].astype(jnp.bfloat16)
        return scale * lax.dot_general(weights, x, contract, preferred_element_type=jnp.float32)

    e = edge(w_low[which], lax.rem(group + reach - 1, reach))
    out[tail : tail + 2 * HALO, :rows] = e[SUB - 2 * HALO :]
    e = edge(w_high[which], lax.rem(group + 1, reach))
    out[tail : tail + 2 * HALO, LANE : LANE + rows] = e[: 2 * HALO]


def forward(plan, which, counts, rows_in, courant, vertical, offset, w, w_low, w_high, scale, tail):
    rows = rows_in.shape[0]
    win, slots = w.shape[1:]
    return pl.pallas_call(
        functools.partial(forward_kernel, plan, which, scale, tail),
        in_specs=[VMEM] * 8,
        out_specs=VMEM,
        out_shape=jax.ShapeDtypeStruct((rows, win), jnp.float32),
        compiler_params=pltpu.CompilerParams(vmem_limit_bytes=8 << 20),
        cost_estimate=cost(2 * rows * win * slots, 4 * rows_in.size),
    )(counts, rows_in, courant, vertical, offset, w, w_low, w_high)


def collect(plan, unscale, tail, numbers, pieces, acc, low, high, c_low, c_high):
    reach = plan.reach
    span = pieces[0].shape[1] // 2
    for k, piece in zip(numbers, pieces):
        group = plan.taken(k)
        first = pl.multiple_of(group * span, LANE)
        second = pl.multiple_of(lax.rem(group + 1, reach) * span, LANE)
        acc[:, pl.ds(first, span)] += unscale * piece[:, :span]
        acc[:, pl.ds(second, span)] += unscale * piece[:, span:]
        is_low = (group == 0) | (group == reach - 1)
        is_high = (group == reach - 2) | (group == reach - 1)
        low = low + jnp.where(is_low, piece[tail : tail + 2 * HALO, :LANE], 0.0)
        high = high + jnp.where(is_high, piece[tail : tail + 2 * HALO, LANE : 2 * LANE], 0.0)
        c_low = jnp.where(group == reach // 2 + 1, piece[tail : tail + COEFS, 2 * LANE : 3 * LANE], c_low)
        c_high = jnp.where(group == reach // 2 - 1, piece[tail : tail + COEFS, 3 * LANE :], c_high)
    return low, high, c_low, c_high


HALO_SLOTS = ((0, 2 * HALO), (SUB, 2 * HALO), (2 * SUB, COEFS), (3 * SUB, COEFS))


def assemble_kernel(plan, unscale, tail, numbers, *refs):
    pieces, (acc, side) = refs[:-2], refs[-2:]
    acc[...] = jnp.zeros_like(acc)
    side[...] = jnp.zeros_like(side)
    blank = [jnp.zeros((size, LANE), jnp.float32) for _, size in HALO_SLOTS]
    halo = collect(plan, unscale, tail, numbers, pieces, acc, *blank)
    for (at, size), part in zip(HALO_SLOTS, halo):
        side[at : at + size, :] = part


def assemble(plan, numbers, pieces, unscale, tail, cols):
    rows = pieces[0].shape[0]
    return pl.pallas_call(
        functools.partial(assemble_kernel, plan, unscale, tail, numbers),
        in_specs=[VMEM] * len(pieces),
        out_specs=[VMEM] * 2,
        out_shape=[
            jax.ShapeDtypeStruct((rows, cols + LANE), jnp.float32),
            jax.ShapeDtypeStruct((4 * SUB, LANE), jnp.float32),
        ],
        compiler_params=pltpu.CompilerParams(vmem_limit_bytes=8 << 20),
        cost_estimate=cost(4 * rows * cols, 8 * rows * cols),
        name="assemble",
    )(*pieces)


def stencil_kernel(plan, unscale, tail, numbers, kappa_in, acc_in, side, *refs):
    rounds, reach = plan.rounds, plan.reach
    pieces = refs[: len(numbers)]
    courant_in, vertical_in, offset_in, tangent_out = refs[len(numbers) : len(numbers) + 4]
    windows_out = refs[len(numbers) + 4 : len(numbers) + 4 + rounds]
    acc, turn, adj = refs[len(numbers) + 4 + rounds :]
    tracers = kappa_in.shape[1]
    levels = tangent_out.shape[0] // (2 * tracers)
    cols = courant_in.shape[1]
    main = tracers * levels
    rows = acc.shape[0]
    span = cols // reach
    wide = cols + LANE

    acc[...] = acc_in[...]
    halo = [side[at : at + size, :] for at, size in HALO_SLOTS]
    low, high, c_low, c_high = collect(plan, unscale, tail, numbers, pieces, acc, *halo)
    turn[...] = jnp.zeros_like(turn)
    turn[: 2 * HALO, :] = unscale * high
    turn[LANE - 2 * HALO :, :] = unscale * low
    acc[:, cols:] = turn[...].T[:rows, :]

    lane = lax.broadcasted_iota(jnp.int32, (COEFS, LANE), 1)
    beyond = unscale * jnp.where(lane < LANE // 2, c_high, c_low)
    spread = lambda row: jnp.broadcast_to(row, (SUB, wide))
    kappa = [jnp.broadcast_to(kappa_in[:, m : m + 1], (SUB, wide)) for m in range(tracers)]
    row_of = lambda ref, extra: spread(jnp.concatenate([ref[...].astype(jnp.float32), extra], axis=1))
    courant = row_of(courant_in, beyond[0:1] + beyond[1:2])
    vertical = row_of(vertical_in, beyond[2:3] + beyond[3:4])
    offset = row_of(offset_in, beyond[4:5])
    rising = jnp.maximum(vertical, 0.0)
    sinking = jnp.maximum(-vertical, 0.0)
    shifts = range(-HALO, HALO + 1)
    picked = {s: offset == jnp.float32(s) for s in shifts}
    turned = lambda x, by: x if by % wide == 0 else pltpu.roll(x, by % wide, axis=1)
    keep = 1.0 - courant - rising - sinking

    def tangent_of(delta, loss, below, above):
        departed = jnp.zeros_like(delta)
        for s in shifts:
            departed = jnp.where(picked[s], turned(delta, -s), departed)
        return (keep - loss) * delta + courant * departed + rising * below + sinking * above

    sub = lax.broadcasted_iota(jnp.int32, (SUB, wide), 0)
    has_prev, has_next = plan.has_prev(), plan.has_next()
    state_of = lambda h, m: acc[2 * h * main + m * levels : 2 * h * main + (m + 1) * levels, :]
    delta_of = lambda h, m: acc[(2 * h + 1) * main + m * levels : (2 * h + 1) * main + (m + 1) * levels, :]
    line = lambda r: acc[4 * main + r : 4 * main + r + 1, :]
    x_state = jnp.zeros((SUB, wide), jnp.float32)
    x_delta, x_below, x_above, x_kappa = x_state, x_state, x_state, x_state
    for m in range(tracers):
        here = sub == m
        outer = line(2 * tracers + m)
        first = delta_of(0, m)[:1]
        final = delta_of(1, m)[levels - 1 :]
        x_state = jnp.where(here, spread(line(m)), x_state)
        x_delta = jnp.where(here, spread(line(tracers + m)), x_delta)
        x_below = jnp.where(here, spread(jnp.where(has_next, final, outer)), x_below)
        x_above = jnp.where(here, spread(jnp.where(has_next, outer, first)), x_above)
        x_kappa = jnp.where(here, kappa[m], x_kappa)
    x_tangent = tangent_of(x_delta, 2.0 * x_kappa * x_state, x_below, x_above)

    def beside(halves, edge):
        lo, hi = halves
        lo_below = jnp.where(has_prev, edge, 0.0)
        hi_above = jnp.where(has_next, edge, 0.0)
        below = (
            jnp.where(sub == 0, spread(lo_below), pltpu.roll(lo, 1, axis=0)),
            jnp.where(sub == 0, spread(lo[levels - 1 :]), pltpu.roll(hi, 1, axis=0)),
        )
        above = (
            jnp.where(sub == levels - 1, spread(hi[:1]), pltpu.roll(lo, levels - 1, axis=0)),
            jnp.where(sub == levels - 1, spread(hi_above), pltpu.roll(hi, levels - 1, axis=0)),
        )
        return below, above

    for m in range(tracers):
        deltas = (delta_of(0, m), delta_of(1, m))
        losses = tuple(2.0 * kappa[m] * state_of(h, m) for h in range(2))
        below, above = beside(deltas, x_delta[m : m + 1])
        tangents = tuple(tangent_of(deltas[h], losses[h], below[h], above[h]) for h in range(2))
        for h in range(2):
            at = h * main + m * levels
            tangent_out[at : at + levels, :] = tangents[h][:, :cols]
        t_below, t_above = beside(tangents, x_tangent[m : m + 1])
        for h in range(2):
            tangent = tangents[h]
            flux = courant * tangent
            arrived = jnp.zeros_like(tangent)
            for s in shifts:
                arrived = arrived + turned(jnp.where(picked[s], flux, 0.0), s)
            adjoint = (keep - losses[h]) * tangent + arrived + rising * t_above[h] + sinking * t_below[h]
            at = h * main + m * levels
            adj[at : at + levels, :cols] = adjoint[:, :cols]
            adj[at : at + levels, cols:] = adjoint[:, :span]
    for j in range(rounds):
        first = pl.multiple_of(plan.taken(j) * span, LANE)
        windows_out[j][...] = adj[:, pl.ds(first, 2 * span)].astype(jnp.bfloat16)


def stencil(plan, kappa, acc, side, numbers, pieces, courant, vertical, offset, levels, unscale, tail):
    rows = pieces[0].shape[0]
    cols = courant.shape[1]
    span = cols // plan.reach
    main = 2 * kappa.shape[1] * levels
    return pl.pallas_call(
        functools.partial(stencil_kernel, plan, unscale, tail, numbers),
        in_specs=[VMEM] * (6 + len(pieces)),
        out_specs=[VMEM] * (1 + plan.rounds),
        out_shape=[jax.ShapeDtypeStruct((main, cols), jnp.float32)]
        + [jax.ShapeDtypeStruct((main, 2 * span), jnp.bfloat16)] * plan.rounds,
        scratch_shapes=[
            pltpu.VMEM((rows, cols + LANE), jnp.float32),
            pltpu.VMEM((LANE, LANE), jnp.float32),
            pltpu.VMEM((main, cols + span), jnp.float32),
        ],
        compiler_params=pltpu.CompilerParams(vmem_limit_bytes=24 << 20),
        cost_estimate=cost(100 * rows * cols, 8 * rows * cols),
        name="stencil",
    )(kappa, acc, side, *pieces, courant, vertical, offset)


def emit_kernel(plan, both, out):
    tracers, levels, _ = out.shape
    at = pl.multiple_of(plan.core() * tracers * levels, SUB)
    for m in range(tracers):
        out[m] = both[pl.ds(at + m * levels, levels), :]


def emit(plan, both, tracers):
    main, cols = both.shape
    return pl.pallas_call(
        functools.partial(emit_kernel, plan),
        in_specs=[VMEM],
        out_specs=VMEM,
        out_shape=jax.ShapeDtypeStruct((tracers, main // 2 // tracers, cols), jnp.float32),
        compiler_params=pltpu.CompilerParams(vmem_limit_bytes=4 << 20),
        cost_estimate=cost(0, 4 * both.size),
        name="emit",
    )(both)


def backward_kernel(plan, last, numbers, counts, weight, *refs):
    pieces = refs[: len(numbers)]
    start = refs[len(numbers)] if last else None
    out = refs[len(numbers) + last]
    acc = refs[-1] if last else out
    slots = weight.shape[-1]
    main = acc.shape[0]
    acc[...] = start[...] if last else jnp.zeros_like(acc)
    lane = lax.broadcasted_iota(jnp.int32, (main, LANE), 1)
    for k, piece in zip(numbers, pieces):
        group = plan.returned(k)
        both = piece[...].astype(jnp.float32)
        own = jnp.where(plan.core() == 0, both[:main], both[main:]).astype(jnp.bfloat16)
        grad = jnp.dot(own, weight[0, group], preferred_element_type=jnp.float32)
        base, shift, size = place(counts, group)
        acc[:, pl.ds(base, slots + LANE)] += shifted(grad, lane, shift, size)
    if last:
        tracers, levels, cols = out.shape
        for m in range(tracers):
            out[m] = acc[m * levels : (m + 1) * levels, :cols]


def backward(plan, counts, weight, numbers, pieces, start, shape):
    tracers, levels, cols = shape
    slots = weight.shape[-1]
    main = tracers * levels
    last = start is not None
    padded = (main, cols + slots)
    return pl.pallas_call(
        functools.partial(backward_kernel, plan, int(last), numbers),
        in_specs=[VMEM] * (2 + len(pieces) + last),
        out_specs=VMEM,
        out_shape=jax.ShapeDtypeStruct(shape if last else padded, jnp.float32),
        scratch_shapes=[pltpu.VMEM(padded, jnp.float32)] if last else [],
        compiler_params=pltpu.CompilerParams(vmem_limit_bytes=12 << 20),
        cost_estimate=cost(2 * len(pieces) * main * 512 * slots, weight.size),
        name="back_last" if last else "back",
    )(counts, weight, *pieces, *([start] if last else []))


def step(trajectory, increment, counts, remap_weight, kappa, courant, vertical, offset):
    tracers, levels, cols = trajectory.shape
    reach, _, slots = remap_weight.shape[1:]
    tiles, slabs = lax.axis_size("tile"), lax.axis_size("lev")
    if slabs not in (2, 4) or reach % 2:
        raise ValueError("unsupported mesh")
    both = ("tile", "lev")
    plan = Plan(tiles, slabs, reach)
    routes = [plan.route(j) for j in range(plan.rounds)]
    scale = send_scale(slots)
    tail = 4 * tracers * levels + EDGE * tracers
    rows = -(-(tail + COEFS) // SUB) * SUB

    swap = [(v, v ^ 1) for v in range(slabs)]
    near = [(v, v + 1 if v % 2 else v - 1) for v in range(slabs)]
    far = [(v, v + 2 if v % 2 else v - 2) for v in range(slabs)]
    near, far = ([(a, b) for a, b in way if 0 <= b < slabs] for way in (near, far))
    traj_own, inc_own, border = fetch_border(plan, *(pltpu.with_memory_space_constraint(x, pltpu.HBM) for x in (trajectory, increment)))
    ext = lax.ppermute(border, "lev", near)
    ext_too = lax.ppermute(border, "lev", far)

    traj_too = lax.ppermute(trajectory, "lev", swap)
    inc_too = lax.ppermute(increment, "lev", swap)

    w, w_low, w_high = load(plan, pltpu.with_memory_space_constraint(remap_weight, pltpu.HBM))
    lines = [x.reshape(1, cols) for x in (courant, vertical, offset)]
    rows_in = gather(plan, traj_own, inc_own, traj_too, inc_too, ext, ext_too, rows, cols + slots)
    pieces, message_0 = [], None
    for j, route in enumerate(routes):
        message = forward(plan, j, counts, rows_in, *lines, w, w_low, w_high, scale, tail)
        message = message.astype(jnp.float16)
        message_0 = message_0 if j else message
        pieces.append(lax.ppermute(message, both, route))
    if tiles != reach:
        hops = (reach // 2, -(reach // 2) - 1)
        route = [(t * slabs + v, (t + hops[v % 2]) % tiles * slabs + v) for t in range(tiles) for v in range(slabs)]
        corner = lax.ppermute(message_0[tail:, : 2 * LANE], both, route)
        low_half = lax.broadcasted_iota(jnp.int32, corner.shape, 1) < LANE
        fresh = low_half == (lax.axis_index("lev") % 2 == 0)
        pieces[0] = pieces[0].at[tail:, : 2 * LANE].set(
            jnp.where(fresh, corner, pieces[0][tail:, : 2 * LANE])
        )
    others = []
    for piece in pieces:
        others.append(lax.ppermute(piece, "lev", swap))
    whole = [piece.astype(jnp.float32) for piece in pieces + others]
    early = list(range(2 * plan.rounds - 1))
    late = [2 * plan.rounds - 1]
    pick = lambda values, numbers: [values[k] for k in numbers]

    acc, side = assemble(plan, early, pick(whole, early), 1.0 / scale, tail, cols)
    tangents, *windows = stencil(
        plan, kappa.reshape(1, -1), acc, side, late, pick(whole, late), *lines, levels, 1.0 / scale, tail
    )
    returned, regained = [], []
    for window, route in zip(windows, routes):
        returned.append(lax.ppermute(window, both, [(b, a) for a, b in route]))
    for window in returned:
        regained.append(lax.ppermute(window, "lev", swap))
    tangent = emit(plan, tangents, tracers)
    parts = returned + regained
    grad = backward(plan, counts, remap_weight, early, pick(parts, early), None, trajectory.shape)
    grad = backward(plan, counts, remap_weight, late, pick(parts, late), grad, trajectory.shape)
    return (tangent, grad)


def solution(mesh):
    return jax.shard_map(
        step,
        mesh=mesh,
        in_specs=(
            P(None, "lev", "tile"),
            P(None, "lev", "tile"),
            P("tile", None),
            P("tile", None, None, None),
            P(),
            P("tile"),
            P("tile"),
            P("tile"),
        ),
        out_specs=(P(None, "lev", "tile"), P(None, "lev", "tile")),
        check_vma=False,
    )
```

```python
import functools

import jax
import jax.numpy as jnp
from jax import lax
from jax.experimental import pallas as pl
from jax.experimental.pallas import tpu as pltpu
from jax.sharding import PartitionSpec as P

HALO = 2
LANE = 128
SUB = 8
EDGE = 3
COEFS = 5
PACK = 1024
TUNED = {8: ((5, 2, 6, 1), (4, 3, 7, 0))}
VALUE_MAX = 6.0
WEIGHT_MAX = 0.25
F16_MAX = 65504.0


VMEM = pl.BlockSpec(memory_space=pltpu.VMEM)
SMEM = pl.BlockSpec(memory_space=pltpu.SMEM)
HBM = pl.BlockSpec(memory_space=pltpu.HBM)


def send_scale(slot_count):
    bound = VALUE_MAX * WEIGHT_MAX * slot_count
    scale = 1.0
    while 2.0 * scale * bound < F16_MAX:
        scale *= 2.0
    while scale * bound >= F16_MAX:
        scale *= 0.5
    return scale


def cost(flops, moved):
    return pl.CostEstimate(flops=flops, bytes_accessed=moved, transcendentals=0)


def place(counts, which):
    sizes = counts[...].astype(jnp.float32)
    lane = lax.broadcasted_iota(jnp.int32, sizes.shape, 1)
    packed = jnp.sum(jnp.where(lane < which, PACK * sizes, jnp.where(lane == which, sizes, 0.0)))
    packed = packed.astype(jnp.int32)
    begin = packed // PACK
    size = packed - begin * PACK
    base = pl.multiple_of((begin // LANE) * LANE, LANE)
    return base, begin - base, size


def columns(x):
    return [x[:, at : at + LANE] for at in range(0, x.shape[1], LANE)]


def shifted(x, lane, shift, size):
    turned = [
        pltpu.roll(jnp.where(lane < size - at * LANE, part, 0.0), shift, axis=1)
        for at, part in enumerate(columns(x))
    ]
    blank = jnp.zeros_like(turned[0])
    parts = [jnp.where(lane < shift, low, high) for low, high in zip([blank] + turned, turned + [blank])]
    return jnp.concatenate(parts, axis=1)


class Plan:
    def __init__(self, tiles, slabs, reach):
        self.tiles, self.slabs, self.reach = tiles, slabs, reach
        self.rounds = reach // 2
        self.cube = tiles == reach and tiles & (tiles - 1) == 0
        if self.cube:
            self.hops = TUNED.get(reach) or self.balanced(reach)
        else:
            self.hops = [list(range(-(reach // 2), 0)), list(range(reach // 2 - 1, -1, -1))]

    def balanced(self, reach):
        hops, load = [[], []], [0, 0]
        for flip in range(reach - 1, -1, -1):
            core = 0 if (load[0], len(hops[0])) < (load[1], len(hops[1])) else 1
            core = 1 if flip == 0 or len(hops[0]) == self.rounds else core
            core = 0 if len(hops[1]) == self.rounds - (flip > 0) else core
            hops[core].append(flip)
            load[core] += (flip >> 1) + (flip & 1)
        return hops

    def target(self, tile, core, j):
        hop = self.hops[core][j]
        return tile ^ hop if self.cube else (tile + hop) % self.tiles

    def route(self, j):
        cells = [(t, v) for t in range(self.tiles) for v in range(self.slabs)]
        return [(t * self.slabs + v, self.target(t, v % 2, j) * self.slabs + v) for t, v in cells]

    def core(self):
        return lax.rem(lax.axis_index("lev"), 2)

    def has_next(self):
        return lax.axis_index("lev") < self.slabs - 2

    def has_prev(self):
        return lax.axis_index("lev") >= 2

    def group(self, core, j, sign):
        hop = jnp.where(core == 0, jnp.int32(self.hops[0][j]), jnp.int32(self.hops[1][j]))
        centre = self.reach // 2
        if not self.cube:
            return centre + hop
        tile = lax.axis_index("tile")
        return lax.rem(sign * ((tile ^ hop) - tile) + centre + self.reach, self.reach)

    def sent(self, j):
        return self.group(self.core(), j, 1)

    def taken(self, k):
        return self.group(self.owner(k), k % self.rounds, -1)

    def returned(self, k):
        return self.group(self.owner(k), k % self.rounds, 1)

    def owner(self, k):
        return self.core() if k < self.rounds else 1 - self.core()


def border_kernel(plan, traj, inc, traj_out, inc_out, border, lines, sems):
    copies = [
        pltpu.make_async_copy(traj, traj_out, sems.at[0]),
        pltpu.make_async_copy(inc, inc_out, sems.at[1]),
    ]
    for copy in copies:
        copy.start()
    for copy in copies:
        copy.wait()
    tracers, levels, cols = traj_out.shape
    lower = plan.core() == 1
    row = 0
    for ref, depth in ((traj_out, 0), (inc_out, 0), (inc_out, 1)):
        for m in range(tracers):
            x = ref[m].astype(jnp.float32)
            low, high = levels - 1 - depth, depth
            line = jnp.where(lower, x[low : low + 1], x[high : high + 1])
            if row < SUB:
                lines[row : row + 1, :cols] = line
            else:
                part = cols // SUB
                at = cols + (row - SUB) * part
                for piece in range(SUB):
                    lines[piece : piece + 1, at : at + part] = line[:, piece * part : (piece + 1) * part]
            row += 1
    border[...] = lines[...].astype(border.dtype)


def unpacked(border, count, cols):
    part = cols // SUB
    rows = [border[:, :cols]]
    for row in range(SUB, count):
        at = cols + (row - SUB) * part
        pieces = [border[piece : piece + 1, at : at + part] for piece in range(SUB)]
        rows.append(jnp.concatenate(pieces, axis=1))
    return jnp.concatenate(rows, axis=0)[:count]


def fetch_border(plan, traj, inc):
    tracers, _, cols = traj.shape
    like = lambda *shape: jax.ShapeDtypeStruct(shape, traj.dtype)
    wide = cols + max(0, EDGE * tracers - SUB) * (cols // SUB)
    return pl.pallas_call(
        functools.partial(border_kernel, plan),
        in_specs=[HBM] * 2,
        out_specs=[VMEM] * 3,
        out_shape=[like(*traj.shape), like(*inc.shape), like(SUB, wide)],
        scratch_shapes=[pltpu.VMEM((SUB, wide), jnp.float32), pltpu.SemaphoreType.DMA((2,))],
        compiler_params=pltpu.CompilerParams(vmem_limit_bytes=4 << 20),
        cost_estimate=cost(0, 8 * traj.size),
        name="border",
    )(traj, inc)


def load_kernel(plan, weight, w_out, edges, sems):
    reach, win = weight.shape[1:3]
    half = win // 2
    copies = [
        pltpu.make_async_copy(weight.at[0, plan.sent(j)], w_out.at[j], sems.at[j])
        for j in range(plan.rounds)
    ]
    parts = ((reach - 1, half - SUB, 2 * SUB), (reach - 2, win - SUB, SUB), (0, 0, SUB))
    at = 0
    for part, (group, first, size) in enumerate(parts):
        copies.append(
            pltpu.make_async_copy(
                weight.at[0, group, pl.ds(first, size)], edges.at[pl.ds(at, size)], sems.at[plan.rounds + part]
            )
        )
        at += size
    for copy in copies:
        copy.start()
    for copy in copies:
        copy.wait()


def load(plan, weight):
    _, _, win, slots = weight.shape
    like = lambda *shape: jax.ShapeDtypeStruct(shape, weight.dtype)
    return pl.pallas_call(
        functools.partial(load_kernel, plan),
        in_specs=[HBM],
        out_specs=[VMEM] * 2,
        out_shape=[like(plan.rounds, win, slots), like(4 * SUB, slots)],
        scratch_shapes=[pltpu.SemaphoreType.DMA((plan.rounds + 3,))],
        compiler_params=pltpu.CompilerParams(vmem_limit_bytes=8 << 20),
        cost_estimate=cost(0, 4 * plan.rounds * win * slots),
        name="fetch",
    )(weight)


def gather_kernel(plan, traj, inc, traj_too, inc_too, ext, ext_too, rows_out):
    tracers, levels, cols = traj.shape
    main = tracers * levels
    mine = pl.multiple_of(plan.core() * 2 * main, SUB)
    theirs = pl.multiple_of((1 - plan.core()) * 2 * main, SUB)
    for m in range(tracers):
        for at, t, i in ((mine, traj, inc), (theirs, traj_too, inc_too)):
            rows_out[pl.ds(at + m * levels, levels), :cols] = t[m].astype(jnp.float32)
            rows_out[pl.ds(at + main + m * levels, levels), :cols] = i[m].astype(jnp.float32)
    rows_out[:, cols:] = jnp.zeros_like(rows_out[:, cols:])
    rows_out[4 * main :, :cols] = jnp.zeros_like(rows_out[4 * main :, :cols])
    beyond = ext[...].astype(jnp.float32) + ext_too[...].astype(jnp.float32)
    rows_out[4 * main : 4 * main + EDGE * tracers, :cols] = unpacked(beyond, EDGE * tracers, cols)


def gather(plan, traj, inc, traj_too, inc_too, ext, ext_too, rows, cols):
    return pl.pallas_call(
        functools.partial(gather_kernel, plan),
        in_specs=[VMEM] * 6,
        out_specs=VMEM,
        out_shape=jax.ShapeDtypeStruct((rows, cols), jnp.float32),
        compiler_params=pltpu.CompilerParams(vmem_limit_bytes=8 << 20),
        cost_estimate=cost(0, 6 * rows * cols),
        name="gather",
    )(traj, inc, traj_too, inc_too, ext, ext_too)


def forward_kernel(plan, which, scale, tail, counts, rows_in, courant, vertical, offset, w, edges, out):
    reach, rows, cols = plan.reach, rows_in.shape[0], courant.shape[1]
    slots = w.shape[-1]
    contract = (((1,), (1,)), ((), ()))
    lane = lax.broadcasted_iota(jnp.int32, (rows, LANE), 1)

    def slotted(group):
        base, shift, size = place(counts, group)
        turned = [
            pltpu.roll(x, lax.rem(LANE - shift, LANE), axis=1)
            for x in columns(rows_in[:, pl.ds(base, slots + LANE)])
        ]
        parts = []
        for at, (x, following) in enumerate(zip(turned[:-1], turned[1:])):
            x = jnp.where(lane < LANE - shift, x, following)
            parts.append(jnp.where(lane < size - at * LANE, x, 0.0))
        return jnp.concatenate(parts, axis=1).astype(jnp.bfloat16)

    group = plan.sent(which)
    y = slotted(group)
    out[...] = scale * lax.dot_general(y, w[which], contract, preferred_element_type=jnp.float32)
    for part, at in enumerate((cols - LANE, 0)):
        span = slice((2 + part) * LANE, (3 + part) * LANE)
        for row, ref in ((0, courant), (2, vertical)):
            value = ref[:, at : at + LANE]
            top = value.astype(jnp.bfloat16).astype(jnp.float32)
            out[tail + row : tail + row + 1, span] = scale * top
            out[tail + row + 1 : tail + row + 2, span] = scale * (value - top)
        out[tail + 4 : tail + 5, span] = scale * offset[:, at : at + LANE].astype(jnp.float32)

    def edge(weights, group):
        base, shift, size = place(counts, group)
        lane = lax.broadcasted_iota(jnp.int32, (SUB, LANE), 1)
        weights = shifted(weights, lane, shift, size).astype(jnp.bfloat16)
        x = rows_in[:, pl.ds(base, slots + LANE)].astype(jnp.bfloat16)
        return scale * lax.dot_general(weights, x, contract, preferred_element_type=jnp.float32)

    e_rows = edges[...].astype(jnp.float32)
    low, high = (e_rows[at : at + SUB] for at in (0, SUB))
    low = jnp.where(group == 0, low, e_rows[2 * SUB : 3 * SUB])
    high = jnp.where(group == reach - 2, high, e_rows[3 * SUB :])
    e = edge(low, lax.rem(group + reach - 1, reach))
    out[tail : tail + 2 * HALO, :rows] = e[SUB - 2 * HALO :]
    e = edge(high, lax.rem(group + 1, reach))
    out[tail : tail + 2 * HALO, LANE : LANE + rows] = e[: 2 * HALO]


def forward(plan, which, counts, rows_in, courant, vertical, offset, w, edges, scale, tail):
    rows = rows_in.shape[0]
    win, slots = w.shape[1:]
    return pl.pallas_call(
        functools.partial(forward_kernel, plan, which, scale, tail),
        in_specs=[VMEM] * 7,
        out_specs=VMEM,
        out_shape=jax.ShapeDtypeStruct((rows, win), jnp.float32),
        compiler_params=pltpu.CompilerParams(vmem_limit_bytes=8 << 20),
        cost_estimate=cost(2 * rows * win * slots, 4 * rows_in.size),
    )(counts, rows_in, courant, vertical, offset, w, edges)


def collect(plan, unscale, tail, numbers, pieces, acc, low, high, c_low, c_high):
    reach = plan.reach
    span = pieces[0].shape[1] // 2
    for k, piece in zip(numbers, pieces):
        group = plan.taken(k)
        first = pl.multiple_of(group * span, LANE)
        second = pl.multiple_of(lax.rem(group + 1, reach) * span, LANE)
        acc[:, pl.ds(first, span)] += unscale * piece[:, :span]
        acc[:, pl.ds(second, span)] += unscale * piece[:, span:]
        is_low = (group == 0) | (group == reach - 1)
        is_high = (group == reach - 2) | (group == reach - 1)
        low = low + jnp.where(is_low, piece[tail : tail + 2 * HALO, :LANE], 0.0)
        high = high + jnp.where(is_high, piece[tail : tail + 2 * HALO, LANE : 2 * LANE], 0.0)
        c_low = jnp.where(group == reach // 2 + 1, piece[tail : tail + COEFS, 2 * LANE : 3 * LANE], c_low)
        c_high = jnp.where(group == reach // 2 - 1, piece[tail : tail + COEFS, 3 * LANE :], c_high)
    return low, high, c_low, c_high


HALO_SLOTS = ((0, 2 * HALO), (SUB, 2 * HALO), (2 * SUB, COEFS), (3 * SUB, COEFS))


def assemble_kernel(plan, unscale, tail, numbers, *refs):
    pieces, (acc, side) = refs[:-2], refs[-2:]
    acc[...] = jnp.zeros_like(acc)
    side[...] = jnp.zeros_like(side)
    blank = [jnp.zeros((size, LANE), jnp.float32) for _, size in HALO_SLOTS]
    halo = collect(plan, unscale, tail, numbers, pieces, acc, *blank)
    for (at, size), part in zip(HALO_SLOTS, halo):
        side[at : at + size, :] = part


def assemble(plan, numbers, pieces, unscale, tail, cols):
    rows = pieces[0].shape[0]
    return pl.pallas_call(
        functools.partial(assemble_kernel, plan, unscale, tail, numbers),
        in_specs=[VMEM] * len(pieces),
        out_specs=[VMEM] * 2,
        out_shape=[
            jax.ShapeDtypeStruct((rows, cols + LANE), jnp.float32),
            jax.ShapeDtypeStruct((4 * SUB, LANE), jnp.float32),
        ],
        compiler_params=pltpu.CompilerParams(vmem_limit_bytes=8 << 20),
        cost_estimate=cost(4 * rows * cols, 8 * rows * cols),
        name="assemble",
    )(*pieces)


def stencil_kernel(plan, unscale, tail, numbers, kappa_in, acc_in, side, *refs):
    rounds, reach = plan.rounds, plan.reach
    pieces = refs[: len(numbers)]
    courant_in, vertical_in, offset_in, tangent_out = refs[len(numbers) : len(numbers) + 4]
    windows_out = refs[len(numbers) + 4 : len(numbers) + 4 + rounds]
    acc, turn, adj = refs[len(numbers) + 4 + rounds :]
    tracers = kappa_in.shape[1]
    levels = tangent_out.shape[0] // (2 * tracers)
    cols = courant_in.shape[1]
    main = tracers * levels
    rows = acc.shape[0]
    span = cols // reach
    wide = cols + LANE

    acc[...] = acc_in[...]
    halo = [side[at : at + size, :] for at, size in HALO_SLOTS]
    low, high, c_low, c_high = collect(plan, unscale, tail, numbers, pieces, acc, *halo)
    turn[...] = jnp.zeros_like(turn)
    turn[: 2 * HALO, :] = unscale * high
    turn[LANE - 2 * HALO :, :] = unscale * low
    acc[:, cols:] = turn[...].T[:rows, :]

    lane = lax.broadcasted_iota(jnp.int32, (COEFS, LANE), 1)
    beyond = unscale * jnp.where(lane < LANE // 2, c_high, c_low)
    spread = lambda row: jnp.broadcast_to(row, (SUB, wide))
    kappa = [jnp.broadcast_to(kappa_in[:, m : m + 1], (SUB, wide)) for m in range(tracers)]
    row_of = lambda ref, extra: spread(jnp.concatenate([ref[...].astype(jnp.float32), extra], axis=1))
    courant = row_of(courant_in, beyond[0:1] + beyond[1:2])
    vertical = row_of(vertical_in, beyond[2:3] + beyond[3:4])
    offset = row_of(offset_in, beyond[4:5])
    rising = jnp.maximum(vertical, 0.0)
    sinking = jnp.maximum(-vertical, 0.0)
    shifts = range(-HALO, HALO + 1)
    upwind = {s: jnp.where(offset == jnp.float32(s), courant, 0.0) for s in shifts}
    turned = lambda x, by: x if by % wide == 0 else pltpu.roll(x, by % wide, axis=1)
    downwind = {s: turned(upwind[s], s) for s in shifts}
    keep = 1.0 - courant - rising - sinking

    def tangent_of(delta, loss, below, above):
        moved = (keep - loss) * delta
        for s in shifts:
            moved = moved + upwind[s] * turned(delta, -s)
        return moved + rising * below + sinking * above

    sub = lax.broadcasted_iota(jnp.int32, (SUB, wide), 0)
    has_prev, has_next = plan.has_prev(), plan.has_next()
    state_of = lambda h, m: acc[2 * h * main + m * levels : 2 * h * main + (m + 1) * levels, :]
    delta_of = lambda h, m: acc[(2 * h + 1) * main + m * levels : (2 * h + 1) * main + (m + 1) * levels, :]
    line = lambda r: acc[4 * main + r : 4 * main + r + 1, :]
    x_state = jnp.zeros((SUB, wide), jnp.float32)
    x_delta, x_below, x_above, x_kappa = x_state, x_state, x_state, x_state
    for m in range(tracers):
        here = sub == m
        outer = line(2 * tracers + m)
        first = delta_of(0, m)[:1]
        final = delta_of(1, m)[levels - 1 :]
        x_state = jnp.where(here, spread(line(m)), x_state)
        x_delta = jnp.where(here, spread(line(tracers + m)), x_delta)
        x_below = jnp.where(here, spread(jnp.where(has_next, final, outer)), x_below)
        x_above = jnp.where(here, spread(jnp.where(has_next, outer, first)), x_above)
        x_kappa = jnp.where(here, kappa[m], x_kappa)
    x_tangent = tangent_of(x_delta, 2.0 * x_kappa * x_state, x_below, x_above)

    def beside(halves, edge):
        lo, hi = halves
        lo_below = jnp.where(has_prev, edge, 0.0)
        hi_above = jnp.where(has_next, edge, 0.0)
        below = (
            jnp.where(sub == 0, spread(lo_below), pltpu.roll(lo, 1, axis=0)),
            jnp.where(sub == 0, spread(lo[levels - 1 :]), pltpu.roll(hi, 1, axis=0)),
        )
        above = (
            jnp.where(sub == levels - 1, spread(hi[:1]), pltpu.roll(lo, levels - 1, axis=0)),
            jnp.where(sub == levels - 1, spread(hi_above), pltpu.roll(hi, levels - 1, axis=0)),
        )
        return below, above

    for m in range(tracers):
        deltas = (delta_of(0, m), delta_of(1, m))
        losses = tuple(2.0 * kappa[m] * state_of(h, m) for h in range(2))
        below, above = beside(deltas, x_delta[m : m + 1])
        tangents = tuple(tangent_of(deltas[h], losses[h], below[h], above[h]) for h in range(2))
        for h in range(2):
            at = h * main + m * levels
            tangent_out[at : at + levels, :] = tangents[h][:, :cols]
        t_below, t_above = beside(tangents, x_tangent[m : m + 1])
        for h in range(2):
            tangent = tangents[h]
            adjoint = (keep - losses[h]) * tangent
            for s in shifts:
                adjoint = adjoint + downwind[s] * turned(tangent, s)
            adjoint = adjoint + rising * t_above[h] + sinking * t_below[h]
            at = h * main + m * levels
            adj[at : at + levels, :cols] = adjoint[:, :cols]
            adj[at : at + levels, cols:] = adjoint[:, :span]
    for j in range(rounds):
        first = pl.multiple_of(plan.taken(j) * span, LANE)
        windows_out[j][...] = adj[:, pl.ds(first, 2 * span)].astype(jnp.bfloat16)


def stencil(plan, kappa, acc, side, numbers, pieces, courant, vertical, offset, levels, unscale, tail):
    rows = pieces[0].shape[0]
    cols = courant.shape[1]
    span = cols // plan.reach
    main = 2 * kappa.shape[1] * levels
    return pl.pallas_call(
        functools.partial(stencil_kernel, plan, unscale, tail, numbers),
        in_specs=[VMEM] * (6 + len(pieces)),
        out_specs=[VMEM] * (1 + plan.rounds),
        out_shape=[jax.ShapeDtypeStruct((main, cols), jnp.float32)]
        + [jax.ShapeDtypeStruct((main, 2 * span), jnp.bfloat16)] * plan.rounds,
        scratch_shapes=[
            pltpu.VMEM((rows, cols + LANE), jnp.float32),
            pltpu.VMEM((LANE, LANE), jnp.float32),
            pltpu.VMEM((main, cols + span), jnp.float32),
        ],
        compiler_params=pltpu.CompilerParams(vmem_limit_bytes=24 << 20),
        cost_estimate=cost(100 * rows * cols, 8 * rows * cols),
        name="stencil",
    )(kappa, acc, side, *pieces, courant, vertical, offset)


def emit_kernel(plan, both, out):
    tracers, levels, _ = out.shape
    at = pl.multiple_of(plan.core() * tracers * levels, SUB)
    for m in range(tracers):
        out[m] = both[pl.ds(at + m * levels, levels), :]


def emit(plan, both, tracers):
    main, cols = both.shape
    return pl.pallas_call(
        functools.partial(emit_kernel, plan),
        in_specs=[VMEM],
        out_specs=VMEM,
        out_shape=jax.ShapeDtypeStruct((tracers, main // 2 // tracers, cols), jnp.float32),
        compiler_params=pltpu.CompilerParams(vmem_limit_bytes=4 << 20),
        cost_estimate=cost(0, 4 * both.size),
        name="emit",
    )(both)


def backward_kernel(plan, last, numbers, counts, weight, *refs):
    pieces = refs[: len(numbers)]
    start = refs[len(numbers)] if last else None
    out = refs[len(numbers) + last]
    acc = refs[-1] if last else out
    slots = weight.shape[-1]
    main = acc.shape[0]
    acc[...] = start[...] if last else jnp.zeros_like(acc)
    lane = lax.broadcasted_iota(jnp.int32, (main, LANE), 1)
    for k, piece in zip(numbers, pieces):
        group = plan.returned(k)
        both = piece[...].astype(jnp.float32)
        own = jnp.where(plan.core() == 0, both[:main], both[main:]).astype(jnp.bfloat16)
        grad = jnp.dot(own, weight[0, group], preferred_element_type=jnp.float32)
        base, shift, size = place(counts, group)
        acc[:, pl.ds(base, slots + LANE)] += shifted(grad, lane, shift, size)
    if last:
        tracers, levels, cols = out.shape
        for m in range(tracers):
            out[m] = acc[m * levels : (m + 1) * levels, :cols]


def backward(plan, counts, weight, numbers, pieces, start, shape):
    tracers, levels, cols = shape
    slots = weight.shape[-1]
    main = tracers * levels
    last = start is not None
    padded = (main, cols + slots)
    return pl.pallas_call(
        functools.partial(backward_kernel, plan, int(last), numbers),
        in_specs=[VMEM] * (2 + len(pieces) + last),
        out_specs=VMEM,
        out_shape=jax.ShapeDtypeStruct(shape if last else padded, jnp.float32),
        scratch_shapes=[pltpu.VMEM(padded, jnp.float32)] if last else [],
        compiler_params=pltpu.CompilerParams(vmem_limit_bytes=12 << 20),
        cost_estimate=cost(2 * len(pieces) * main * 512 * slots, weight.size),
        name="back_last" if last else "back",
    )(counts, weight, *pieces, *([start] if last else []))


def step(trajectory, increment, counts, remap_weight, kappa, courant, vertical, offset):
    tracers, levels, cols = trajectory.shape
    reach, _, slots = remap_weight.shape[1:]
    tiles, slabs = lax.axis_size("tile"), lax.axis_size("lev")
    if slabs not in (2, 4) or reach % 2:
        raise ValueError("unsupported mesh")
    both = ("tile", "lev")
    plan = Plan(tiles, slabs, reach)
    routes = [plan.route(j) for j in range(plan.rounds)]
    scale = send_scale(slots)
    tail = 4 * tracers * levels + EDGE * tracers
    rows = -(-(tail + COEFS) // SUB) * SUB

    swap = [(v, v ^ 1) for v in range(slabs)]
    near = [(v, v + 1 if v % 2 else v - 1) for v in range(slabs)]
    far = [(v, v + 2 if v % 2 else v - 2) for v in range(slabs)]
    near, far = ([(a, b) for a, b in way if 0 <= b < slabs] for way in (near, far))
    traj_own, inc_own, border = fetch_border(plan, *(pltpu.with_memory_space_constraint(x, pltpu.HBM) for x in (trajectory, increment)))
    ext = lax.ppermute(border, "lev", near)
    ext_too = lax.ppermute(border, "lev", far)

    traj_too = lax.ppermute(trajectory, "lev", swap)
    inc_too = lax.ppermute(increment, "lev", swap)

    w, edges = load(plan, pltpu.with_memory_space_constraint(remap_weight, pltpu.HBM))
    lines = [x.reshape(1, cols) for x in (courant, vertical, offset)]
    rows_in = gather(plan, traj_own, inc_own, traj_too, inc_too, ext, ext_too, rows, cols + slots)
    pieces, message_0 = [], None
    for j, route in enumerate(routes):
        message = forward(plan, j, counts, rows_in, *lines, w, edges, scale, tail)
        message = message.astype(jnp.float16)
        message_0 = message_0 if j else message
        pieces.append(lax.ppermute(message, both, route))
    if tiles != reach:
        hops = (reach // 2, -(reach // 2) - 1)
        route = [(t * slabs + v, (t + hops[v % 2]) % tiles * slabs + v) for t in range(tiles) for v in range(slabs)]
        corner = lax.ppermute(message_0[tail:, : 2 * LANE], both, route)
        low_half = lax.broadcasted_iota(jnp.int32, corner.shape, 1) < LANE
        fresh = low_half == (lax.axis_index("lev") % 2 == 0)
        pieces[0] = pieces[0].at[tail:, : 2 * LANE].set(
            jnp.where(fresh, corner, pieces[0][tail:, : 2 * LANE])
        )
    others = []
    for piece in pieces:
        others.append(lax.ppermute(piece, "lev", swap))
    whole = [piece.astype(jnp.float32) for piece in pieces + others]
    early = list(range(2 * plan.rounds - 1))
    late = [2 * plan.rounds - 1]
    pick = lambda values, numbers: [values[k] for k in numbers]

    acc, side = assemble(plan, early, pick(whole, early), 1.0 / scale, tail, cols)
    tangents, *windows = stencil(
        plan, kappa.reshape(1, -1), acc, side, late, pick(whole, late), *lines, levels, 1.0 / scale, tail
    )
    returned, regained = [], []
    for window, route in zip(windows, routes):
        returned.append(lax.ppermute(window, both, [(b, a) for a, b in route]))
    for window in returned:
        regained.append(lax.ppermute(window, "lev", swap))
    tangent = emit(plan, tangents, tracers)
    parts = returned + regained
    grad = backward(plan, counts, remap_weight, early, pick(parts, early), None, trajectory.shape)
    grad = backward(plan, counts, remap_weight, late, pick(parts, late), grad, trajectory.shape)
    return (tangent, grad)


def solution(mesh):
    return jax.shard_map(
        step,
        mesh=mesh,
        in_specs=(
            P(None, "lev", "tile"),
            P(None, "lev", "tile"),
            P("tile", None),
            P("tile", None, None, None),
            P(),
            P("tile"),
            P("tile"),
            P("tile"),
        ),
        out_specs=(P(None, "lev", "tile"), P(None, "lev", "tile")),
        check_vma=False,
    )
```

```python
import functools

import jax
import jax.numpy as jnp
from jax import lax
from jax.experimental import pallas as pl
from jax.experimental.pallas import tpu as pltpu
from jax.sharding import PartitionSpec as P

HALO = 2
LANE = 128
SUB = 8
EDGE = 3
COEFS = 5
PACK = 1024
TUNED = {8: ((5, 2, 6, 1), (4, 3, 7, 0))}
VALUE_MAX = 6.0
WEIGHT_MAX = 0.25
F16_MAX = 65504.0


VMEM = pl.BlockSpec(memory_space=pltpu.VMEM)
SMEM = pl.BlockSpec(memory_space=pltpu.SMEM)
HBM = pl.BlockSpec(memory_space=pltpu.HBM)


def send_scale(slot_count):
    bound = VALUE_MAX * WEIGHT_MAX * slot_count
    scale = 1.0
    while 2.0 * scale * bound < F16_MAX:
        scale *= 2.0
    while scale * bound >= F16_MAX:
        scale *= 0.5
    return scale


def cost(flops, moved):
    return pl.CostEstimate(flops=flops, bytes_accessed=moved, transcendentals=0)


def place(counts, which):
    sizes = counts[...].astype(jnp.float32)
    lane = lax.broadcasted_iota(jnp.int32, sizes.shape, 1)
    packed = jnp.sum(jnp.where(lane < which, PACK * sizes, jnp.where(lane == which, sizes, 0.0)))
    packed = packed.astype(jnp.int32)
    begin = packed // PACK
    size = packed - begin * PACK
    base = pl.multiple_of((begin // LANE) * LANE, LANE)
    return base, begin - base, size


def columns(x):
    return [x[:, at : at + LANE] for at in range(0, x.shape[1], LANE)]


def shifted(x, lane, shift, size):
    turned = [
        pltpu.roll(jnp.where(lane < size - at * LANE, part, 0.0), shift, axis=1)
        for at, part in enumerate(columns(x))
    ]
    blank = jnp.zeros_like(turned[0])
    parts = [jnp.where(lane < shift, low, high) for low, high in zip([blank] + turned, turned + [blank])]
    return jnp.concatenate(parts, axis=1)


class Plan:
    def __init__(self, tiles, slabs, reach):
        self.tiles, self.slabs, self.reach = tiles, slabs, reach
        self.rounds = reach // 2
        self.cube = tiles == reach and tiles & (tiles - 1) == 0
        if self.cube:
            self.hops = TUNED.get(reach) or self.balanced(reach)
        else:
            self.hops = [list(range(-(reach // 2), 0)), list(range(reach // 2 - 1, -1, -1))]

    def balanced(self, reach):
        hops, load = [[], []], [0, 0]
        for flip in range(reach - 1, -1, -1):
            core = 0 if (load[0], len(hops[0])) < (load[1], len(hops[1])) else 1
            core = 1 if flip == 0 or len(hops[0]) == self.rounds else core
            core = 0 if len(hops[1]) == self.rounds - (flip > 0) else core
            hops[core].append(flip)
            load[core] += (flip >> 1) + (flip & 1)
        return hops

    def target(self, tile, core, j):
        hop = self.hops[core][j]
        return tile ^ hop if self.cube else (tile + hop) % self.tiles

    def route(self, j):
        cells = [(t, v) for t in range(self.tiles) for v in range(self.slabs)]
        return [(t * self.slabs + v, self.target(t, v % 2, j) * self.slabs + v) for t, v in cells]

    def core(self):
        return lax.rem(lax.axis_index("lev"), 2)

    def has_next(self):
        return lax.axis_index("lev") < self.slabs - 2

    def has_prev(self):
        return lax.axis_index("lev") >= 2

    def group(self, core, j, sign):
        hop = jnp.where(core == 0, jnp.int32(self.hops[0][j]), jnp.int32(self.hops[1][j]))
        centre = self.reach // 2
        if not self.cube:
            return centre + hop
        tile = lax.axis_index("tile")
        return lax.rem(sign * ((tile ^ hop) - tile) + centre + self.reach, self.reach)

    def sent(self, j):
        return self.group(self.core(), j, 1)

    def taken(self, k):
        return self.group(self.owner(k), k % self.rounds, -1)

    def returned(self, k):
        return self.group(self.owner(k), k % self.rounds, 1)

    def owner(self, k):
        return self.core() if k < self.rounds else 1 - self.core()


def border_kernel(plan, traj, inc, fields, border, lines, sems):
    tracers, levels, cols = traj.shape
    copies = [
        pltpu.make_async_copy(traj, fields.at[pl.ds(0, tracers)], sems.at[0]),
        pltpu.make_async_copy(inc, fields.at[pl.ds(tracers, tracers)], sems.at[1]),
    ]
    for copy in copies:
        copy.start()
    for copy in copies:
        copy.wait()
    lower = plan.core() == 1
    row = 0
    for start, depth in ((0, 0), (tracers, 0), (tracers, 1)):
        for m in range(tracers):
            x = fields[start + m].astype(jnp.float32)
            low, high = levels - 1 - depth, depth
            line = jnp.where(lower, x[low : low + 1], x[high : high + 1])
            if row < SUB:
                lines[row : row + 1, :cols] = line
            else:
                part = cols // SUB
                at = cols + (row - SUB) * part
                for piece in range(SUB):
                    lines[piece : piece + 1, at : at + part] = line[:, piece * part : (piece + 1) * part]
            row += 1
    border[...] = lines[...].astype(border.dtype)


def unpacked(border, count, cols):
    part = cols // SUB
    rows = [border[:, :cols]]
    for row in range(SUB, count):
        at = cols + (row - SUB) * part
        pieces = [border[piece : piece + 1, at : at + part] for piece in range(SUB)]
        rows.append(jnp.concatenate(pieces, axis=1))
    return jnp.concatenate(rows, axis=0)[:count]


def fetch_border(plan, traj, inc):
    tracers, levels, cols = traj.shape
    like = lambda *shape: jax.ShapeDtypeStruct(shape, traj.dtype)
    wide = cols + max(0, EDGE * tracers - SUB) * (cols // SUB)
    return pl.pallas_call(
        functools.partial(border_kernel, plan),
        in_specs=[HBM] * 2,
        out_specs=[VMEM] * 2,
        out_shape=[like(2 * tracers, levels, cols), like(SUB, wide)],
        scratch_shapes=[pltpu.VMEM((SUB, wide), jnp.float32), pltpu.SemaphoreType.DMA((2,))],
        compiler_params=pltpu.CompilerParams(vmem_limit_bytes=4 << 20),
        cost_estimate=cost(0, 8 * traj.size),
        name="border",
    )(traj, inc)


def load_kernel(plan, weight, w_out, edges, sems):
    reach, win = weight.shape[1:3]
    half = win // 2
    copies = [
        pltpu.make_async_copy(weight.at[0, plan.sent(j)], w_out.at[j], sems.at[j])
        for j in range(plan.rounds)
    ]
    parts = ((reach - 1, half - SUB, 2 * SUB), (reach - 2, win - SUB, SUB), (0, 0, SUB))
    at = 0
    for part, (group, first, size) in enumerate(parts):
        copies.append(
            pltpu.make_async_copy(
                weight.at[0, group, pl.ds(first, size)], edges.at[pl.ds(at, size)], sems.at[plan.rounds + part]
            )
        )
        at += size
    for copy in copies:
        copy.start()
    for copy in copies:
        copy.wait()


def load(plan, weight):
    _, _, win, slots = weight.shape
    like = lambda *shape: jax.ShapeDtypeStruct(shape, weight.dtype)
    return pl.pallas_call(
        functools.partial(load_kernel, plan),
        in_specs=[HBM],
        out_specs=[VMEM] * 2,
        out_shape=[like(plan.rounds, win, slots), like(4 * SUB, slots)],
        scratch_shapes=[pltpu.SemaphoreType.DMA((plan.rounds + 3,))],
        compiler_params=pltpu.CompilerParams(vmem_limit_bytes=8 << 20),
        cost_estimate=cost(0, 4 * plan.rounds * win * slots),
        name="fetch",
    )(weight)


def gather_kernel(plan, fields, fields_too, ext, ext_too, rows_out):
    levels, cols = fields.shape[1:]
    tracers = fields.shape[0] // 2
    main = tracers * levels
    mine = pl.multiple_of(plan.core() * 2 * main, SUB)
    theirs = pl.multiple_of((1 - plan.core()) * 2 * main, SUB)
    for m in range(tracers):
        for at, both in ((mine, fields), (theirs, fields_too)):
            rows_out[pl.ds(at + m * levels, levels), :cols] = both[m].astype(jnp.float32)
            rows_out[pl.ds(at + main + m * levels, levels), :cols] = both[tracers + m].astype(jnp.float32)
    rows_out[:, cols:] = jnp.zeros_like(rows_out[:, cols:])
    rows_out[4 * main :, :cols] = jnp.zeros_like(rows_out[4 * main :, :cols])
    beyond = ext[...].astype(jnp.float32) + ext_too[...].astype(jnp.float32)
    rows_out[4 * main : 4 * main + EDGE * tracers, :cols] = unpacked(beyond, EDGE * tracers, cols)


def gather(plan, fields, fields_too, ext, ext_too, rows, cols):
    return pl.pallas_call(
        functools.partial(gather_kernel, plan),
        in_specs=[VMEM] * 4,
        out_specs=VMEM,
        out_shape=jax.ShapeDtypeStruct((rows, cols), jnp.float32),
        compiler_params=pltpu.CompilerParams(vmem_limit_bytes=8 << 20),
        cost_estimate=cost(0, 6 * rows * cols),
        name="gather",
    )(fields, fields_too, ext, ext_too)


def forward_kernel(plan, which, scale, tail, counts, rows_in, courant, vertical, offset, w, edges, out):
    reach, rows, cols = plan.reach, rows_in.shape[0], courant.shape[1]
    slots = w.shape[-1]
    contract = (((1,), (1,)), ((), ()))
    lane = lax.broadcasted_iota(jnp.int32, (rows, LANE), 1)

    def slotted(group):
        base, shift, size = place(counts, group)
        turned = [
            pltpu.roll(x, lax.rem(LANE - shift, LANE), axis=1)
            for x in columns(rows_in[:, pl.ds(base, slots + LANE)])
        ]
        parts = []
        for at, (x, following) in enumerate(zip(turned[:-1], turned[1:])):
            x = jnp.where(lane < LANE - shift, x, following)
            parts.append(jnp.where(lane < size - at * LANE, x, 0.0))
        return jnp.concatenate(parts, axis=1).astype(jnp.bfloat16)

    group = plan.sent(which)
    y = slotted(group)
    out[...] = scale * lax.dot_general(y, w[which], contract, preferred_element_type=jnp.float32)
    for part, at in enumerate((cols - LANE, 0)):
        span = slice((2 + part) * LANE, (3 + part) * LANE)
        for row, ref in ((0, courant), (2, vertical)):
            value = ref[:, at : at + LANE]
            top = value.astype(jnp.bfloat16).astype(jnp.float32)
            out[tail + row : tail + row + 1, span] = scale * top
            out[tail + row + 1 : tail + row + 2, span] = scale * (value - top)
        out[tail + 4 : tail + 5, span] = scale * offset[:, at : at + LANE].astype(jnp.float32)

    def edge(weights, group):
        base, shift, size = place(counts, group)
        lane = lax.broadcasted_iota(jnp.int32, (SUB, LANE), 1)
        weights = shifted(weights, lane, shift, size).astype(jnp.bfloat16)
        x = rows_in[:, pl.ds(base, slots + LANE)].astype(jnp.bfloat16)
        return scale * lax.dot_general(weights, x, contract, preferred_element_type=jnp.float32)

    e_rows = edges[...].astype(jnp.float32)
    low, high = (e_rows[at : at + SUB] for at in (0, SUB))
    low = jnp.where(group == 0, low, e_rows[2 * SUB : 3 * SUB])
    high = jnp.where(group == reach - 2, high, e_rows[3 * SUB :])
    e = edge(low, lax.rem(group + reach - 1, reach))
    out[tail : tail + 2 * HALO, :rows] = e[SUB - 2 * HALO :]
    e = edge(high, lax.rem(group + 1, reach))
    out[tail : tail + 2 * HALO, LANE : LANE + rows] = e[: 2 * HALO]


def forward(plan, which, counts, rows_in, courant, vertical, offset, w, edges, scale, tail):
    rows = rows_in.shape[0]
    win, slots = w.shape[1:]
    return pl.pallas_call(
        functools.partial(forward_kernel, plan, which, scale, tail),
        in_specs=[VMEM] * 7,
        out_specs=VMEM,
        out_shape=jax.ShapeDtypeStruct((rows, win), jnp.float32),
        compiler_params=pltpu.CompilerParams(vmem_limit_bytes=8 << 20),
        cost_estimate=cost(2 * rows * win * slots, 4 * rows_in.size),
    )(counts, rows_in, courant, vertical, offset, w, edges)


def collect(plan, unscale, tail, numbers, pieces, acc, low, high, c_low, c_high):
    reach = plan.reach
    span = pieces[0].shape[1] // 2
    for k, piece in zip(numbers, pieces):
        group = plan.taken(k)
        first = pl.multiple_of(group * span, LANE)
        second = pl.multiple_of(lax.rem(group + 1, reach) * span, LANE)
        acc[:, pl.ds(first, span)] += unscale * piece[:, :span]
        acc[:, pl.ds(second, span)] += unscale * piece[:, span:]
        is_low = (group == 0) | (group == reach - 1)
        is_high = (group == reach - 2) | (group == reach - 1)
        low = low + jnp.where(is_low, piece[tail : tail + 2 * HALO, :LANE], 0.0)
        high = high + jnp.where(is_high, piece[tail : tail + 2 * HALO, LANE : 2 * LANE], 0.0)
        c_low = jnp.where(group == reach // 2 + 1, piece[tail : tail + COEFS, 2 * LANE : 3 * LANE], c_low)
        c_high = jnp.where(group == reach // 2 - 1, piece[tail : tail + COEFS, 3 * LANE :], c_high)
    return low, high, c_low, c_high


HALO_SLOTS = ((0, 2 * HALO), (SUB, 2 * HALO), (2 * SUB, COEFS), (3 * SUB, COEFS))


def assemble_kernel(plan, unscale, tail, numbers, *refs):
    pieces, (acc, side) = refs[:-2], refs[-2:]
    acc[...] = jnp.zeros_like(acc)
    side[...] = jnp.zeros_like(side)
    blank = [jnp.zeros((size, LANE), jnp.float32) for _, size in HALO_SLOTS]
    halo = collect(plan, unscale, tail, numbers, pieces, acc, *blank)
    for (at, size), part in zip(HALO_SLOTS, halo):
        side[at : at + size, :] = part


def assemble(plan, numbers, pieces, unscale, tail, cols):
    rows = pieces[0].shape[0]
    return pl.pallas_call(
        functools.partial(assemble_kernel, plan, unscale, tail, numbers),
        in_specs=[VMEM] * len(pieces),
        out_specs=[VMEM] * 2,
        out_shape=[
            jax.ShapeDtypeStruct((rows, cols + LANE), jnp.float32),
            jax.ShapeDtypeStruct((4 * SUB, LANE), jnp.float32),
        ],
        compiler_params=pltpu.CompilerParams(vmem_limit_bytes=8 << 20),
        cost_estimate=cost(4 * rows * cols, 8 * rows * cols),
        name="assemble",
    )(*pieces)


def stencil_kernel(plan, unscale, tail, numbers, kappa_in, acc_in, side, *refs):
    rounds, reach = plan.rounds, plan.reach
    pieces = refs[: len(numbers)]
    courant_in, vertical_in, offset_in, tangent_out = refs[len(numbers) : len(numbers) + 4]
    windows_out = refs[len(numbers) + 4 : len(numbers) + 4 + rounds]
    acc, turn, adj = refs[len(numbers) + 4 + rounds :]
    tracers = kappa_in.shape[1]
    levels = tangent_out.shape[0] // (2 * tracers)
    cols = courant_in.shape[1]
    main = tracers * levels
    rows = acc.shape[0]
    span = cols // reach
    wide = cols + LANE

    acc[...] = acc_in[...]
    halo = [side[at : at + size, :] for at, size in HALO_SLOTS]
    low, high, c_low, c_high = collect(plan, unscale, tail, numbers, pieces, acc, *halo)
    turn[...] = jnp.zeros_like(turn)
    turn[: 2 * HALO, :] = unscale * high
    turn[LANE - 2 * HALO :, :] = unscale * low
    acc[:, cols:] = turn[...].T[:rows, :]

    lane = lax.broadcasted_iota(jnp.int32, (COEFS, LANE), 1)
    beyond = unscale * jnp.where(lane < LANE // 2, c_high, c_low)
    spread = lambda row: jnp.broadcast_to(row, (SUB, wide))
    kappa = [jnp.broadcast_to(kappa_in[:, m : m + 1], (SUB, wide)) for m in range(tracers)]
    row_of = lambda ref, extra: spread(jnp.concatenate([ref[...].astype(jnp.float32), extra], axis=1))
    courant = row_of(courant_in, beyond[0:1] + beyond[1:2])
    vertical = row_of(vertical_in, beyond[2:3] + beyond[3:4])
    offset = row_of(offset_in, beyond[4:5])
    rising = jnp.maximum(vertical, 0.0)
    sinking = jnp.maximum(-vertical, 0.0)
    shifts = range(-HALO, HALO + 1)
    upwind = {s: jnp.where(offset == jnp.float32(s), courant, 0.0) for s in shifts}
    turned = lambda x, by: x if by % wide == 0 else pltpu.roll(x, by % wide, axis=1)
    downwind = {s: turned(upwind[s], s) for s in shifts}
    keep = 1.0 - courant - rising - sinking

    def tangent_of(delta, loss, below, above):
        moved = (keep - loss) * delta
        for s in shifts:
            moved = moved + upwind[s] * turned(delta, -s)
        return moved + rising * below + sinking * above

    sub = lax.broadcasted_iota(jnp.int32, (SUB, wide), 0)
    has_prev, has_next = plan.has_prev(), plan.has_next()
    state_of = lambda h, m: acc[2 * h * main + m * levels : 2 * h * main + (m + 1) * levels, :]
    delta_of = lambda h, m: acc[(2 * h + 1) * main + m * levels : (2 * h + 1) * main + (m + 1) * levels, :]
    line = lambda r: acc[4 * main + r : 4 * main + r + 1, :]
    x_state = jnp.zeros((SUB, wide), jnp.float32)
    x_delta, x_below, x_above, x_kappa = x_state, x_state, x_state, x_state
    for m in range(tracers):
        here = sub == m
        outer = line(2 * tracers + m)
        first = delta_of(0, m)[:1]
        final = delta_of(1, m)[levels - 1 :]
        x_state = jnp.where(here, spread(line(m)), x_state)
        x_delta = jnp.where(here, spread(line(tracers + m)), x_delta)
        x_below = jnp.where(here, spread(jnp.where(has_next, final, outer)), x_below)
        x_above = jnp.where(here, spread(jnp.where(has_next, outer, first)), x_above)
        x_kappa = jnp.where(here, kappa[m], x_kappa)
    x_tangent = tangent_of(x_delta, 2.0 * x_kappa * x_state, x_below, x_above)

    def beside(halves, edge):
        lo, hi = halves
        lo_below = jnp.where(has_prev, edge, 0.0)
        hi_above = jnp.where(has_next, edge, 0.0)
        below = (
            jnp.where(sub == 0, spread(lo_below), pltpu.roll(lo, 1, axis=0)),
            jnp.where(sub == 0, spread(lo[levels - 1 :]), pltpu.roll(hi, 1, axis=0)),
        )
        above = (
            jnp.where(sub == levels - 1, spread(hi[:1]), pltpu.roll(lo, levels - 1, axis=0)),
            jnp.where(sub == levels - 1, spread(hi_above), pltpu.roll(hi, levels - 1, axis=0)),
        )
        return below, above

    for m in range(tracers):
        deltas = (delta_of(0, m), delta_of(1, m))
        losses = tuple(2.0 * kappa[m] * state_of(h, m) for h in range(2))
        below, above = beside(deltas, x_delta[m : m + 1])
        tangents = tuple(tangent_of(deltas[h], losses[h], below[h], above[h]) for h in range(2))
        for h in range(2):
            at = h * main + m * levels
            tangent_out[at : at + levels, :] = tangents[h][:, :cols]
        t_below, t_above = beside(tangents, x_tangent[m : m + 1])
        for h in range(2):
            tangent = tangents[h]
            adjoint = (keep - losses[h]) * tangent
            for s in shifts:
                adjoint = adjoint + downwind[s] * turned(tangent, s)
            adjoint = adjoint + rising * t_above[h] + sinking * t_below[h]
            at = h * main + m * levels
            adj[at : at + levels, :cols] = adjoint[:, :cols]
            adj[at : at + levels, cols:] = adjoint[:, :span]
    for j in range(rounds):
        first = pl.multiple_of(plan.taken(j) * span, LANE)
        windows_out[j][...] = adj[:, pl.ds(first, 2 * span)].astype(jnp.bfloat16)


def stencil(plan, kappa, acc, side, numbers, pieces, courant, vertical, offset, levels, unscale, tail):
    rows = pieces[0].shape[0]
    cols = courant.shape[1]
    span = cols // plan.reach
    main = 2 * kappa.shape[1] * levels
    return pl.pallas_call(
        functools.partial(stencil_kernel, plan, unscale, tail, numbers),
        in_specs=[VMEM] * (6 + len(pieces)),
        out_specs=[VMEM] * (1 + plan.rounds),
        out_shape=[jax.ShapeDtypeStruct((main, cols), jnp.float32)]
        + [jax.ShapeDtypeStruct((main, 2 * span), jnp.bfloat16)] * plan.rounds,
        scratch_shapes=[
            pltpu.VMEM((rows, cols + LANE), jnp.float32),
            pltpu.VMEM((LANE, LANE), jnp.float32),
            pltpu.VMEM((main, cols + span), jnp.float32),
        ],
        compiler_params=pltpu.CompilerParams(vmem_limit_bytes=24 << 20),
        cost_estimate=cost(100 * rows * cols, 8 * rows * cols),
        name="stencil",
    )(kappa, acc, side, *pieces, courant, vertical, offset)


def emit_kernel(plan, both, out):
    tracers, levels, _ = out.shape
    at = pl.multiple_of(plan.core() * tracers * levels, SUB)
    for m in range(tracers):
        out[m] = both[pl.ds(at + m * levels, levels), :]


def emit(plan, both, tracers):
    main, cols = both.shape
    return pl.pallas_call(
        functools.partial(emit_kernel, plan),
        in_specs=[VMEM],
        out_specs=VMEM,
        out_shape=jax.ShapeDtypeStruct((tracers, main // 2 // tracers, cols), jnp.float32),
        compiler_params=pltpu.CompilerParams(vmem_limit_bytes=4 << 20),
        cost_estimate=cost(0, 4 * both.size),
        name="emit",
    )(both)


def backward_kernel(plan, last, numbers, counts, weight, *refs):
    pieces = refs[: len(numbers)]
    start = refs[len(numbers)] if last else None
    out = refs[len(numbers) + last]
    acc = refs[-1] if last else out
    slots = weight.shape[-1]
    main = acc.shape[0]
    acc[...] = start[...] if last else jnp.zeros_like(acc)
    lane = lax.broadcasted_iota(jnp.int32, (main, LANE), 1)
    for k, piece in zip(numbers, pieces):
        group = plan.returned(k)
        both = piece[...].astype(jnp.float32)
        own = jnp.where(plan.core() == 0, both[:main], both[main:]).astype(jnp.bfloat16)
        grad = jnp.dot(own, weight[0, group], preferred_element_type=jnp.float32)
        base, shift, size = place(counts, group)
        acc[:, pl.ds(base, slots + LANE)] += shifted(grad, lane, shift, size)
    if last:
        tracers, levels, cols = out.shape
        for m in range(tracers):
            out[m] = acc[m * levels : (m + 1) * levels, :cols]


def backward(plan, counts, weight, numbers, pieces, start, shape):
    tracers, levels, cols = shape
    slots = weight.shape[-1]
    main = tracers * levels
    last = start is not None
    padded = (main, cols + slots)
    return pl.pallas_call(
        functools.partial(backward_kernel, plan, int(last), numbers),
        in_specs=[VMEM] * (2 + len(pieces) + last),
        out_specs=VMEM,
        out_shape=jax.ShapeDtypeStruct(shape if last else padded, jnp.float32),
        scratch_shapes=[pltpu.VMEM(padded, jnp.float32)] if last else [],
        compiler_params=pltpu.CompilerParams(vmem_limit_bytes=12 << 20),
        cost_estimate=cost(2 * len(pieces) * main * 512 * slots, weight.size),
        name="back_last" if last else "back",
    )(counts, weight, *pieces, *([start] if last else []))


def step(trajectory, increment, counts, remap_weight, kappa, courant, vertical, offset):
    tracers, levels, cols = trajectory.shape
    reach, _, slots = remap_weight.shape[1:]
    tiles, slabs = lax.axis_size("tile"), lax.axis_size("lev")
    if slabs not in (2, 4) or reach % 2:
        raise ValueError("unsupported mesh")
    both = ("tile", "lev")
    plan = Plan(tiles, slabs, reach)
    routes = [plan.route(j) for j in range(plan.rounds)]
    scale = send_scale(slots)
    tail = 4 * tracers * levels + EDGE * tracers
    rows = -(-(tail + COEFS) // SUB) * SUB

    swap = [(v, v ^ 1) for v in range(slabs)]
    near = [(v, v + 1 if v % 2 else v - 1) for v in range(slabs)]
    far = [(v, v + 2 if v % 2 else v - 2) for v in range(slabs)]
    near, far = ([(a, b) for a, b in way if 0 <= b < slabs] for way in (near, far))
    fields, border = fetch_border(plan, *(pltpu.with_memory_space_constraint(x, pltpu.HBM) for x in (trajectory, increment)))
    ext = lax.ppermute(border, "lev", near)
    ext_too = lax.ppermute(border, "lev", far)

    fields_too = lax.ppermute(fields, "lev", swap)

    w, edges = load(plan, pltpu.with_memory_space_constraint(remap_weight, pltpu.HBM))
    lines = [x.reshape(1, cols) for x in (courant, vertical, offset)]
    rows_in = gather(plan, fields, fields_too, ext, ext_too, rows, cols + slots)
    pieces, message_0 = [], None
    for j, route in enumerate(routes):
        message = forward(plan, j, counts, rows_in, *lines, w, edges, scale, tail)
        message = message.astype(jnp.float16)
        message_0 = message_0 if j else message
        pieces.append(lax.ppermute(message, both, route))
    if tiles != reach:
        hops = (reach // 2, -(reach // 2) - 1)
        route = [(t * slabs + v, (t + hops[v % 2]) % tiles * slabs + v) for t in range(tiles) for v in range(slabs)]
        corner = lax.ppermute(message_0[tail:, : 2 * LANE], both, route)
        low_half = lax.broadcasted_iota(jnp.int32, corner.shape, 1) < LANE
        fresh = low_half == (lax.axis_index("lev") % 2 == 0)
        pieces[0] = pieces[0].at[tail:, : 2 * LANE].set(
            jnp.where(fresh, corner, pieces[0][tail:, : 2 * LANE])
        )
    others = []
    for piece in pieces:
        others.append(lax.ppermute(piece, "lev", swap))
    whole = [piece.astype(jnp.float32) for piece in pieces + others]
    early = list(range(2 * plan.rounds - 1))
    late = [2 * plan.rounds - 1]
    pick = lambda values, numbers: [values[k] for k in numbers]

    acc, side = assemble(plan, early, pick(whole, early), 1.0 / scale, tail, cols)
    tangents, *windows = stencil(
        plan, kappa.reshape(1, -1), acc, side, late, pick(whole, late), *lines, levels, 1.0 / scale, tail
    )
    returned, regained = [], []
    for window, route in zip(windows, routes):
        returned.append(lax.ppermute(window, both, [(b, a) for a, b in route]))
    for window in returned:
        regained.append(lax.ppermute(window, "lev", swap))
    tangent = emit(plan, tangents, tracers)
    parts = returned + regained
    grad = backward(plan, counts, remap_weight, early, pick(parts, early), None, trajectory.shape)
    grad = backward(plan, counts, remap_weight, late, pick(parts, late), grad, trajectory.shape)
    return (tangent, grad)


def solution(mesh):
    return jax.shard_map(
        step,
        mesh=mesh,
        in_specs=(
            P(None, "lev", "tile"),
            P(None, "lev", "tile"),
            P("tile", None),
            P("tile", None, None, None),
            P(),
            P("tile"),
            P("tile"),
            P("tile"),
        ),
        out_specs=(P(None, "lev", "tile"), P(None, "lev", "tile")),
        check_vma=False,
    )
```
